128 devices in a mesh: rep: 1, dp: 128 (over x, y, z, core).
Axes of the slice: x: 4, y: 4, z: 4, core: 2. Of those that a mesh axis runs over, the one named last changes fastest.
Arguments:
- x: bfloat16 [128, 2048, 768], P(('rep', 'dp'))
- dy: bfloat16 [128, 2048, 768], P(('rep', 'dp'))
- wq: bfloat16 [1, 768, 768], P(None, 'dp')
- wk: bfloat16 [1, 768, 128], P(None, 'dp')
- wv: bfloat16 [1, 768, 128], P(None, 'dp')
- wo: bfloat16 [1, 768, 768], P(None, 'dp')
- w_gate: bfloat16 [1, 768, 2048], P(None, 'dp')
- w_up: bfloat16 [1, 768, 2048], P(None, 'dp')
- w_down: bfloat16 [1, 2048, 768], P(None, 'dp')
Outputs:
- output 1: bfloat16 [128, 2048, 768], P(('rep', 'dp'))
- output 2: bfloat16 [1, 768, 768], P('rep', 'dp')
- output 3: bfloat16 [1, 768, 128], P('rep', 'dp')
- output 4: bfloat16 [1, 768, 128], P('rep', 'dp')
- output 5: bfloat16 [1, 768, 768], P('rep', 'dp')
- output 6: bfloat16 [1, 768, 2048], P('rep', 'dp')
- output 7: bfloat16 [1, 768, 2048], P('rep', 'dp')
- output 8: bfloat16 [1, 2048, 768], P('rep', 'dp')
All inputs are finite; a program needn't handle non-finite values.
Results may differ from the reference program's by a relative error of at most 0.024.
Values are sent between devices in bfloat16 or wider.
A program may use at most 1.5 GiB of HBM per device.

```python
import jax
import jax.numpy as jnp
from jax import lax

SEQUENCES = 128
TOKENS = 2048
D = 768
HEADS = 6
KV_HEADS = 1
HEAD = 128
FF = 2048
LAYERS = 1
THETA = 10000
NAMES = ("wq", "wk", "wv", "wo", "w_gate", "w_up", "w_down")
SHAPES = {
    "wq": (LAYERS, D, HEADS * HEAD),
    "wk": (LAYERS, D, KV_HEADS * HEAD),
    "wv": (LAYERS, D, KV_HEADS * HEAD),
    "wo": (LAYERS, HEADS * HEAD, D),
    "w_gate": (LAYERS, D, FF),
    "w_up": (LAYERS, D, FF),
    "w_down": (LAYERS, FF, D),
}


def bump(key, n, height):
    away = (jnp.arange(n, dtype=jnp.int32) - jax.random.randint(key, (), 0, n, jnp.int32)) % n
    return jnp.where(away < n // 8, height, 1.0)


def together(key, own, strength):
    shared = jax.random.normal(key, own.shape[1:], jnp.float32)
    return (own + strength * shared) * lax.rsqrt(1 + strength * strength)


def setup_inputs(seed: int = 0, part: int = 0) -> dict:
    kx, kdy, ka, kb, kz, kf, kh, kl, *keys = jax.random.split(jax.random.key(seed), 8 + 3 * len(NAMES))
    kx, kdy, ka, kb = (jax.random.fold_in(k, part) for k in (kx, kdy, ka, kb))
    kw, km, kv = (keys[i::3] for i in range(3))
    shape = (SEQUENCES, TOKENS, D)
    much_x, much_dy = jax.random.uniform(kz, (2,), jnp.float32, 0.0, 1.0)
    loud = 2.0 ** jax.random.uniform(jax.random.fold_in(kz, 1), (), jnp.float32, -1.0, 2.0)
    layers = 2.0 ** jax.random.uniform(kl, (LAYERS, 1, 1), jnp.float32, -1.0, 1.0)
    times = {"wq": 1.0, "wk": 1.0, "wv": 2.0, "wo": layers, "w_gate": 1.0, "w_up": bump(kh, FF, 4.0), "w_down": layers}
    x = together(ka, jax.random.normal(kx, shape, jnp.float32), much_x) * bump(kf, D, 4.0)
    dy = together(kb, jax.random.normal(kdy, shape, jnp.float32), much_dy)
    drawn = {"x": x.astype(jnp.bfloat16), "dy": (loud * dy * (SEQUENCES * TOKENS) ** -0.5).astype(jnp.bfloat16)}
    for key, name in zip(kw, NAMES, strict=True):
        drawn[name] = (jax.random.normal(key, SHAPES[name], jnp.float32) * SHAPES[name][1] ** -0.5 * times[name]).astype(jnp.bfloat16)
    return drawn


def matmul(a, w):
    return jnp.dot(a, w, preferred_element_type=jnp.float32).astype(jnp.bfloat16)


def normed(h):
    wide = h.astype(jnp.float32)
    scale = lax.rsqrt(jnp.mean(wide**2, -1, keepdims=True) + 1e-6)
    return (wide * scale).astype(jnp.bfloat16)


def turned(t, theta):
    half = t.shape[-1] // 2
    angle = jnp.arange(t.shape[0], dtype=jnp.float32)[:, None] * theta ** (-jnp.arange(half, dtype=jnp.float32) / half)
    cos, sin = jnp.cos(angle)[:, None], jnp.sin(angle)[:, None]
    a, b = t[..., :half].astype(jnp.float32), t[..., half:].astype(jnp.float32)
    return jnp.concatenate([a * cos - b * sin, b * cos + a * sin], -1).astype(jnp.bfloat16)


def seen_by(q, k, v):
    tokens, kv = q.shape[0], k.shape[1]
    q = q.reshape(tokens, kv, -1, q.shape[-1])
    scores = jnp.einsum("tgsd,ugd->gstu", q.astype(jnp.float32), k.astype(jnp.float32)) * q.shape[-1] ** -0.5
    place = jnp.arange(tokens)
    weights = jax.nn.softmax(jnp.where(place[:, None] >= place, scores, -jnp.inf), -1).astype(jnp.bfloat16)
    return jnp.einsum("gstu,ugd->tgsd", weights.astype(jnp.float32), v.astype(jnp.float32)).astype(jnp.bfloat16).reshape(tokens, -1)


def layer(h, w):
    a = normed(h)
    q, k = (turned(matmul(a, w[name]).reshape(h.shape[0], -1, HEAD), THETA) for name in ("wq", "wk"))
    h = h + matmul(seen_by(q, k, matmul(a, w["wv"]).reshape(h.shape[0], -1, HEAD)), w["wo"])
    b = normed(h)
    gate = jnp.dot(b, w["w_gate"], preferred_element_type=jnp.float32)
    up = jnp.dot(b, w["w_up"], preferred_element_type=jnp.float32)
    return h + matmul((jax.nn.silu(gate) * up).astype(jnp.bfloat16), w["w_down"])


def stack(weights, h):
    return lax.scan(lambda h, w: (layer(h, w), None), h, weights)[0]


def reference(x, dy, wq, wk, wv, wo, w_gate, w_up, w_down):
    weights = dict(zip(NAMES, (wq, wk, wv, wo, w_gate, w_up, w_down), strict=True))

    def take(so_far, sequence):
        h, by_y = sequence
        _, back = jax.vjp(stack, weights, h)
        by_weights, by_h = back(by_y)
        return jax.tree.map(lambda total, term: total + term.astype(jnp.float32), so_far, by_weights), by_h

    none_yet = {name: jnp.zeros(w.shape, jnp.float32) for name, w in weights.items()}
    by_weights, by_x = lax.scan(take, none_yet, (x, dy))
    return (by_x, *(by_weights[name].astype(jnp.bfloat16) for name in NAMES))
```

```python
import functools

import jax
import jax.numpy as jnp
from jax import lax
from jax.experimental import pallas as pl
from jax.experimental.pallas import tpu as pltpu
from jax.sharding import PartitionSpec as P

HEAD = 128
THETA = 10000
EPS = 1e-6
ZERO, ONE, HALF, FULL, DIM, WIDE, ROWS, MATES, PLACES, SIX = 0, 1, 1024, 2048, 768, 256, 16, 8, 4, 6
GRID = (PLACES, PLACES)
NEG = -1e30
HIDDEN = 2 * NEG
LOG2E = 1.4426950408889634
VMEM = 56 * 2**20
BLOCK = 512
BF, F32 = jnp.bfloat16, jnp.float32
SCALE = HEAD**-0.5
E = SCALE * LOG2E


def _dot(a, b, ca, cb):
    return lax.dot_general(a, b, (((ca,), (cb,)), ((), ())), preferred_element_type=F32)


def _mm(a, b):
    return _dot(a, b, ONE, ZERO)


def _mt(a, b):
    return _dot(a, b, ONE, ONE)


def _first():
    return pl.program_id(ZERO) == ZERO


def _last():
    return pl.program_id(ZERO) == pl.num_programs(ZERO) - ONE


def _visible():
    return lax.broadcasted_iota(jnp.int32, (BLOCK, BLOCK), 0) <= lax.broadcasted_iota(jnp.int32, (BLOCK, BLOCK), 1)


def _forward(q_ref, k_ref, v_ref, o_ref, lse_ref, top_s, mix_s):
    heads = q_ref.shape[0]
    iq = pl.program_id(0)
    top_s[...] = jnp.full(top_s.shape, NEG, F32)
    mix_s[...] = jnp.zeros(mix_s.shape, F32)
    ones = jnp.ones((8, BLOCK), BF)

    def block(j, masked):
        here = pl.ds(j * BLOCK, BLOCK)
        scores = [_mt(k_ref[ZERO, here, :], q_ref[n]) for n in range(heads)]
        weights, keeps = [], []
        for n, s in enumerate(scores):
            if masked:
                s = jnp.where(_visible(), s, HIDDEN)
            old = top_s[n : n + ONE, :]
            top = jnp.maximum(old, s.max(axis=ZERO, keepdims=ONE))
            top_s[n : n + ONE, :] = top
            weights.append(jnp.exp2((s - top) * E).astype(BF))
            keeps.append(jnp.exp2((old - top) * E))
        values = jnp.concatenate([v_ref[ZERO, here, :].T, ones], axis=ZERO)
        for n, (p, keep) in enumerate(zip(weights, keeps, strict=ONE)):
            mix_s[n] = mix_s[n] * keep + _mm(values, p)

    lax.fori_loop(0, iq, lambda j, _: block(j, False), None)
    block(iq, True)
    for n in range(heads):
        total = mix_s[n, HEAD : HEAD + 1, :]
        o_ref[n] = (mix_s[n, :HEAD, :] * (1 / total)).T.astype(BF)
        lse_ref[n : n + ONE, :] = top_s[n : n + ONE, :] * SCALE + jnp.log(total)


def attend(q, k, v):
    heads, n, _ = q.shape
    block, whole = _second(heads, BLOCK, HEAD), _all(ONE, n, HEAD)
    return _call(_forward, "attend", n // BLOCK, [(q, *block), (k, *whole), (v, *whole)],
                 [((heads, n, HEAD), BF, *block), ((heads, n), F32, *_second(heads, BLOCK))],
                 [pltpu.VMEM((heads, BLOCK), F32), pltpu.VMEM((heads, HEAD + 8, BLOCK), F32)], flops=2 * heads * n * n * HEAD)


def _backward(q_ref, k_ref, v_ref, do_ref, lse_ref, delta_ref, dq_ref, dk_ref, dv_ref, dq_s, dk_s, dv_s):
    heads = q_ref.shape[0]
    iq = pl.program_id(0)

    @pl.when(_first())
    def _():
        dk_s[...] = jnp.zeros_like(dk_s)
        dv_s[...] = jnp.zeros_like(dv_s)

    dq_s[...] = jnp.zeros_like(dq_s)
    lses = [lse_ref[n : n + ONE, :] * LOG2E for n in range(heads)]

    def block(j, masked):
        here = pl.ds(j * BLOCK, BLOCK)
        scores = [_mt(k_ref[ZERO, here, :], q_ref[n]) for n in range(heads)]
        dps = [_mt(v_ref[ZERO, here, :], do_ref[n]) for n in range(heads)]
        for n in range(heads):
            p = jnp.exp2(scores[n] * E - lses[n])
            if masked:
                p = jnp.where(_visible(), p, 0.0)
            ds = (p * (dps[n] - delta_ref[n : n + ONE, :])).astype(BF)
            dv_s[here, :] += _mm(p.astype(BF), do_ref[n])
            dk_s[here, :] += _mm(ds, q_ref[n])
            dq_s[n] += _mm(k_ref[ZERO, here, :].T, ds)

    lax.fori_loop(0, iq, lambda j, _: block(j, False), None)
    block(iq, True)
    for n in range(heads):
        dq_ref[n] = (dq_s[n] * SCALE).T.astype(BF)

    @pl.when(_last())
    def _():
        dk_ref[ZERO] = (dk_s[...] * SCALE).astype(BF)
        dv_ref[ZERO] = dv_s[...].astype(BF)


def attend_bwd(q, k, v, d_out, lse, delta):
    heads, n, _ = q.shape
    block, whole, stats = _second(heads, BLOCK, HEAD), _all(ONE, n, HEAD), _second(heads, BLOCK)
    return _call(_backward, "attend_back", n // BLOCK,
                 [(q, *block), (k, *whole), (v, *whole), (d_out, *block), (lse, *stats), (delta, *stats)],
                 [((heads, n, HEAD), BF, *block), ((ONE, n, HEAD), BF, *whole), ((ONE, n, HEAD), BF, *whole)],
                 [pltpu.VMEM((heads, HEAD, BLOCK), F32), pltpu.VMEM((n, HEAD), F32), pltpu.VMEM((n, HEAD), F32)],
                 flops=5 * heads * n * n * HEAD)


TOKENS_STEP = 512


def _call(kernel, name, grid, ins, outs, scratch=(), flops=0):
    given = [a for a, _, _ in ins]
    moved = sum(a.size * a.dtype.itemsize for a in given)
    return pl.pallas_call(
        kernel,
        grid=(grid,),
        in_specs=[pl.BlockSpec(block, index) for _, block, index in ins],
        out_specs=[pl.BlockSpec(block, index) for _, _, block, index in outs],
        out_shape=[jax.ShapeDtypeStruct(shape, dtype) for shape, dtype, _, _ in outs],
        scratch_shapes=list(scratch),
        compiler_params=pltpu.CompilerParams(dimension_semantics=("arbitrary",), vmem_limit_bytes=VMEM),
        cost_estimate=pl.CostEstimate(flops=flops, transcendentals=0, bytes_accessed=2 * moved),
        name=name,
    )(*given)


def _rows(*shape):
    return shape, lambda i: (i,) + (0,) * (len(shape) - 1)


def _second(*shape):
    return shape, lambda i: (0, i) + (0,) * (len(shape) - 2)


def _all(*shape):
    return shape, lambda i: (0,) * len(shape)


def _norm(h):
    wide = h.astype(F32)
    return (wide * lax.rsqrt(jnp.mean(wide * wide, -1, keepdims=ONE) + EPS)).astype(BF)


def _norm_back(h, g):
    wide, g = h.astype(F32), g.astype(F32)
    scale = lax.rsqrt(jnp.mean(wide * wide, -1, keepdims=ONE) + EPS)
    return scale * (g - wide * (scale * scale * jnp.mean(g * wide, -1, keepdims=ONE)))


def _prepare(x_ref, dy_ref, a_ref, at_ref, dyt_ref):
    a = _norm(x_ref[...])
    a_ref[...] = a
    at_ref[...] = a.T
    dyt_ref[...] = dy_ref[...].T


def prepare(x, dy):
    n, d = x.shape
    s = TOKENS_STEP
    return _call(_prepare, "prepare", n // s, [(x, *_rows(s, d)), (dy, *_rows(s, d))],
                 [((n, d), BF, *_rows(s, d)), ((d, n), BF, *_second(d, s)), ((d, n), BF, *_second(d, s))])


def _project(a_ref, w_ref, cos_ref, sin_ref, q_ref, k_ref, v_ref):
    t = _mm(a_ref[...], w_ref[...]).astype(BF)
    cos, sin = cos_ref[...], sin_ref[...]
    heads = q_ref.shape[0]
    for n in range(heads + 1):
        one = t[:, n * HEAD : (n + 1) * HEAD].astype(F32)
        one = (one * cos + pltpu.roll(one, HEAD // 2, 1) * sin).astype(BF)
        if n < heads:
            q_ref[n] = one
        else:
            k_ref[ZERO] = one
    v_ref[ZERO] = t[:, (heads + 1) * HEAD :]


def project(a, mixed, cos, sin):
    n, d = a.shape
    s, heads = TOKENS_STEP, d // HEAD
    width = d + 2 * HEAD
    return _call(_project, "project", n // s,
                 [(a, *_rows(s, d)), (mixed, *_all(d, width)), (cos, *_rows(s, HEAD)), (sin, *_rows(s, HEAD))],
                 [((heads, n, HEAD), BF, *_second(heads, s, HEAD))] + [((ONE, n, HEAD), BF, *_second(ONE, s, HEAD))] * 2, flops=2 * n * d * width)


def _close(o_ref, x_ref, wo_ref, h_ref, b_ref, bt_ref):
    o = jnp.concatenate([o_ref[n] for n in range(o_ref.shape[0])], axis=ONE)
    h = x_ref[...] + _mm(o, wo_ref[...])[:, : x_ref.shape[1]].astype(BF)
    h_ref[...] = h
    b = _norm(h)
    b_ref[...] = b
    bt_ref[...] = b.T


def close(o, x, mixed):
    n, d = x.shape
    s, heads = TOKENS_STEP, o.shape[0]
    return _call(_close, "close", n // s, [(o, *_second(heads, s, HEAD)), (x, *_rows(s, d)), (mixed, (d, HALF), lambda i: (0, 1))],
                 [((n, d), BF, *_rows(s, d)), ((n, d), BF, *_rows(s, d)), ((d, n), BF, *_second(d, s))], flops=2 * n * d * d)


def _feed(b_ref, bt_ref, dy_ref, dyt_ref, wg_ref, wu_ref, wd_ref, db_ref, dwg_ref, dwu_ref, dwd_ref, db_s, z_s):
    f = wg_ref.shape[1]
    n = b_ref.shape[0]
    s = TOKENS_STEP

    @pl.when(_first())
    def _():
        db_s[...] = jnp.zeros_like(db_s)

    both = jnp.concatenate([wg_ref[...], wu_ref[...]], axis=ONE)
    for lo in range(0, n, s):
        here = slice(lo, lo + s)
        gate_up = _mm(b_ref[here, :], both)
        gate, up = gate_up[:, :f], gate_up[:, f:]
        dmid = _mt(dy_ref[here, :], wd_ref[...]).astype(BF).astype(F32)
        sig = 1 / (1 + jnp.exp2(gate * -LOG2E))
        silu = gate * sig
        z_s[here, 2 * f :] = (silu * up).astype(BF)
        dup = (dmid * silu).astype(BF)
        dgate = (dmid * up * (sig + silu * (1 - sig))).astype(BF)
        z_s[here, :f] = dgate
        z_s[here, f : 2 * f] = dup
        db_s[here, :] += _mt(jnp.concatenate([dgate, dup], axis=ONE), both)
    dw = _mm(bt_ref[...], z_s[:, : 2 * f])
    dwg_ref[...] = dw[:, :f].astype(BF)
    dwu_ref[...] = dw[:, f:].astype(BF)
    dwd_ref[...] = _mm(dyt_ref[...], z_s[:, 2 * f :]).astype(BF).T

    @pl.when(_last())
    def _():
        db_ref[...] = db_s[...].astype(BF)


FEED_STEP = 256


def feed(b, bt, dy, dyt, gate, up, down):
    n, d = b.shape
    f, ff = FEED_STEP, gate.shape[1]
    cols, rows = ((d, f), lambda i: (0, i)), ((f, d), lambda i: (i, 0))
    return _call(_feed, "feed", ff // f,
                 [(b, *_all(n, d)), (bt, *_all(d, n)), (dy, *_all(n, d)), (dyt, *_all(d, n)), (gate, *cols), (up, *cols), (down, *rows)],
                 [((n, d), BF, *_all(n, d)), ((d, ff), BF, *cols), ((d, ff), BF, *cols), ((ff, d), BF, *rows)],
                 [pltpu.VMEM((n, d), F32), pltpu.VMEM((n, 3 * f), BF)], flops=ROWS * n * d * ff)


def _open_back(db_ref, h_ref, dy_ref, o_ref, wo_ref, dh_ref, do_ref, delta_ref, dwo_ref, acc_s):
    i = pl.program_id(0)

    @pl.when(_first())
    def _():
        acc_s[...] = jnp.zeros_like(acc_s)

    heads = o_ref.shape[0]
    d = dy_ref.shape[1]
    dh = (dy_ref[...].astype(F32) + _norm_back(h_ref[...], db_ref[...])).astype(BF)
    dh_ref[...] = dh
    do = _mt(dh, wo_ref[:, :d]).astype(BF)
    for n in range(heads):
        mine = do[:, n * HEAD : (n + 1) * HEAD]
        do_ref[n] = mine
        delta_ref[n : n + ONE, :] = (mine.astype(F32) * o_ref[n].astype(F32)).T.sum(axis=ZERO, keepdims=ONE)
        acc_s[n * HEAD : (n + 1) * HEAD, :] += _dot(o_ref[n], dh, 0, 0)

    @pl.when(_last())
    def _():
        dwo_ref[:, :d] = acc_s[...].astype(BF)
        dwo_ref[:, d:] = jnp.zeros_like(dwo_ref[:, d:])


def open_back(db, h, dy, o, mixed):
    n, d = h.shape
    s, heads = TOKENS_STEP, o.shape[0]
    rows = _rows(s, d)
    return _call(_open_back, "open_back", n // s,
                 [(db, *rows), (h, *rows), (dy, *rows), (o, *_second(heads, s, HEAD)), (mixed, (d, HALF), lambda i: (0, 1))],
                 [((n, d), BF, *rows), ((heads, n, HEAD), BF, *_second(heads, s, HEAD)), ((heads, n), F32, *_second(heads, s)),
                  ((d, HALF), BF, *_all(d, HALF))], [pltpu.VMEM((d, d), F32)], flops=4 * n * d * d)


def _project_back(dq_ref, dk_ref, dv_ref, cos_ref, sin_ref, x_ref, dh_ref, at_ref, w_ref, dx_ref, dw_ref, acc_s):
    i = pl.program_id(0)

    @pl.when(_first())
    def _():
        acc_s[...] = jnp.zeros_like(acc_s)

    cos, sin = cos_ref[...], sin_ref[...]
    parts = []
    for one in (*(dq_ref[n] for n in range(dq_ref.shape[0])), dk_ref[ZERO]):
        one = one.astype(F32)
        parts.append((one * cos - pltpu.roll(one, HEAD // 2, 1) * sin).astype(BF))
    by = jnp.concatenate([*parts, dv_ref[ZERO]], axis=ONE)
    acc_s[...] += _mm(at_ref[...], by)
    da = _mt(by, w_ref[...]).astype(BF)
    dx_ref[...] = (dh_ref[...].astype(F32) + _norm_back(x_ref[...], da)).astype(BF)

    @pl.when(_last())
    def _():
        dw_ref[...] = acc_s[...].astype(BF)


def project_back(dq, dk, dv, cos, sin, x, dh, at, mixed):
    n, d = x.shape
    s, heads = TOKENS_STEP, dq.shape[0]
    rows, width = _rows(s, d), d + 2 * HEAD
    return _call(_project_back, "project_back", n // s,
                 [(dq, *_second(heads, s, HEAD)), (dk, *_second(ONE, s, HEAD)), (dv, *_second(ONE, s, HEAD)), (cos, *_rows(s, HEAD)),
                  (sin, *_rows(s, HEAD)), (x, *rows), (dh, *rows), (at, *_second(d, s)), (mixed, *_all(d, width))],
                 [((n, d), BF, *rows), ((d, width), BF, *_all(d, width))], [pltpu.VMEM((d, width), F32)], flops=4 * n * d * width)


def tables(n):
    half = HEAD // 2
    angle = jnp.arange(n, dtype=F32)[:, None] * THETA ** (-jnp.arange(half, dtype=F32) / half)
    cos, sin = jnp.cos(angle), jnp.sin(angle)
    return jnp.concatenate([cos, cos], -1), jnp.concatenate([-sin, sin], -1)


def through(x, dy, mixed, gate, up, down):
    cos, sin = tables(x.shape[ZERO])
    a, at, dyt = prepare(x, dy)
    q, k, v = project(a, mixed, cos, sin)
    o, lse = attend(q, k, v)
    h, b, bt = close(o, x, mixed)
    db, dwg, dwu, dwd = feed(b, bt, dy, dyt, gate, up, down)
    dh, do, delta, dwo = open_back(db, h, dy, o, mixed)
    dq, dk, dv = attend_bwd(q, k, v, do, lse, delta)
    dx, dqkv = project_back(dq, dk, dv, cos, sin, x, dh, at, mixed)
    return dx, dqkv, dwo, dwg, dwu, dwd


RING = 4
ORDERS = ("xyz", "yzx", "zxy")
MIXED, GATE, UP, DOWN = range(PLACES)


def _place():
    me = lax.axis_index("dp")
    return {"x": me // 32, "y": me // 8 % 4, "z": me // 2 % 4, "k": me % 2}


def _device(at, **other):
    at = {**at, **other}
    return {"dp": ((at["x"] * 4 + at["y"]) * 4 + at["z"]) * 2 + at["k"]}


def _beside(at, axis, by):
    return _device(at, **{axis: (at[axis] + by) % RING})


def _mate(at, by):
    other = (at["z"] * 2 + at["k"] + by) % 8
    return _device(at, z=other // 2, k=other % 2)


def _greet(at):
    barrier = pltpu.get_barrier_semaphore()
    peers = [_beside(at, axis, by) for axis in "xy" for by in (1, 3)] + [_mate(at, by) for by in range(1, 8)]
    for peer in peers:
        pl.semaphore_signal(barrier, inc=1, device_id=peer, device_id_type=pl.DeviceIdType.MESH)
    pl.semaphore_wait(barrier, len(peers))


def _remote(src, dst, send, recv, device):
    copy = pltpu.make_async_remote_copy(src_ref=src, dst_ref=dst, send_sem=send, recv_sem=recv, device_id=device,
                                        device_id_type=pl.DeviceIdType.MESH)
    copy.start()
    return copy


def _lanes(z, lo=0, n=WIDE):
    return pl.ds(pl.multiple_of(z * WIDE + lo, HEAD), n)


def _pieces(axis_at):
    return axis_at if axis_at is not None else slice(None)


def _gather_kernel(wq, wk, wv, wo, wg, wu, wd, mixed_o, gate_o, up_o, down_o, out_s, in_s, ws, wds, mate_sems, ring_send, ring_recv,
                   pair_send, pair_recv, own_sem):
    at = _place()
    seat = at["z"] * 2 + at["k"]
    outs = (mixed_o, gate_o, up_o)
    for j in range(MATES):
        first = (j % 2) * HALF + (j // 2) * WIDE
        for t in range(3):
            if t == MIXED:
                parts = []
                for lo in (first, first + HEAD):
                    for ref, base, width in ((wq, 0, DIM), (wk, DIM, HEAD), (wv, 896, HEAD), (wo, HALF, DIM)):
                        if base <= lo < base + width:
                            parts.append(ref[:, lo - base : lo - base + HEAD])
                if parts:
                    out_s[j, t, ZERO:SIX, :] = jnp.concatenate(parts, axis=ONE)
                else:
                    out_s[j, t, ZERO:SIX, :] = jnp.zeros((6, WIDE), BF)
            else:
                out_s[j, t, ZERO:SIX, :] = (wg, wu)[t - 1][:, first : first + WIDE]
            out_s[j, t, SIX:MATES, :] = jnp.zeros((2, WIDE), BF)
    _greet(at)
    copies = [_remote(out_s.at[(seat + by) % 8], in_s.at[seat], mate_sems.at[ZERO, by], mate_sems.at[ONE, by], _mate(at, by)) for by in range(1, 8)]
    in_s[seat] = out_s[seat]
    for c in range(3):
        wds[at["x"], at["y"], at["z"], :, WIDE * c : WIDE * c + WIDE] = wd[:, WIDE * c : WIDE * c + WIDE]

    def region(t, c, fixed, half=None):
        x, y = _pieces(fixed.get("x")), _pieces(fixed.get("y"))
        lo, n = (0, WIDE) if half is None else (HEAD * half, HEAD)
        if t == DOWN:
            return wds.at[x, y, _pieces(fixed.get("z")), :, WIDE * c + lo : WIDE * c + lo + n]
        if "z" in fixed:
            return ws.at[t, x, y, c, :, _lanes(fixed["z"], lo, n)]
        return ws.at[t, x, y, c]

    def half_of(t, c, fixed, half):
        if t != DOWN and "z" not in fixed:
            x, y = _pieces(fixed.get("x")), _pieces(fixed.get("y"))
            return ws.at[t, x, y, c, :, 512 * half : 512 * half + 512]
        return region(t, c, fixed, half)

    def known(c, phase, place):
        order = ORDERS[c][::-1]
        return {**{a: at[a] for a in order[phase + 1 :]}, order[phase]: place}

    def send_own(t, c, phase):
        axis = ORDERS[c][::-1][phase]
        here = region(t, c, known(c, phase, at[axis]))
        for slot, by in ((0, 1), (1, 3)):
            copies.append(_remote(here, here, ring_send.at[t, c, phase, slot], ring_recv.at[t, c, phase, slot], _beside(at, axis, by)))

    def landed(ref, t, c, phase, slot):
        pltpu.make_async_copy(ref, ref, ring_recv.at[t, c, phase, slot]).wait()

    def pass_on(t, c, phase):
        axis = ORDERS[c][::-1][phase]
        for slot, by in ((0, 3), (1, 1)):
            fixed = known(c, phase, (at[axis] + by) % RING)
            landed(region(t, c, fixed), t, c, phase, slot)
            half = 1 - slot
            here = half_of(t, c, fixed, half)
            copies.append(_remote(here, here, ring_send.at[t, c, phase, 2 + slot], ring_recv.at[t, c, phase, 2 + slot],
                                  _beside(at, axis, 1 if slot == 0 else 3)))

    def finish(t, c, phase):
        axis = ORDERS[c][::-1][phase]
        for slot in (0, 1):
            landed(half_of(t, c, known(c, phase, (at[axis] + 2) % RING), 1 - slot), t, c, phase, 2 + slot)

    order = (DOWN, MIXED, GATE, UP)

    def each(act, phase, ts):
        for t in ts:
            for c in range(3):
                act(t, c, phase)

    own = []

    def to_result(t):
        src = wds if t == DOWN else ws.at[t]
        if t == DOWN:
            dst = down_o.at[:, :, :, at["k"]]
        else:
            dst = outs[t].at[:, :, :, :, pl.ds(pl.multiple_of(at["k"] * HALF, HALF), HALF)]
        copies.append(_remote(src, dst, pair_send.at[t], pair_recv.at[t], _device(at, k=ONE - at["k"])))
        copy = pltpu.make_async_copy(src, dst, own_sem.at[t])
        copy.start()
        own.append(copy)

    for by in range(1, 8):
        copies[by - 1].wait_recv()
    for t in range(3):
        rows = jnp.concatenate([in_s[j, t].astype(F32)[ZERO:SIX, :] for j in range(MATES)], axis=ZERO).astype(BF)
        for c in range(3):
            ws[t, at["x"], at["y"], c, :, _lanes(at["z"])] = rows[ROWS * c : ROWS * c + ROWS, :]
    every = (MIXED, GATE, UP, DOWN)
    for phase in (0, 1):
        each(send_own, phase, every)
        each(pass_on, phase, every)
        each(finish, phase, every)
    each(send_own, 2, every[:2])
    for n, t in enumerate(every):
        each(pass_on, 2, [t])
        if n + 2 < 4:
            each(send_own, 2, [every[n + 2]])
        if n >= 1:
            each(finish, 2, [every[n - 1]])
            to_result(every[n - 1])
    each(finish, 2, [every[3]])
    to_result(every[3])
    for n, copy in enumerate(copies):
        copy.wait_send()
    for t in every:
        src = wds if t == DOWN else ws.at[t]
        dst = down_o.at[:, :, :, ONE - at["k"]] if t == DOWN else outs[t].at[:, :, :, :, pl.ds(pl.multiple_of((ONE - at["k"]) * HALF, HALF), HALF)]
        pltpu.make_async_copy(dst, dst, pair_recv.at[t]).wait()
    for copy in own:
        copy.wait()


def gather(wq, wk, wv, wo, w_gate, w_up, w_down):
    vmem, anywhere = pl.BlockSpec(memory_space=pltpu.VMEM), pl.BlockSpec(memory_space=pl.ANY)
    wide = jax.ShapeDtypeStruct((*GRID, 3, ROWS, FULL), BF)
    mixed, gate, up, down = pl.pallas_call(
        _gather_kernel,
        in_specs=[vmem] * 7,
        out_specs=[anywhere] * 4,
        out_shape=[wide, wide, wide, jax.ShapeDtypeStruct((*GRID, PLACES, 2, ROWS, DIM), BF)],
        scratch_shapes=[
            pltpu.VMEM((MATES, 3, MATES, WIDE), BF),
            pltpu.VMEM((MATES, 3, MATES, WIDE), BF),
            pltpu.VMEM((3, *GRID, 3, ROWS, HALF), BF),
            pltpu.VMEM((*GRID, PLACES, ROWS, DIM), BF),
            pltpu.SemaphoreType.DMA((2, 8)),
            pltpu.SemaphoreType.DMA((PLACES, 3, 3, PLACES)),
            pltpu.SemaphoreType.DMA((PLACES, 3, 3, PLACES)),
            pltpu.SemaphoreType.DMA((PLACES,)),
            pltpu.SemaphoreType.DMA((PLACES,)),
            pltpu.SemaphoreType.DMA((PLACES,)),
        ],
        compiler_params=pltpu.CompilerParams(collective_id=0, has_side_effects=True, vmem_limit_bytes=VMEM),
        name="gather_weights",
    )(wq, wk, wv, wo, w_gate, w_up, w_down)
    return mixed.reshape(DIM, FULL), gate.reshape(DIM, FULL), up.reshape(DIM, FULL), down.reshape(FULL, DIM)


def _scatter_kernel(qkv, wo, gate, up, down, rows_o, down_o, own, theirs, own_d, theirs_d,
                    to1, in1, over1, last1, acc1, to2, in2, over2, last2, acc2, to3, in3, over3, last3, out_s, in_s,
                    own_sems, pair_sems, ring_send, ring_recv, mate_sems):
    at = _place()
    seat = at["z"] * 2 + at["k"]
    given = (None, gate, up)
    _greet(at)
    partner = _device(at, k=ONE - at["k"])
    copies = []

    def part(t, k):
        return down.at[:, :, :, k] if t == DOWN else given[t].at[:, :, :, :, pl.ds(pl.multiple_of(k * HALF, HALF), HALF)]

    def share(t, give, keep):
        copy = pltpu.make_async_copy(keep, own_d if t == DOWN else own.at[t], own_sems.at[t])
        copy.start()
        return _remote(give, theirs_d if t == DOWN else theirs.at[t], pair_sems.at[ZERO, t], pair_sems.at[ONE, t], partner), copy

    for k, (give, keep) in enumerate(((wo, qkv), (qkv, wo))):
        pl.when(at["k"] == k)(lambda give=give, keep=keep: share(MIXED, give, keep) and None)
    for t in (GATE, UP, DOWN):
        share(t, part(t, ONE - at["k"]), part(t, at["k"]))

    def shared(t):
        mine, other = (own_d, theirs_d) if t == DOWN else (own.at[t], theirs.at[t])
        pltpu.make_async_copy(other, other, pair_sems.at[ONE, t]).wait()
        pltpu.make_async_copy(mine, mine, own_sems.at[t]).wait()

    def cell(t, c, place):
        x, y, z = (place[a] for a in "xyz")
        if t == DOWN:
            both = (ref[x, y, z, :, WIDE * c : WIDE * c + WIDE] for ref in (own_d, theirs_d))
        else:
            both = (ref[t, x, y, c, :, _lanes(z)] for ref in (own, theirs))
        return sum(b.astype(F32) for b in both)

    bufs = {0: (to1, in1, over1, last1), 1: (to2, in2, over2, last2), 2: (to3, in3, over3, last3)}

    def term(t, c, phase, q, i, j):
        if phase == 0:
            return cell(t, c, dict(zip(ORDERS[c], (q, i, j), strict=ONE)))
        return acc1[t, c, q, j] if phase == 1 else acc2[t, c, q]

    def over_cells(phase, act):
        if phase == 0:
            def row(i, _):
                for j in range(PLACES):
                    act(i, j, (i, j))
            lax.fori_loop(0, 4, row, None)
        elif phase == 1:
            for j in range(PLACES):
                act(0, j, (j,))
        else:
            act(0, 0, ())

    def send(t, c, phase, slot, src, dst):
        axis = ORDERS[c][phase]
        copies.append(_remote(src, dst, ring_send.at[t, c, phase, slot], ring_recv.at[t, c, phase, slot], _beside(at, axis, 1 if slot % 2 == 0 else 3)))

    def landed(ref, t, c, phase, slot):
        pltpu.make_async_copy(ref, ref, ring_recv.at[t, c, phase, slot]).wait()

    def begin(t, c, phase):
        to, into, _, _ = bufs[phase]
        p = at[ORDERS[c][phase]]
        up1, far, down1 = (p + ONE) % RING, (p + 2) % RING, (p + 3) % RING

        def act(i, j, where):
            above, opposite, below = (term(t, c, phase, q, i, j) for q in (up1, far, down1))
            to[(t, c, ZERO, *where)] = jnp.concatenate([above[:, :HEAD], opposite[:, HEAD:]], axis=ONE).astype(BF)
            to[(t, c, ONE, *where)] = jnp.concatenate([opposite[:, :HEAD], below[:, HEAD:]], axis=ONE).astype(BF)

        over_cells(phase, act)
        for slot in (0, 1):
            send(t, c, phase, slot, to.at[t, c, slot], into.at[t, c, slot])

    def relay(t, c, phase):
        _, into, over, last = bufs[phase]
        p = at[ORDERS[c][phase]]
        up1, down1 = (p + ONE) % RING, (p + 3) % RING
        landed(into.at[t, c, ZERO], t, c, phase, 0)

        def act0(i, j, where):
            over[(t, c, ZERO, *where)] = (term(t, c, phase, up1, i, j)[:, HEAD:] + into[(t, c, ZERO, *where)][:, HEAD:].astype(F32)).astype(BF)

        over_cells(phase, act0)
        send(t, c, phase, 2, over.at[t, c, ZERO], last.at[t, c, ZERO])
        landed(into.at[t, c, ONE], t, c, phase, 1)

        def act1(i, j, where):
            over[(t, c, ONE, *where)] = (term(t, c, phase, down1, i, j)[:, :HEAD] + into[(t, c, ONE, *where)][:, :HEAD].astype(F32)).astype(BF)

        over_cells(phase, act1)
        send(t, c, phase, 3, over.at[t, c, ONE], last.at[t, c, ONE])

    def finish(t, c, phase):
        _, into, _, last = bufs[phase]
        p = at[ORDERS[c][phase]]
        for slot in (0, 1):
            landed(last.at[t, c, slot], t, c, phase, 2 + slot)

        def act(i, j, where):
            mine = term(t, c, phase, p, i, j)
            a = mine[:, :HEAD] + into[(t, c, ZERO, *where)][:, :HEAD].astype(F32) + last[(t, c, ONE, *where)].astype(F32)
            b = mine[:, HEAD:] + into[(t, c, ONE, *where)][:, HEAD:].astype(F32) + last[(t, c, ZERO, *where)].astype(F32)
            total = jnp.concatenate([a, b], axis=ONE)
            if phase == 0:
                acc1[(t, c, *where)] = total
            elif phase == 1:
                acc2[(t, c, *where)] = total
            else:
                done(t, c, total)

        over_cells(phase, act)

    whole = {}

    def done(t, c, total):
        if t == DOWN:
            down_o[:, WIDE * c : WIDE * c + WIDE] = total.astype(BF)
        else:
            whole[t, c] = total

    def stage(t, n):
        for c in range(3):
            phase, what = divmod(n, 2)
            if what == 0:
                if phase == 0:
                    if c == 0:
                        shared(t)
                else:
                    finish(t, c, phase - 1)
                if phase < 3:
                    begin(t, c, phase)
            else:
                relay(t, c, phase)

    for n in range(7 + 3):
        for t in range(PLACES):
            if 0 <= n - t < 7:
                stage(t, n - t)

    for t in range(3):
        rows = jnp.concatenate([whole[t, c] for c in range(3)], axis=ZERO)
        for j in range(MATES):
            out_s[j, t, ZERO:SIX, :] = rows[6 * j : 6 * j + 6, :].astype(BF)
            out_s[j, t, SIX:MATES, :] = jnp.zeros((2, WIDE), BF)
    mates = [_remote(out_s.at[(seat + by) % 8], in_s.at[seat], mate_sems.at[ZERO, by], mate_sems.at[ONE, by], _mate(at, by)) for by in range(1, 8)]
    in_s[seat] = out_s[seat]
    for copy in mates:
        copy.wait_recv()
    rows_o[...] = in_s[...]
    for copy in (*copies, *mates):
        copy.wait_send()
    for t in range(PLACES):
        gone = theirs_d if t == DOWN else theirs.at[t]
        pltpu.make_async_copy(gone, gone, pair_sems.at[ZERO, t]).wait()


def _deal(rows_ref, down_ref, wq_o, wk_o, wv_o, wo_o, wg_o, wu_o, wd_o):
    for j in range(MATES):
        first = (j % 2) * HALF + (j // 2) * WIDE
        for lo in (0, HEAD):
            for ref, base in ((wq_o, 0), (wk_o, DIM), (wv_o, 896), (wo_o, HALF)):
                at = first + lo - base
                if 0 <= at < ref.shape[1]:
                    ref[:, at : at + HEAD] = rows_ref[j, MIXED, ZERO:SIX, lo : lo + HEAD]
        wg_o[:, first : first + WIDE] = rows_ref[j, GATE, ZERO:SIX, :]
        wu_o[:, first : first + WIDE] = rows_ref[j, UP, ZERO:SIX, :]
    wd_o[...] = down_ref[...]


def deal(rows, down):
    outs = ((6, DIM), (6, HEAD), (6, HEAD), (6, DIM), (6, FULL), (6, FULL), (ROWS, DIM))
    return _call(_deal, "deal", 1, [(a, *_all(*a.shape)) for a in (rows, down)], [(shape, BF, *_all(*shape)) for shape in outs])


def scatter(qkv, wo, gate, up, down):
    vmem, anywhere = pl.BlockSpec(memory_space=pltpu.VMEM), pl.BlockSpec(memory_space=pl.ANY)
    scratch = [pltpu.VMEM((3, *GRID, 3, ROWS, HALF), BF), pltpu.VMEM((3, *GRID, 3, ROWS, HALF), BF),
               pltpu.VMEM((*GRID, PLACES, ROWS, DIM), BF), pltpu.VMEM((*GRID, PLACES, ROWS, DIM), BF)]
    for left in ((4, 4), (4,), ()):
        scratch += [pltpu.VMEM((4, 3, 2, *left, ROWS, WIDE), BF)] * 2 + [pltpu.VMEM((4, 3, 2, *left, ROWS, HEAD), BF)] * 2
        if left:
            scratch += [pltpu.VMEM((4, 3, *left, ROWS, WIDE), F32)]
    scratch += [pltpu.VMEM((MATES, 3, MATES, WIDE), BF)] * 2
    scratch += [pltpu.SemaphoreType.DMA((PLACES,)), pltpu.SemaphoreType.DMA((2, 4)), pltpu.SemaphoreType.DMA((PLACES, 3, 3, PLACES)),
                pltpu.SemaphoreType.DMA((PLACES, 3, 3, PLACES)), pltpu.SemaphoreType.DMA((2, 8))]
    rows, down = pl.pallas_call(
        _scatter_kernel,
        in_specs=[anywhere] * 5,
        out_specs=[vmem] * 2,
        out_shape=[jax.ShapeDtypeStruct((MATES, 3, MATES, WIDE), BF), jax.ShapeDtypeStruct((ROWS, DIM), BF)],
        scratch_shapes=scratch,
        compiler_params=pltpu.CompilerParams(collective_id=1, has_side_effects=True, vmem_limit_bytes=VMEM),
        name="scatter_gradients",
    )(*(a.reshape(*GRID, 3, ROWS, -ONE) for a in (qkv, wo, gate, up)), down.reshape(*GRID, PLACES, 2, ROWS, DIM))
    return deal(rows, down)


def solution(mesh):
    def step(x, dy, *weights):
        mixed, gate, up, down = gather(*(w[0] for w in weights))
        by_h, *by_w = through(x[0], dy[0], mixed, gate, up, down)
        return (by_h[None], *(g[None] for g in scatter(*by_w)))

    states, cut = P(("rep", "dp"), None, None), P(None, "dp", None)
    return jax.shard_map(
        step,
        mesh=mesh,
        in_specs=(states, states) + (cut,) * 7,
        out_specs=(states,) + (P("rep", "dp", None),) * 7,
        check_vma=False,
    )
```

```python
import jax
import jax.numpy as jnp
import numpy as np
from jax import lax
from jax.experimental import pallas as pl
from jax.experimental.pallas import tpu as pltpu
from jax.sharding import PartitionSpec as P

HEAD = 128
THETA = 10000
EPS = 1e-6
ZERO, ONE, HALF, FULL, DIM, WIDE, ROWS, MATES, PLACES, SIX, TWO, THREE, COLOURS = 0, 1, 1024, 2048, 768, 256, 16, 8, 4, 6, 2, 3, 3
GRID = (PLACES, PLACES)
NEG = -1e30
HIDDEN = 2 * NEG
LOG2E = 1.4426950408889634
VMEM = 56 * 2**20
BLOCK = 512
BF, F32 = jnp.bfloat16, jnp.float32
SCALE = HEAD**-0.5
E = SCALE * LOG2E


def _dot(a, b, ca, cb):
    return lax.dot_general(a, b, (((ca,), (cb,)), ((), ())), preferred_element_type=F32)


def _mm(a, b):
    return _dot(a, b, ONE, ZERO)


def _mt(a, b):
    return _dot(a, b, ONE, ONE)


def _first():
    return pl.program_id(ZERO) == ZERO


def _last():
    return pl.program_id(ZERO) == pl.num_programs(ZERO) - ONE


def _visible():
    return lax.broadcasted_iota(jnp.int32, (BLOCK, BLOCK), 0) <= lax.broadcasted_iota(jnp.int32, (BLOCK, BLOCK), 1)


TOKENS_STEP = 512


def _call(kernel, name, grid, ins, outs, scratch=(), flops=0):
    given = [a for a, _, _ in ins]
    moved = sum(a.size * a.dtype.itemsize for a in given)
    return pl.pallas_call(
        kernel,
        grid=(grid,),
        in_specs=[pl.BlockSpec(block, index) for _, block, index in ins],
        out_specs=[pl.BlockSpec(block, index) for _, _, block, index in outs],
        out_shape=[jax.ShapeDtypeStruct(shape, dtype) for shape, dtype, _, _ in outs],
        scratch_shapes=list(scratch),
        compiler_params=pltpu.CompilerParams(dimension_semantics=("arbitrary",), vmem_limit_bytes=VMEM),
        cost_estimate=pl.CostEstimate(flops=flops, transcendentals=0, bytes_accessed=2 * moved),
        name=name,
    )(*given)


def _rows(*shape):
    return shape, lambda i: (i,) + (0,) * (len(shape) - 1)


def _second(*shape):
    return shape, lambda i: (0, i) + (0,) * (len(shape) - 2)


def _all(*shape):
    return shape, lambda i: (0,) * len(shape)


def _norm(h):
    wide = h.astype(F32)
    return (wide * lax.rsqrt(jnp.mean(wide * wide, -1, keepdims=ONE) + EPS)).astype(BF)


def _norm_back(h, g):
    wide, g = h.astype(F32), g.astype(F32)
    scale = lax.rsqrt(jnp.mean(wide * wide, -1, keepdims=ONE) + EPS)
    return scale * (g - wide * (scale * scale * jnp.mean(g * wide, -1, keepdims=ONE)))


def _close(o_ref, x_ref, wo_ref, h_ref, b_ref, bt_ref):
    o = jnp.concatenate([o_ref[n] for n in range(o_ref.shape[ZERO])], axis=ONE)
    h = x_ref[...] + _mm(o, wo_ref[...])[:, : x_ref.shape[ONE]].astype(BF)
    h_ref[...] = h
    b = _norm(h)
    b_ref[...] = b
    bt_ref[...] = b.T


def close(o, x, wo):
    n, d = x.shape
    s, heads = TOKENS_STEP, o.shape[ZERO]
    return _call(_close, "close", n // s, [(o, *_second(heads, s, HEAD)), (x, *_rows(s, d)), (wo, *_all(d, HALF))],
                 [((n, d), BF, *_rows(s, d)), ((n, d), BF, *_rows(s, d)), ((d, n), BF, *_second(d, s))], flops=2 * n * d * d)


def _feed(b_ref, bt_ref, dy_ref, dyt_ref, wg_ref, wu_ref, wd_ref, db_ref, dwg_ref, dwu_ref, dwd_ref, db_s, z_s):
    f = wg_ref.shape[ONE]
    n = b_ref.shape[ZERO]
    s = TOKENS_STEP

    @pl.when(_first())
    def _():
        db_s[...] = jnp.zeros_like(db_s)

    both = jnp.concatenate([wg_ref[...], wu_ref[...]], axis=ONE)
    for lo in range(0, n, s):
        here = slice(lo, lo + s)
        gate_up = _mm(b_ref[here, :], both)
        gate, up = gate_up[:, :f], gate_up[:, f:]
        dmid = _mt(dy_ref[here, :], wd_ref[...]).astype(BF).astype(F32)
        sig = 1 / (1 + jnp.exp2(gate * -LOG2E))
        silu = gate * sig
        z_s[here, 2 * f :] = (silu * up).astype(BF)
        dup = (dmid * silu).astype(BF)
        dgate = (dmid * up * (sig + silu * (1 - sig))).astype(BF)
        z_s[here, :f] = dgate
        z_s[here, f : 2 * f] = dup
        db_s[here, :] += _mt(jnp.concatenate([dgate, dup], axis=ONE), both)
    dw = _mm(bt_ref[...], z_s[:, : 2 * f])
    dwg_ref[...] = dw[:, :f].astype(BF)
    dwu_ref[...] = dw[:, f:].astype(BF)
    dwd_ref[...] = _mm(dyt_ref[...], z_s[:, 2 * f :]).astype(BF).T

    @pl.when(_last())
    def _():
        db_ref[...] = db_s[...].astype(BF)


FEED_STEP = 256


def feed(b, bt, dy, dyt, gate, up, down):
    n, d = b.shape
    f, ff = FEED_STEP, gate.shape[ONE]
    cols, rows = ((d, f), lambda i: (0, i)), ((f, d), lambda i: (i, 0))
    return _call(_feed, "feed", ff // f,
                 [(b, *_all(n, d)), (bt, *_all(d, n)), (dy, *_all(n, d)), (dyt, *_all(d, n)), (gate, *cols), (up, *cols), (down, *rows)],
                 [((n, d), BF, *_all(n, d)), ((d, ff), BF, *cols), ((d, ff), BF, *cols), ((ff, d), BF, *rows)],
                 [pltpu.VMEM((n, d), F32), pltpu.VMEM((n, 3 * f), BF)], flops=ROWS * n * d * ff)


def _open_back(db_ref, h_ref, dy_ref, o_ref, wo_ref, dh_ref, do_ref, delta_ref, dwo_ref, acc_s):
    i = pl.program_id(0)

    @pl.when(_first())
    def _():
        acc_s[...] = jnp.zeros_like(acc_s)

    heads = o_ref.shape[ZERO]
    d = dy_ref.shape[ONE]
    dh = (dy_ref[...].astype(F32) + _norm_back(h_ref[...], db_ref[...])).astype(BF)
    dh_ref[...] = dh
    do = _mt(dh, wo_ref[:, :d]).astype(BF)
    for n in range(heads):
        mine = do[:, n * HEAD : (n + ONE) * HEAD]
        do_ref[n] = mine
        delta_ref[n : n + ONE, :] = (mine.astype(F32) * o_ref[n].astype(F32)).T.sum(axis=ZERO, keepdims=ONE)
        acc_s[n * HEAD : (n + ONE) * HEAD, :] += _dot(o_ref[n], dh, 0, 0)

    @pl.when(_last())
    def _():
        dwo_ref[:, :d] = acc_s[...].astype(BF)
        dwo_ref[:, d:] = jnp.zeros_like(dwo_ref[:, d:])


def open_back(db, h, dy, o, wo):
    n, d = h.shape
    s, heads = TOKENS_STEP, o.shape[ZERO]
    rows = _rows(s, d)
    return _call(_open_back, "open_back", n // s,
                 [(db, *rows), (h, *rows), (dy, *rows), (o, *_second(heads, s, HEAD)), (wo, *_all(d, HALF))],
                 [((n, d), BF, *rows), ((heads, n, HEAD), BF, *_second(heads, s, HEAD)), ((heads, n), F32, *_second(heads, s)),
                  ((d, HALF), BF, *_all(d, HALF))], [pltpu.VMEM((d, d), F32)], flops=4 * n * d * d)


RING = 4
ORDERS = ("xyz", "yzx", "zxy")
MIXED, GATE, UP, DOWN = range(PLACES)


def _place():
    me = lax.axis_index("dp")
    return {"x": me // 32, "y": me // 8 % RING, "z": me // TWO % RING, "k": me % TWO}


def _device(at, **other):
    at = {**at, **other}
    return {"dp": ((at["x"] * 4 + at["y"]) * 4 + at["z"]) * TWO + at["k"]}


def _beside(at, axis, by):
    return _device(at, **{axis: (at[axis] + by) % RING})


def _mate(at, by):
    other = (at["z"] * TWO + at["k"] + by) % 8
    return _device(at, z=other // TWO, k=other % TWO)


def _greet(at):
    barrier = pltpu.get_barrier_semaphore()
    peers = [_beside(at, axis, by) for axis in "xy" for by in (ONE, THREE)] + [_mate(at, by) for by in range(ONE, MATES)]
    for peer in peers:
        pl.semaphore_signal(barrier, inc=1, device_id=peer, device_id_type=pl.DeviceIdType.MESH)
    pl.semaphore_wait(barrier, len(peers))


def _remote(src, dst, send, recv, device):
    pltpu.make_async_remote_copy(src_ref=src, dst_ref=dst, send_sem=send, recv_sem=recv, device_id=device,
                                 device_id_type=pl.DeviceIdType.MESH).start()


def _start(src, dst, sem):
    pltpu.make_async_copy(src, dst, sem).start()


def _arrived(ref, sem):
    pltpu.make_async_copy(ref, ref, sem).wait()


def _lanes(z, lo=0, n=WIDE):
    return pl.ds(pl.multiple_of(z * WIDE + lo, HEAD), n)


def _half_columns(k):
    return pl.ds(pl.multiple_of(k * HALF, HALF), HALF)


def _tokens(i):
    return pl.ds(i * BLOCK if isinstance(i, int) else pl.multiple_of(i * BLOCK, BLOCK), BLOCK)


def _columns(j):
    return (j % TWO) * HALF + (j // TWO) * WIDE


STARTS = (0, DIM, 896, HALF)


def _from_mixed(refs, lo):
    return next(((ref, lo - base) for ref, base in zip(refs, STARTS, strict=ONE) if 0 <= lo - base < ref.shape[ONE]), None)


def _advance(wq, wk, wv, wo, wg, wu, wd, freq, x, dy, qkv_o, wo_o, gate_o, up_o, down_o, at_o, dyt_o, q_o, k_o, v_o, o_o, cos_o, sin_o, lse_o,
             out_s, in_s, ws, wds, mixed_s, x_s, dy_s, a_s, at_s, dyt_s, q_s, k_s, v_s, o_s, top_s, mix_s, cos_s, sin_s,
             mate_sems, ring_send, ring_recv, pair_sems, own_sem, load_sems, store_sems):
    at = _place()
    seat = at["z"] * TWO + at["k"]
    outs = (None, gate_o, up_o)
    heads = q_s.shape[ZERO]
    blocks = x_s.shape[ZERO] // BLOCK
    sent = {}
    kept = []

    def send(key, ref, dst, sem, recv, device):
        _remote(ref(), dst(), sem(), recv, device)
        sent[key] = ref, sem

    def store(src, dst, n):
        _start(src, dst, store_sems.at[n])
        kept.append((src, store_sems.at[n]))

    _start(x, x_s, load_sems.at[ZERO])
    _start(dy, dy_s, load_sems.at[ONE])
    for j in range(MATES):
        for lo in (0, HEAD):
            found = _from_mixed((wq, wk, wv, wo), _columns(j) + lo)
            if found:
                ref, first = found
                out_s[j, MIXED, ZERO:SIX, lo : lo + HEAD] = ref[:, first : first + HEAD]
            else:
                out_s[j, MIXED, ZERO:SIX, lo : lo + HEAD] = jnp.zeros((6, HEAD), BF)
        for t, ref in ((GATE, wg), (UP, wu)):
            out_s[j, t, ZERO:SIX, :] = ref[:, _columns(j) : _columns(j) + WIDE]
        out_s[j, :, SIX:MATES, :] = jnp.zeros((3, 2, WIDE), BF)
    _greet(at)
    for by in range(ONE, MATES):
        send(by, lambda by=by: out_s.at[(seat + by) % 8], lambda: in_s.at[seat], lambda by=by: mate_sems.at[ZERO, by], mate_sems.at[ONE, by],
             _mate(at, by))
    in_s[seat] = out_s[seat]
    for c in range(COLOURS):
        wds[at["x"], at["y"], at["z"], :, WIDE * c : WIDE * c + WIDE] = wd[:, WIDE * c : WIDE * c + WIDE]

    def region(t, c, fixed, half=None):
        x, y = (fixed.get(axis, slice(None)) for axis in "xy")
        if t != DOWN and "z" not in fixed:
            return ws.at[t, x, y, c, :, slice(None) if half is None else slice(512 * half, 512 * half + 512)]
        lo, n = (0, WIDE) if half is None else (HEAD * half, HEAD)
        if t == DOWN:
            return wds.at[x, y, fixed.get("z", slice(None)), :, WIDE * c + lo : WIDE * c + lo + n]
        return ws.at[t, x, y, c, :, _lanes(fixed["z"], lo, n)]

    def known(c, phase, place):
        order = ORDERS[c][::-1]
        return {**{a: at[a] for a in order[phase + 1 :]}, order[phase]: place}

    def hop(t, c, phase, slot, here):
        axis = ORDERS[c][::-1][phase]
        key = t, c, phase, slot
        send(key, here, here, lambda: ring_send.at[key], ring_recv.at[key], _beside(at, axis, ONE if slot % TWO == ZERO else THREE))

    def send_own(phase, *ts):
        for t in ts:
            for c in range(COLOURS):
                for slot in (ZERO, ONE):
                    hop(t, c, phase, slot, lambda t=t, c=c: region(t, c, known(c, phase, at[ORDERS[c][::-1][phase]])))

    def pass_on(phase, *ts):
        for t in ts:
            for c in range(COLOURS):
                axis = ORDERS[c][::-1][phase]
                for slot, by in ((0, 3), (1, 1)):

                    def here(half, t=t, c=c, axis=axis, by=by):
                        return region(t, c, known(c, phase, (at[axis] + by) % RING), half)

                    _arrived(here(None), ring_recv.at[t, c, phase, slot])
                    hop(t, c, phase, 2 + slot, lambda here=here, slot=slot: here(1 - slot))

    def finish(phase, *ts):
        for t in ts:
            for c in range(COLOURS):
                fixed = known(c, phase, (at[ORDERS[c][::-1][phase]] + 2) % RING)
                for slot in (ZERO, ONE):
                    _arrived(region(t, c, fixed, 1 - slot), ring_recv.at[t, c, phase, 2 + slot])

    partner = _device(at, k=ONE - at["k"])

    def half(t, k):
        return down_o.at[:, :, :, k] if t == DOWN else outs[t].at[:, :, :, :, _half_columns(k)]

    def to_result(t):
        src = wds if t == DOWN else ws.at[t]
        _remote(src, half(t, at["k"]), pair_sems.at[ZERO, t], pair_sems.at[ONE, t], partner)
        _start(src, half(t, at["k"]), own_sem.at[t])

    def prepare(i):
        here = slice(i * BLOCK, i * BLOCK + BLOCK)
        a = _norm(x_s[here, :])
        a_s[here, :] = a
        at_s[:, here] = a.T

    def turn(i):
        here = slice(i * BLOCK, i * BLOCK + BLOCK)
        dyt_s[:, here] = dy_s[here, :].T

    def tables():
        half, rows = HEAD // TWO, 64
        place = lax.broadcasted_iota(jnp.int32, (rows, HEAD), 0).astype(F32)
        left = lax.broadcasted_iota(jnp.int32, (rows, HEAD), 1) < half
        near, far = place * freq[...], place[: x_s.shape[ZERO] // rows] * rows * freq[: x_s.shape[ZERO] // rows]
        near_cos, near_sin, far_cos, far_sin = jnp.cos(near), jnp.sin(near), jnp.cos(far), jnp.sin(far)
        for n in range(x_s.shape[ZERO] // rows):
            c, s = far_cos[n : n + ONE, :], far_sin[n : n + ONE, :]
            cos_s[n * rows : n * rows + rows, :] = near_cos * c - near_sin * s
            sin = near_sin * c + near_cos * s
            sin_s[n * rows : n * rows + rows, :] = jnp.where(left, -sin, sin)
        store(cos_s, cos_o, 6)
        store(sin_s, sin_o, 7)

    def project(i):
        here = slice(i * BLOCK, i * BLOCK + BLOCK)
        t = _mm(a_s[here, :], mixed_s[...].reshape(a_s.shape[ONE], -1)).astype(BF)
        cos, sin = cos_s[here, :], sin_s[here, :]
        for n in range(heads + ONE):
            one = t[:, n * HEAD : (n + ONE) * HEAD].astype(F32)
            one = (one * cos + pltpu.roll(one, HEAD // TWO, 1) * sin).astype(BF)
            if n < heads:
                q_s[n, here, :] = one
            else:
                k_s[here, :] = one
        v_s[here, :] = t[:, (heads + ONE) * HEAD :]

    rest = (GATE, UP, DOWN)
    _arrived(x_s, load_sems.at[ZERO])
    prepare(0)
    for by in range(ONE, MATES):
        _arrived(in_s.at[ZERO], mate_sems.at[ONE, by])
    for t in range(COLOURS):
        rows = jnp.concatenate([in_s[j, t].astype(F32)[ZERO:SIX, :] for j in range(MATES)], axis=ZERO).astype(BF)
        for c in range(COLOURS):
            ws[t, at["x"], at["y"], c, :, _lanes(at["z"])] = rows[ROWS * c : ROWS * c + ROWS, :]
    send_own(0, MIXED)
    send_own(0, *rest)
    prepare(1)
    pass_on(0, MIXED)
    pass_on(0, *rest)
    prepare(2)
    finish(0, MIXED)
    send_own(1, MIXED)
    finish(0, *rest)
    send_own(1, *rest)
    prepare(3)
    store(at_s, at_o, 0)
    pass_on(1, MIXED)
    pass_on(1, *rest)
    tables()
    finish(1, MIXED)
    send_own(2, MIXED)
    finish(1, *rest)
    send_own(2, GATE)
    _arrived(dy_s, load_sems.at[ONE])
    turn(0)
    turn(1)
    pass_on(2, MIXED)
    send_own(2, UP)
    turn(2)
    turn(3)
    store(dyt_s, dyt_o, 1)
    finish(2, MIXED)

    @pl.when(at["k"] == ZERO)
    def _():
        _remote(ws.at[MIXED], mixed_s, pair_sems.at[ZERO, MIXED], pair_sems.at[ONE, MIXED], partner)
        mixed_s[...] = ws[MIXED]

    @pl.when(at["k"] == ONE)
    def _():
        _remote(ws.at[MIXED], wo_o, pair_sems.at[ZERO, MIXED], pair_sems.at[ONE, MIXED], partner)
        _start(ws.at[MIXED], wo_o, own_sem.at[MIXED])

    pass_on(2, GATE)
    send_own(2, DOWN)
    _arrived(mixed_s, pair_sems.at[ONE, MIXED])
    store(mixed_s, qkv_o, 2)
    for i in range(blocks):
        project(i)
        if i == 1:
            pass_on(2, UP)
    store(q_s, q_o, 3)
    store(k_s, k_o, 4)
    store(v_s, v_o, 5)

    def between(n):
        @pl.when(n == 0)
        def _():
            finish(2, GATE)
            to_result(GATE)

        @pl.when(n == 1)
        def _():
            pass_on(2, DOWN)

        @pl.when(n == 2)
        def _():
            finish(2, UP)
            to_result(UP)

        @pl.when(n == 3)
        def _():
            finish(2, DOWN)
            to_result(DOWN)

    ones = jnp.ones((8, BLOCK), BF)

    def block(iq, j, masked):
        here = _tokens(j)
        mine = _tokens(iq)
        scores = [_mt(k_s[here, :], q_s[n, mine, :]) for n in range(heads)]
        weights, keeps = [], []
        for n, s in enumerate(scores):
            if masked:
                s = jnp.where(_visible(), s, HIDDEN)
            old = top_s[n : n + ONE, :]
            top = jnp.maximum(old, s.max(axis=ZERO, keepdims=ONE))
            top_s[n : n + ONE, :] = top
            weights.append(jnp.exp2((s - top) * E).astype(BF))
            keeps.append(jnp.exp2((old - top) * E))
        values = jnp.concatenate([v_s[here, :].T, ones], axis=ZERO)
        for n, (p, keep) in enumerate(zip(weights, keeps, strict=ONE)):
            mix_s[n] = mix_s[n] * keep + _mm(values, p)

    def row(iq, _):
        top_s[...] = jnp.full(top_s.shape, NEG, F32)
        mix_s[...] = jnp.zeros(mix_s.shape, F32)

        def step(j, _):
            block(iq, j, False)
            between(iq * (iq + ONE) // TWO + j)

        lax.fori_loop(0, iq, step, None)
        block(iq, iq, True)
        between(iq * (iq + ONE) // TWO + iq)
        mine = _tokens(iq)
        for n in range(heads):
            total = mix_s[n, HEAD : HEAD + 1, :]
            o_s[n, mine, :] = (mix_s[n, :HEAD, :] * (1 / total)).T.astype(BF)
            lse_o[n : n + ONE, mine] = top_s[n : n + ONE, :] * SCALE + jnp.log(total)
        _start(o_s.at[:, mine], o_o.at[:, mine], own_sem.at[4])

    lax.fori_loop(0, blocks, row, None)
    _arrived(o_s, own_sem.at[4])
    for ref, sem in sent.values():
        _arrived(ref(), sem())
    for t in (MIXED, *rest):
        src = wds if t == DOWN else ws.at[t]
        _arrived(src, pair_sems.at[ZERO, t])
        if t != MIXED:
            _arrived(src, pair_sems.at[ONE, t])
            _arrived(src, own_sem.at[t])

    @pl.when(at["k"] == ONE)
    def _():
        _arrived(ws.at[MIXED], own_sem.at[MIXED])

    for ref, sem in kept:
        _arrived(ref, sem)


def advance(x, dy, *shards):
    n, d = x.shape
    heads = d // HEAD
    half = HEAD // TWO
    freq = np.tile(float(THETA) ** (-np.arange(half) / half), (half, 2)).astype(np.float32)
    vmem, anywhere = pl.BlockSpec(memory_space=pltpu.VMEM), pl.BlockSpec(memory_space=pl.ANY)
    wide, narrow = (*GRID, COLOURS, ROWS, FULL), (*GRID, COLOURS, ROWS, HALF)
    tall = (*GRID, PLACES, 2, ROWS, DIM)
    many, one = (heads, n, HEAD), (n, HEAD)
    shapes = (narrow, narrow, wide, wide, tall, (d, n), (d, n), many, one, one, many)
    dma = pltpu.SemaphoreType.DMA
    qkv, wo, gate, up, down, *rest = pl.pallas_call(
        _advance,
        in_specs=[vmem] * 8 + [anywhere] * 2,
        out_specs=[anywhere] * (len(shapes) + 2) + [vmem],
        out_shape=[jax.ShapeDtypeStruct(s, BF) for s in shapes] + [jax.ShapeDtypeStruct(s, F32) for s in (one, one, (heads, n))],
        scratch_shapes=[pltpu.VMEM(s, BF) for s in ((MATES, 3, MATES, WIDE), (MATES, 3, MATES, WIDE), (3, *narrow), (*GRID, PLACES, ROWS, DIM), narrow,
                                                    (n, d), (n, d), (n, d), (d, n), (d, n), many, one, one, many)]
        + [pltpu.VMEM(s, F32) for s in ((heads, BLOCK), (heads, HEAD + 8, BLOCK), one, one)]
        + [dma((2, 8)), dma((PLACES, COLOURS, COLOURS, PLACES)), dma((PLACES, COLOURS, COLOURS, PLACES)), dma((2, 4)), dma((5,)), dma((2,)), dma((8,))],
        compiler_params=pltpu.CompilerParams(collective_id=0, has_side_effects=True, vmem_limit_bytes=VMEM),
        name="advance",
    )(*shards, freq, x, dy)
    return qkv.reshape(d, -1), wo.reshape(d, -1), gate.reshape(d, -1), up.reshape(d, -1), down.reshape(-1, d), *rest


class _Sums:
    STEPS = 7

    def __init__(self, at, ts, own, theirs, bufs, total, down_o, ring_send, ring_recv, pair_sems, own_sems):
        self.at, self.ts, self.own, self.theirs, self.bufs, self.total, self.down_o = at, ts, own, theirs, bufs, total, down_o
        self.ring_send, self.ring_recv, self.pair_sems, self.own_sems = ring_send, ring_recv, pair_sems, own_sems
        self.partner = _device(at, k=ONE - at["k"])

    def give(self, t, ref):
        n = self.ts.index(t)
        _remote(ref, self.theirs[n], self.pair_sems.at[ZERO, n], self.pair_sems.at[ONE, n], self.partner)

    def keep(self, t, ref):
        n = self.ts.index(t)
        _start(ref, self.own[n], self.own_sems.at[n])

    def kept(self, t):
        n = self.ts.index(t)
        _arrived(self.own[n], self.own_sems.at[n])

    def term(self, n, c, phase, q, i, j):
        if phase:
            acc = self.bufs[phase - 1][-1]
            return acc[n, c, q, j] if phase == 1 else acc[n, c, q]
        place = dict(zip(ORDERS[c], (q, i, j), strict=ONE))
        x, y, z = (place[a] for a in "xyz")
        if self.ts[n] == DOWN:
            both = (ref[x, y, z, :, WIDE * c : WIDE * c + WIDE] for ref in (self.own[n], self.theirs[n]))
        else:
            both = (ref[x, y, c, :, _lanes(z)] for ref in (self.own[n], self.theirs[n]))
        return sum(b.astype(F32) for b in both)

    @staticmethod
    def over_cells(phase, act):
        if phase == 0:
            lax.fori_loop(0, 4, lambda i, _: [act(i, j, (i, j)) for j in range(PLACES)] and None, None)
        elif phase == 1:
            for j in range(PLACES):
                act(0, j, (j,))
        else:
            act(0, 0, ())

    def hop(self, n, c, phase, slot, src, dst):
        _remote(src, dst, self.ring_send.at[n, c, phase, slot], self.ring_recv.at[n, c, phase, slot],
                _beside(self.at, ORDERS[c][phase], ONE if slot % TWO == ZERO else THREE))

    def near(self, c, phase, by):
        return (self.at[ORDERS[c][phase]] + by) % RING

    def begin(self, n, c, phase):
        to, into = self.bufs[phase][:2]
        places = [self.near(c, phase, by) for by in (1, 2, 3)]

        def act(i, j, where):
            above, opposite, below = (self.term(n, c, phase, q, i, j) for q in places)
            to[(n, c, 0, *where)] = jnp.concatenate([above[:, :HEAD], opposite[:, HEAD:]], axis=ONE).astype(BF)
            to[(n, c, 1, *where)] = jnp.concatenate([opposite[:, :HEAD], below[:, HEAD:]], axis=ONE).astype(BF)

        self.over_cells(phase, act)
        for slot in (ZERO, ONE):
            self.hop(n, c, phase, slot, to.at[n, c, slot], into.at[n, c, slot])

    def relay(self, n, c, phase):
        into, over, last = self.bufs[phase][1:4]
        for slot, by, half in ((0, 1, slice(HEAD, WIDE)), (1, 3, slice(0, HEAD))):
            _arrived(into.at[n, c, slot], self.ring_recv.at[n, c, phase, slot])
            place = self.near(c, phase, by)

            def act(i, j, where, slot=slot, half=half, place=place):
                mine = self.term(n, c, phase, place, i, j)[:, half]
                over[(n, c, slot, *where)] = (mine + into[(n, c, slot, *where)][:, half].astype(F32)).astype(BF)

            self.over_cells(phase, act)
            self.hop(n, c, phase, 2 + slot, over.at[n, c, slot], last.at[n, c, slot])

    def finish(self, n, c, phase):
        into, _, last = self.bufs[phase][1:4]
        for slot in (ZERO, ONE):
            _arrived(last.at[n, c, slot], self.ring_recv.at[n, c, phase, 2 + slot])

        def act(i, j, where):
            mine = self.term(n, c, phase, self.near(c, phase, 0), i, j)
            a = mine[:, :HEAD] + into[(n, c, 0, *where)][:, :HEAD].astype(F32) + last[(n, c, 1, *where)].astype(F32)
            b = mine[:, HEAD:] + into[(n, c, 1, *where)][:, HEAD:].astype(F32) + last[(n, c, 0, *where)].astype(F32)
            whole = jnp.concatenate([a, b], axis=ONE)
            if phase < 2:
                self.bufs[phase][-1][(n, c, *where)] = whole
            elif self.ts[n] == DOWN:
                self.down_o[:, WIDE * c : WIDE * c + WIDE] = whole.astype(BF)
            else:
                self.total[n, ROWS * c : ROWS * c + ROWS, :] = whole

        self.over_cells(phase, act)

    def step(self, n, what):
        phase, second = divmod(what, 2)
        if what == 0:
            _arrived(self.theirs[n], self.pair_sems.at[ONE, n])
        for c in range(COLOURS):
            if second:
                self.relay(n, c, phase)
            else:
                if phase:
                    self.finish(n, c, phase - 1)
                if phase < 3:
                    self.begin(n, c, phase)

    def steps(self, slot):
        for n in range(len(self.ts)):
            if 0 <= slot - n < self.STEPS:
                self.step(n, slot - n)

    def all_sent(self):
        for n in range(len(self.ts)):
            _arrived(self.theirs[n], self.pair_sems.at[ZERO, n])
            for c in range(COLOURS):
                for phase, (to, _, over, *_) in enumerate(self.bufs):
                    for slot in (ZERO, ONE):
                        _arrived(to.at[n, c, slot], self.ring_send.at[n, c, phase, slot])
                        _arrived(over.at[n, c, slot], self.ring_send.at[n, c, phase, 2 + slot])

    def deal_out(self, wide, out_s, in_s, mate_sems):
        seat = self.at["z"] * TWO + self.at["k"]
        for n in range(wide):
            for j in range(MATES):
                out_s[j, n, ZERO:SIX, :] = self.total[n, 6 * j : 6 * j + 6, :].astype(BF)
                out_s[j, n, SIX:MATES, :] = jnp.zeros((2, WIDE), BF)
        for by in range(ONE, MATES):
            _remote(out_s.at[(seat + by) % 8], in_s.at[seat], mate_sems.at[ZERO, by], mate_sems.at[ONE, by], _mate(self.at, by))
        in_s[seat] = out_s[seat]

    @staticmethod
    def dealt(out_s, in_s, mate_sems):
        for by in range(ONE, MATES):
            _arrived(in_s.at[ZERO], mate_sems.at[ONE, by])
            _arrived(out_s.at[ZERO], mate_sems.at[ZERO, by])


def _sum_scratch(ts):
    count = len(ts)
    scratch = [pltpu.VMEM((*GRID, PLACES, ROWS, DIM) if t == DOWN else (*GRID, COLOURS, ROWS, HALF), BF) for t in ts for _ in range(2)]
    for left in ((4, 4), (4,), ()):
        scratch += [pltpu.VMEM((count, 3, 2, *left, ROWS, WIDE), BF)] * TWO + [pltpu.VMEM((count, 3, 2, *left, ROWS, HEAD), BF)] * 2
        scratch += [pltpu.VMEM((count, 3, *left, ROWS, WIDE), F32)] if left else []
    wide = count - (DOWN in ts)
    dma = pltpu.SemaphoreType.DMA
    return scratch + [pltpu.VMEM((wide, 48, WIDE), F32)] + [pltpu.VMEM((8, wide, 8, WIDE), BF)] * TWO + [
        dma((count, COLOURS, COLOURS, PLACES)), dma((count, COLOURS, COLOURS, PLACES)), dma((2, count)), dma((count,)), dma((2, 8))]


def _sums(at, ts, refs, down_o):
    refs = list(refs)
    pairs = [(refs.pop(0), refs.pop(0)) for _ in ts]
    bufs = [[refs.pop(0) for _ in range(5 - (phase == 2))] for phase in range(COLOURS)]
    total, out_s, in_s, ring_send, ring_recv, pair_sems, own_sems, mate_sems = refs
    sums = _Sums(at, ts, [a for a, _ in pairs], [b for _, b in pairs], bufs, total, down_o, ring_send, ring_recv, pair_sems, own_sems)
    return sums, (out_s, in_s, mate_sems)


LATER = (GATE, UP, DOWN)


def _attend_back(q, k, v, do, lse_ref, delta_ref, gate, up, down, dq_o, dk_o, dv_o, rows_o, down_o,
                 q_s, k_s, v_s, do_s, dq_s, dk_s, dv_s, sum_s, load_sems, out_sem, *refs):
    at = _place()
    heads = q_s.shape[ZERO]
    blocks = q_s.shape[ONE] // BLOCK
    sums, mates = _sums(at, LATER, refs, down_o)
    _start(k, k_s, load_sems.at[ZERO, 0])
    _start(v, v_s, load_sems.at[ONE, 0])
    for i in range(blocks):
        _start(q.at[:, _tokens(i)], q_s.at[:, _tokens(i)], load_sems.at[TWO, i])
        _start(do.at[:, _tokens(i)], do_s.at[:, _tokens(i)], load_sems.at[THREE, i])
    _greet(at)

    def part(t, k):
        return down.at[:, :, :, k] if t == DOWN else (gate, up)[t - GATE].at[:, :, :, :, _half_columns(k)]

    for t in LATER:
        sums.give(t, part(t, ONE - at["k"]))
        sums.keep(t, part(t, at["k"]))
    sum_s[...] = jnp.zeros_like(sum_s)
    dk_s[...] = jnp.zeros_like(dk_s)
    dv_s[...] = jnp.zeros_like(dv_s)
    _arrived(k_s, load_sems.at[ZERO, 0])
    _arrived(v_s, load_sems.at[ONE, 0])

    def between(slot):
        if slot < 3:
            sums.kept(LATER[slot])
        sums.steps(slot)
        if slot == sums.STEPS + 1:
            sums.deal_out(2, *mates)

    def block(iq, j):
        here, mine = _tokens(j), _tokens(iq)

        def some(half, _):
            group = [half * (heads // TWO) + n for n in range(heads // TWO)]
            scores = [_mt(k_s[here, :], q_s[n, mine, :]) for n in group]
            dps = [_mt(v_s[here, :], do_s[n, mine, :]) for n in group]
            for n, s, dp in zip(group, scores, dps, strict=ONE):
                p = jnp.exp2(s * E - lse_ref[pl.ds(n, 1), mine] * LOG2E)
                if iq == j:
                    p = jnp.where(_visible(), p, 0.0)
                ds = (p * (dp - delta_ref[pl.ds(n, 1), mine])).astype(BF)
                dv_s[here, :] += _mm(p.astype(BF), do_s[n, mine, :])
                dk_s[here, :] += _mm(ds, q_s[n, mine, :])
                sum_s[n] += _mm(k_s[here, :].T, ds)

        lax.fori_loop(0, 2, some, None)

    for iq in range(blocks):
        mine = _tokens(iq)
        _arrived(q_s.at[:, mine], load_sems.at[TWO, iq])
        _arrived(do_s.at[:, mine], load_sems.at[THREE, iq])
        for j in range(iq + ONE):
            block(iq, j)
            between(iq * (iq + ONE) // TWO + j)
        for n in range(heads):
            dq_s[n, mine, :] = (sum_s[n] * SCALE).T.astype(BF)
        sum_s[...] = jnp.zeros_like(sum_s)
        _start(dq_s.at[:, mine], dq_o.at[:, mine], out_sem.at[ZERO])

    k_s[...] = (dk_s[...] * SCALE).astype(BF)
    v_s[...] = dv_s[...].astype(BF)
    _start(k_s, dk_o, out_sem.at[ONE])
    _start(v_s, dv_o, out_sem.at[2])
    out_s, in_s, mate_sems = mates
    sums.dealt(out_s, in_s, mate_sems)
    rows_o[...] = in_s[...]
    sums.all_sent()
    _arrived(dq_s, out_sem.at[ZERO])
    _arrived(k_s, out_sem.at[ONE])
    _arrived(v_s, out_sem.at[2])


def attend_back(q, k, v, do, lse, delta, gate, up, down):
    heads, n, _ = q.shape
    vmem, anywhere = pl.BlockSpec(memory_space=pltpu.VMEM), pl.BlockSpec(memory_space=pl.ANY)
    shapes = (q.shape, k.shape, k.shape, (8, 2, 8, WIDE), (ROWS, DIM))
    dma = pltpu.SemaphoreType.DMA
    return pl.pallas_call(
        _attend_back,
        in_specs=[anywhere] * 4 + [vmem] * TWO + [anywhere] * 3,
        out_specs=[anywhere] * 3 + [vmem] * 2,
        out_shape=[jax.ShapeDtypeStruct(s, BF) for s in shapes],
        scratch_shapes=[pltpu.VMEM(s, BF) for s in (q.shape, k.shape, k.shape, q.shape, q.shape)]
        + [pltpu.VMEM(s, F32) for s in (k.shape, k.shape, (heads, HEAD, BLOCK))] + [dma((4, 4)), dma((3,))] + _sum_scratch(LATER),
        compiler_params=pltpu.CompilerParams(collective_id=1, has_side_effects=True, vmem_limit_bytes=VMEM),
        name="attend_back",
    )(q, k, v, do, lse, delta, gate.reshape(*GRID, COLOURS, ROWS, -ONE), up.reshape(*GRID, COLOURS, ROWS, -ONE), down.reshape(*GRID, PLACES, 2, ROWS, DIM))


def _project_back(dq, dk, dv, cos_ref, sin_ref, x, dh, turned, qkv, dwo, dx_o, rows_o,
                  dq_s, dk_s, dv_s, x_s, dh_s, at_s, w_s, by_s, dw_s, load_sems, out_sem, *refs):
    at = _place()
    heads, n, _ = dq_s.shape
    blocks = n // BLOCK
    sums, mates = _sums(at, (MIXED,), refs, None)
    for i in range(blocks):
        here = _tokens(i)
        _start(dq.at[:, here], dq_s.at[:, here], load_sems.at[ZERO, i])
        _start(dk.at[here], dk_s.at[here], load_sems.at[ONE, i])
        _start(dv.at[here], dv_s.at[here], load_sems.at[TWO, i])
    later = ((turned, at_s), (x, x_s), (dh, dh_s), (qkv, w_s))
    for i, (src, dst) in enumerate(later):
        _start(src, dst, load_sems.at[THREE, i])
    _greet(at)

    @pl.when(at["k"] == ZERO)
    def _():
        sums.give(MIXED, dwo)

    @pl.when(at["k"] == ONE)
    def _():
        sums.keep(MIXED, dwo)

    for i in range(blocks):
        here = slice(i * BLOCK, i * BLOCK + BLOCK)
        _arrived(dq_s.at[:, here], load_sems.at[ZERO, i])
        _arrived(dk_s.at[here], load_sems.at[ONE, i])
        _arrived(dv_s.at[here], load_sems.at[TWO, i])
        cos, sin = cos_ref[here, :], sin_ref[here, :]
        for m in range(heads + ONE):
            one = (dq_s[m, here, :] if m < heads else dk_s[here, :]).astype(F32)
            by_s[here, m * HEAD : (m + 1) * HEAD] = (one * cos - pltpu.roll(one, HEAD // TWO, 1) * sin).astype(BF)
        by_s[here, (heads + ONE) * HEAD :] = dv_s[here, :]
    _arrived(at_s, load_sems.at[THREE, 0])
    for c in range(0, by_s.shape[ONE], WIDE):
        dw_s[:, :, :, :, c : c + WIDE] = _mm(at_s[...], by_s[:, c : c + WIDE]).astype(BF).reshape(*GRID, COLOURS, ROWS, WIDE)

    @pl.when(at["k"] == ZERO)
    def _():
        sums.own[0][...] = dw_s[...]

    @pl.when(at["k"] == ONE)
    def _():
        sums.give(MIXED, dw_s)
        sums.kept(MIXED)

    for i, (_, dst) in enumerate(later[1:]):
        _arrived(dst, load_sems.at[THREE, i + 1])
    w = w_s[...]

    def back(i):
        here = slice(i * BLOCK, i * BLOCK + BLOCK)
        da = _mt(by_s[here, :], w).astype(BF)
        dh_s[here, :] = (dh_s[here, :].astype(F32) + _norm_back(x_s[here, :], da)).astype(BF)
        _start(dh_s.at[here], dx_o.at[here], out_sem.at[i])

    for i in range(sums.STEPS):
        if i < blocks:
            back(i)
        sums.steps(i)
    sums.deal_out(1, *mates)
    out_s, in_s, mate_sems = mates
    sums.dealt(out_s, in_s, mate_sems)
    rows_o[...] = in_s[...]
    sums.all_sent()
    for i in range(blocks):
        _arrived(dh_s.at[slice(i * BLOCK, i * BLOCK + BLOCK)], out_sem.at[i])


def project_back(dq, dk, dv, cos, sin, x, dh, turned, qkv, dwo):
    n, d = x.shape
    width = qkv.shape[ONE]
    vmem, anywhere = pl.BlockSpec(memory_space=pltpu.VMEM), pl.BlockSpec(memory_space=pl.ANY)
    dma = pltpu.SemaphoreType.DMA
    return pl.pallas_call(
        _project_back,
        in_specs=[anywhere] * 3 + [vmem] * TWO + [anywhere] * 5,
        out_specs=[anywhere, vmem],
        out_shape=[jax.ShapeDtypeStruct(s, BF) for s in ((n, d), (8, 1, 8, WIDE))],
        scratch_shapes=[pltpu.VMEM(s, BF) for s in (dq.shape, dk.shape, dk.shape, (n, d), (n, d), (d, n), (d, width), (n, width),
                                                    (*GRID, COLOURS, ROWS, width))] + [dma((4, 4)), dma((4,))] + _sum_scratch((MIXED,)),
        compiler_params=pltpu.CompilerParams(collective_id=2, has_side_effects=True, vmem_limit_bytes=VMEM),
        name="project_back",
    )(dq, dk, dv, cos, sin, x, dh, turned, qkv, dwo.reshape(*GRID, COLOURS, ROWS, -ONE))


def _deal(mixed_ref, wide_ref, down_ref, wq_o, wk_o, wv_o, wo_o, wg_o, wu_o, wd_o):
    for j in range(MATES):
        for lo in (0, HEAD):
            found = _from_mixed((wq_o, wk_o, wv_o, wo_o), _columns(j) + lo)
            if found:
                ref, first = found
                ref[:, first : first + HEAD] = mixed_ref[j, 0, ZERO:SIX, lo : lo + HEAD]
        for n, ref in enumerate((wg_o, wu_o)):
            ref[:, _columns(j) : _columns(j) + WIDE] = wide_ref[j, n, ZERO:SIX, :]
    wd_o[...] = down_ref[...]


def deal(mixed, wide, down):
    outs = ((6, DIM), (6, HEAD), (6, HEAD), (6, DIM), (6, FULL), (6, FULL), (ROWS, DIM))
    return _call(_deal, "deal", 1, [(a, *_all(*a.shape)) for a in (mixed, wide, down)], [(shape, BF, *_all(*shape)) for shape in outs])


def solution(mesh):
    def step(x, dy, *weights):
        x, dy = x[0], dy[0]
        qkv, wo, gate, up, down, at, dyt, q, k, v, o, cos, sin, lse = advance(x, dy, *(w[0] for w in weights))
        h, b, bt = close(o, x, wo)
        db, dwg, dwu, dwd = feed(b, bt, dy, dyt, gate, up, down)
        dh, do, delta, dwo = open_back(db, h, dy, o, wo)
        dq, dk, dv, wide, tall = attend_back(q, k, v, do, lse, delta, dwg, dwu, dwd)
        dx, mixed = project_back(dq, dk, dv, cos, sin, x, dh, at, qkv, dwo)
        return (dx[None], *(g[None] for g in deal(mixed, wide, tall)))

    states, cut = P(("rep", "dp"), None, None), P(None, "dp", None)
    return jax.shard_map(
        step,
        mesh=mesh,
        in_specs=(states, states) + (cut,) * 7,
        out_specs=(states,) + (P("rep", "dp", None),) * 7,
        check_vma=False,
    )
```

```python
import jax
import jax.numpy as jnp
import numpy as np
from jax import lax
from jax.experimental import pallas as pl
from jax.experimental.pallas import tpu as pltpu
from jax.sharding import PartitionSpec as P

HEAD = 128
THETA = 10000
EPS = 1e-6
ZERO, ONE, HALF, FULL, DIM, WIDE, ROWS, MATES, PLACES, SIX, TWO, THREE, COLOURS = 0, 1, 1024, 2048, 768, 256, 16, 8, 4, 6, 2, 3, 3
GRID = (PLACES, PLACES)
NEG = -1e30
HIDDEN = 2 * NEG
LOG2E = 1.4426950408889634
VMEM = 56 * 2**20
BLOCK = 512
BF, F32 = jnp.bfloat16, jnp.float32
SCALE = HEAD**-0.5
E = SCALE * LOG2E


def _dot(a, b, ca, cb):
    return lax.dot_general(a, b, (((ca,), (cb,)), ((), ())), preferred_element_type=F32)


def _mm(a, b):
    return _dot(a, b, ONE, ZERO)


def _mt(a, b):
    return _dot(a, b, ONE, ONE)


def _first():
    return pl.program_id(ZERO) == ZERO


def _last():
    return pl.program_id(ZERO) == pl.num_programs(ZERO) - ONE


def _visible():
    return lax.broadcasted_iota(jnp.int32, (BLOCK, BLOCK), 0) <= lax.broadcasted_iota(jnp.int32, (BLOCK, BLOCK), 1)


def _call(kernel, name, grid, ins, outs, scratch=(), flops=0):
    given = [a for a, _, _ in ins]
    moved = sum(a.size * a.dtype.itemsize for a in given)
    return pl.pallas_call(
        kernel,
        grid=(grid,),
        in_specs=[pl.BlockSpec(block, index) for _, block, index in ins],
        out_specs=[pl.BlockSpec(block, index) for _, _, block, index in outs],
        out_shape=[jax.ShapeDtypeStruct(shape, dtype) for shape, dtype, _, _ in outs],
        scratch_shapes=list(scratch),
        compiler_params=pltpu.CompilerParams(dimension_semantics=("arbitrary",), vmem_limit_bytes=VMEM),
        cost_estimate=pl.CostEstimate(flops=flops, transcendentals=0, bytes_accessed=2 * moved),
        name=name,
    )(*given)


def _rows(*shape):
    return shape, lambda i: (i,) + (0,) * (len(shape) - 1)


def _all(*shape):
    return shape, lambda i: (0,) * len(shape)


def _norm(h):
    wide = h.astype(F32)
    return (wide * lax.rsqrt(jnp.mean(wide * wide, -1, keepdims=ONE) + EPS)).astype(BF)


def _norm_back(h, g):
    wide, g = h.astype(F32), g.astype(F32)
    scale = lax.rsqrt(jnp.mean(wide * wide, -1, keepdims=ONE) + EPS)
    return scale * (g - wide * (scale * scale * jnp.mean(g * wide, -1, keepdims=ONE)))


FEED_STEP = 512
PIECE = 512
ROWS_AT_ONCE = DIM


def _middle(o, x, dy, dyt, wo, wg_ref, wu_ref, wd_ref, dh_o, do_o, delta_ref, dwo_ref, dwg_ref, dwu_ref, dwd_ref,
            o_s, h_s, dy_s, dyt_s, wo_s, b_s, bt_s, db_s, z_s, load_sems, out_sems):
    f = wg_ref.shape[ONE]
    heads, n, _ = o_s.shape
    d = h_s.shape[ONE]
    pieces = [slice(lo, lo + BLOCK) for lo in range(0, n, BLOCK)]

    @pl.when(_first())
    def _():
        pltpu.make_async_copy(wo, wo_s, load_sems.at[TWO, 0]).start()
        for i, here in enumerate(pieces):
            pltpu.make_async_copy(o.at[:, here], o_s.at[:, here], load_sems.at[ZERO, i]).start()
            pltpu.make_async_copy(x.at[here], h_s.at[here], load_sems.at[ONE, i]).start()
        pltpu.make_async_copy(dy, dy_s, load_sems.at[TWO, 1]).start()
        pltpu.make_async_copy(dyt, dyt_s, load_sems.at[TWO, 2]).start()
        pltpu.make_async_copy(wo, wo_s, load_sems.at[TWO, 0]).wait()

        def open_(i, _):
            here = pl.ds(pl.multiple_of(i * BLOCK, BLOCK), BLOCK)
            pltpu.make_async_copy(o.at[:, here], o_s.at[:, here], load_sems.at[ZERO, i]).wait()
            pltpu.make_async_copy(x.at[here], h_s.at[here], load_sems.at[ONE, i]).wait()
            heard = jnp.concatenate([o_s[m, here, :] for m in range(heads)], axis=ONE)
            h = h_s[here, :] + _mm(heard, wo_s[:, :d]).astype(BF)
            h_s[here, :] = h
            b = _norm(h)
            b_s[here, :] = b
            bt_s[:, here] = b.T

        lax.fori_loop(0, n // BLOCK, open_, None)
        db_s[...] = jnp.zeros_like(db_s)
        pltpu.make_async_copy(dy, dy_s, load_sems.at[TWO, 1]).wait()
        pltpu.make_async_copy(dyt, dyt_s, load_sems.at[TWO, 2]).wait()

    both = jnp.concatenate([wg_ref[...], wu_ref[...]], axis=ONE)

    def piece(i, _):
        here = slice(i * PIECE, i * PIECE + PIECE)
        gate_up = _mm(b_s[here, :], both)
        gate, up = gate_up[:, :f], gate_up[:, f:]
        dmid = _mt(dy_s[here, :], wd_ref[...]).astype(BF).astype(F32)
        sig = 0.5 * jnp.tanh(0.5 * gate) + 0.5
        silu = gate * sig
        z_s[here, 2 * f :] = (silu * up).astype(BF)
        dup = (dmid * silu).astype(BF)
        dgate = (dmid * up * (sig + silu * (1 - sig))).astype(BF)
        z_s[here, :f] = dgate
        z_s[here, f : 2 * f] = dup
        db_s[here, :] += _mt(jnp.concatenate([dgate, dup], axis=ONE), both)

    for i in range(n // PIECE):
        piece(i, None)

    def weights(i, _):
        here = pl.ds(pl.multiple_of(i * ROWS_AT_ONCE, ROWS_AT_ONCE), ROWS_AT_ONCE)
        dw = _mm(bt_s[here, :], z_s[:, : 2 * f])
        dwg_ref[here, :] = dw[:, :f].astype(BF)
        dwu_ref[here, :] = dw[:, f:].astype(BF)
        dwd_ref[:, here] = _mm(dyt_s[here, :], z_s[:, 2 * f :]).astype(BF).T

    lax.fori_loop(0, d // ROWS_AT_ONCE, weights, None)

    @pl.when(_last())
    def _():

        def back(i, _):
            here = pl.ds(pl.multiple_of(i * BLOCK, BLOCK), BLOCK)
            dy_s[here, :] = (dy_s[here, :].astype(F32) + _norm_back(h_s[here, :], db_s[here, :].astype(BF))).astype(BF)
            pltpu.make_async_copy(dy_s.at[here], dh_o.at[here], out_sems.at[ZERO, i]).start()

        lax.fori_loop(0, n // BLOCK, back, None)

        def by_wo(m, _):
            here = pl.ds(pl.multiple_of(m * HEAD, HEAD), HEAD)
            dwo_ref[here, :d] = _dot(o_s[m], dy_s[...], 0, 0).astype(BF)

        lax.fori_loop(0, heads, by_wo, None)
        dwo_ref[:, d:] = jnp.zeros_like(dwo_ref[:, d:])

        def by_o(i, _):
            here = pl.ds(pl.multiple_of(i * BLOCK, BLOCK), BLOCK)
            do = _mt(dy_s[here, :], wo_s[:, :d]).astype(BF)
            for m in range(heads):
                mine = do[:, m * HEAD : (m + 1) * HEAD]
                delta_ref[m : m + 1, here] = (mine.astype(F32) * o_s[m, here, :].astype(F32)).T.sum(axis=ZERO, keepdims=ONE)
                o_s[m, here, :] = mine
            pltpu.make_async_copy(o_s.at[:, here], do_o.at[:, here], out_sems.at[ONE, i]).start()

        lax.fori_loop(0, n // BLOCK, by_o, None)
        for i, here in enumerate(pieces):
            pltpu.make_async_copy(dy_s.at[here], dh_o.at[here], out_sems.at[ZERO, i]).wait()
            pltpu.make_async_copy(o_s.at[:, here], do_o.at[:, here], out_sems.at[ONE, i]).wait()


def middle(o, x, dy, dyt, wo, gate, up, down):
    n, d = x.shape
    heads, f, ff = o.shape[ZERO], FEED_STEP, gate.shape[ONE]
    anywhere = pl.BlockSpec(memory_space=pl.ANY)
    cols, rows = pl.BlockSpec((d, f), lambda i: (0, i)), pl.BlockSpec((f, d), lambda i: (i, 0))
    dma = pltpu.SemaphoreType.DMA
    return pl.pallas_call(
        _middle,
        grid=(ff // f,),
        in_specs=[anywhere] * 5 + [cols, cols, rows],
        out_specs=[anywhere] * TWO + [pl.BlockSpec((heads, n), lambda i: (0, 0)), pl.BlockSpec(wo.shape, lambda i: (0, 0)), cols, cols, rows],
        out_shape=[jax.ShapeDtypeStruct(s, t) for s, t in (((n, d), BF), (o.shape, BF), ((heads, n), F32), (wo.shape, BF),
                                                           (gate.shape, BF), (up.shape, BF), (down.shape, BF))],
        scratch_shapes=[pltpu.VMEM(s, BF) for s in (o.shape, (n, d), (n, d), (d, n), wo.shape, (n, d), (d, n))]
        + [pltpu.VMEM((n, d), F32), pltpu.VMEM((n, 3 * f), BF), dma((3, 4)), dma((2, 4))],
        compiler_params=pltpu.CompilerParams(dimension_semantics=("arbitrary",), vmem_limit_bytes=VMEM),
        cost_estimate=pl.CostEstimate(flops=ROWS * n * d * ff, transcendentals=0, bytes_accessed=2 * n * d * 20),
        name="middle",
    )(o, x, dy, dyt, wo, gate, up, down)


RING = 4
ORDERS = ("xyz", "yzx", "zxy")
MIXED, GATE, UP, DOWN = range(PLACES)


def _place():
    me = lax.axis_index("dp")
    return {"x": me // 32, "y": me // 8 % RING, "z": me // TWO % RING, "k": me % TWO}


def _device(at, **other):
    at = {**at, **other}
    return {"dp": ((at["x"] * 4 + at["y"]) * 4 + at["z"]) * TWO + at["k"]}


def _beside(at, axis, by):
    return _device(at, **{axis: (at[axis] + by) % RING})


def _mate(at, by):
    other = (at["z"] * TWO + at["k"] + by) % 8
    return _device(at, z=other // TWO, k=other % TWO)


def _greet(at):
    barrier = pltpu.get_barrier_semaphore()
    peers = [_beside(at, axis, by) for axis in "xy" for by in range(1, RING)] + [_mate(at, by) for by in range(ONE, MATES)]
    for peer in peers:
        pl.semaphore_signal(barrier, inc=1, device_id=peer, device_id_type=pl.DeviceIdType.MESH)
    pl.semaphore_wait(barrier, len(peers))


def _remote(src, dst, send, recv, device):
    pltpu.make_async_remote_copy(src_ref=src, dst_ref=dst, send_sem=send, recv_sem=recv, device_id=device,
                                 device_id_type=pl.DeviceIdType.MESH).start()


def _start(src, dst, sem):
    pltpu.make_async_copy(src, dst, sem).start()


def _arrived(ref, sem):
    pltpu.make_async_copy(ref, ref, sem).wait()


def _lanes(z, lo=0, n=WIDE):
    return pl.ds(pl.multiple_of(z * WIDE + lo, HEAD), n)


def _half_columns(k):
    return pl.ds(pl.multiple_of(k * HALF, HALF), HALF)


def _tokens(i):
    return pl.ds(i * BLOCK if isinstance(i, int) else pl.multiple_of(i * BLOCK, BLOCK), BLOCK)


def _columns(j):
    return (j % TWO) * HALF + (j // TWO) * WIDE


STARTS = (0, DIM, 896, HALF)


def _from_mixed(refs, lo):
    return next(((ref, lo - base) for ref, base in zip(refs, STARTS, strict=ONE) if 0 <= lo - base < ref.shape[ONE]), None)


def _advance(wq, wk, wv, wo, wg, wu, wd, freq, x, dy, qkv_o, wo_o, gate_o, up_o, down_o, at_o, dyt_o, q_o, k_o, v_o, o_o, cos_o, sin_o, lse_o,
             out_s, in_s, ws, wds, mixed_s, x_s, dy_s, a_s, at_s, dyt_s, q_s, k_s, v_s, o_s, top_s, mix_s, cos_s, sin_s,
             mate_sems, ring_send, ring_recv, pair_sems, own_sem, load_sems, store_sems):
    at = _place()
    seat = at["z"] * TWO + at["k"]
    outs = (None, gate_o, up_o)
    heads = q_s.shape[ZERO]
    blocks = x_s.shape[ZERO] // BLOCK
    sent = {}
    kept = []

    def send(key, ref, dst, sem, recv, device):
        _remote(ref(), dst(), sem(), recv, device)
        sent[key] = ref, sem

    def store(src, dst, n):
        _start(src, dst, store_sems.at[n])
        kept.append((src, store_sems.at[n]))

    _start(x, x_s, load_sems.at[ZERO])
    _start(dy, dy_s, load_sems.at[ONE])
    for j in range(MATES):
        for lo in (0, HEAD):
            found = _from_mixed((wq, wk, wv, wo), _columns(j) + lo)
            if found:
                ref, first = found
                out_s[j, MIXED, ZERO:SIX, lo : lo + HEAD] = ref[:, first : first + HEAD]
            else:
                out_s[j, MIXED, ZERO:SIX, lo : lo + HEAD] = jnp.zeros((6, HEAD), BF)
        for t, ref in ((GATE, wg), (UP, wu)):
            out_s[j, t, ZERO:SIX, :] = ref[:, _columns(j) : _columns(j) + WIDE]
        out_s[j, :, SIX:MATES, :] = jnp.zeros((3, 2, WIDE), BF)
    _greet(at)
    for by in range(ONE, MATES):
        send(by, lambda by=by: out_s.at[(seat + by) % 8], lambda: in_s.at[seat], lambda by=by: mate_sems.at[ZERO, by], mate_sems.at[ONE, by],
             _mate(at, by))
    in_s[seat] = out_s[seat]
    for c in range(COLOURS):
        wds[at["x"], at["y"], at["z"], :, WIDE * c : WIDE * c + WIDE] = wd[:, WIDE * c : WIDE * c + WIDE]

    def region(t, c, fixed, half=None):
        x, y = (fixed.get(axis, slice(None)) for axis in "xy")
        if t != DOWN and "z" not in fixed:
            return ws.at[t, x, y, c, :, slice(None) if half is None else slice(512 * half, 512 * half + 512)]
        lo, n = (0, WIDE) if half is None else (HEAD * half, HEAD)
        if t == DOWN:
            return wds.at[x, y, fixed.get("z", slice(None)), :, WIDE * c + lo : WIDE * c + lo + n]
        return ws.at[t, x, y, c, :, _lanes(fixed["z"], lo, n)]

    def known(c, phase, place):
        order = ORDERS[c][::-1]
        return {**{a: at[a] for a in order[phase + 1 :]}, order[phase]: place}

    def hop(t, c, phase, slot, by, here):
        key = t, c, phase, slot
        send(key, here, here, lambda: ring_send.at[key], ring_recv.at[key], _beside(at, ORDERS[c][::-1][phase], by))

    def send_own(phase, *ts):
        for t in ts:
            for c in range(COLOURS):
                for slot, by in enumerate((1, 2, 3) if phase < 2 else (1, 3)):
                    hop(t, c, phase, slot, by, lambda t=t, c=c: region(t, c, known(c, phase, at[ORDERS[c][::-1][phase]])))

    def pass_on(phase, *ts):
        for t in ts:
            for c in range(COLOURS):
                axis = ORDERS[c][::-1][phase]
                for slot, by in ((0, 3), (1, 1)):

                    def here(half, t=t, c=c, axis=axis, by=by):
                        return region(t, c, known(c, phase, (at[axis] + by) % RING), half)

                    _arrived(here(None), ring_recv.at[t, c, phase, slot])
                    hop(t, c, phase, 2 + slot, RING - by, lambda here=here, slot=slot: here(1 - slot))

    def finish(phase, *ts):
        for t in ts:
            for c in range(COLOURS):
                place = at[ORDERS[c][::-1][phase]]
                for slot in range(COLOURS) if phase < 2 else (2, 3):
                    by, half = (3 - slot, None) if phase < 2 else (2, 3 - slot)
                    _arrived(region(t, c, known(c, phase, (place + by) % RING), half), ring_recv.at[t, c, phase, slot])

    partner = _device(at, k=ONE - at["k"])

    def half(t, k):
        return down_o.at[:, :, :, k] if t == DOWN else outs[t].at[:, :, :, :, _half_columns(k)]

    def to_result(t):
        src = wds if t == DOWN else ws.at[t]
        _remote(src, half(t, at["k"]), pair_sems.at[ZERO, t], pair_sems.at[ONE, t], partner)
        _start(src, half(t, at["k"]), own_sem.at[t])

    def prepare(i):
        here = slice(i * BLOCK, i * BLOCK + BLOCK)
        a = _norm(x_s[here, :])
        a_s[here, :] = a
        at_s[:, here] = a.T

    def turn(i):
        here = slice(i * BLOCK, i * BLOCK + BLOCK)
        dyt_s[:, here] = dy_s[here, :].T

    def tables():
        half, rows = HEAD // TWO, 64
        place = lax.broadcasted_iota(jnp.int32, (rows, HEAD), 0).astype(F32)
        left = lax.broadcasted_iota(jnp.int32, (rows, HEAD), 1) < half
        near, far = place * freq[...], place[: x_s.shape[ZERO] // rows] * rows * freq[: x_s.shape[ZERO] // rows]
        near_cos, near_sin, far_cos, far_sin = jnp.cos(near), jnp.sin(near), jnp.cos(far), jnp.sin(far)
        for n in range(x_s.shape[ZERO] // rows):
            c, s = far_cos[n : n + ONE, :], far_sin[n : n + ONE, :]
            cos_s[n * rows : n * rows + rows, :] = near_cos * c - near_sin * s
            sin = near_sin * c + near_cos * s
            sin_s[n * rows : n * rows + rows, :] = jnp.where(left, -sin, sin)
        store(cos_s, cos_o, 6)
        store(sin_s, sin_o, 7)

    def project(i):
        here = slice(i * BLOCK, i * BLOCK + BLOCK)
        t = _mm(a_s[here, :], mixed_s[...].reshape(a_s.shape[ONE], -1)).astype(BF)
        cos, sin = cos_s[here, :], sin_s[here, :]
        for n in range(heads + ONE):
            one = t[:, n * HEAD : (n + ONE) * HEAD].astype(F32)
            one = (one * cos + pltpu.roll(one, HEAD // TWO, 1) * sin).astype(BF)
            if n < heads:
                q_s[n, here, :] = one
            else:
                k_s[here, :] = one
        v_s[here, :] = t[:, (heads + ONE) * HEAD :]

    rest = (GATE, UP, DOWN)
    _arrived(x_s, load_sems.at[ZERO])
    prepare(0)
    for by in range(ONE, MATES):
        _arrived(in_s.at[ZERO], mate_sems.at[ONE, by])
    for t in range(COLOURS):
        rows = jnp.concatenate([in_s[j, t].astype(F32)[ZERO:SIX, :] for j in range(MATES)], axis=ZERO).astype(BF)
        for c in range(COLOURS):
            ws[t, at["x"], at["y"], c, :, _lanes(at["z"])] = rows[ROWS * c : ROWS * c + ROWS, :]
    send_own(0, MIXED)
    send_own(0, *rest)
    prepare(1)
    prepare(2)
    finish(0, MIXED)
    send_own(1, MIXED)
    finish(0, *rest)
    send_own(1, *rest)
    prepare(3)
    store(at_s, at_o, 0)
    tables()
    finish(1, MIXED)
    send_own(2, MIXED)
    finish(1, *rest)
    send_own(2, GATE)
    _arrived(dy_s, load_sems.at[ONE])
    turn(0)
    turn(1)
    pass_on(2, MIXED)
    send_own(2, UP)
    turn(2)
    turn(3)
    store(dyt_s, dyt_o, 1)
    finish(2, MIXED)

    @pl.when(at["k"] == ZERO)
    def _():
        _remote(ws.at[MIXED], mixed_s, pair_sems.at[ZERO, MIXED], pair_sems.at[ONE, MIXED], partner)
        mixed_s[...] = ws[MIXED]

    @pl.when(at["k"] == ONE)
    def _():
        _remote(ws.at[MIXED], wo_o, pair_sems.at[ZERO, MIXED], pair_sems.at[ONE, MIXED], partner)
        _start(ws.at[MIXED], wo_o, own_sem.at[MIXED])

    pass_on(2, GATE)
    send_own(2, DOWN)
    _arrived(mixed_s, pair_sems.at[ONE, MIXED])
    store(mixed_s, qkv_o, 2)
    for i in range(blocks):
        project(i)
        if i == 1:
            pass_on(2, UP)
    store(q_s, q_o, 3)
    store(k_s, k_o, 4)
    store(v_s, v_o, 5)

    def between(n):
        @pl.when(n == 0)
        def _():
            finish(2, GATE)
            to_result(GATE)

        @pl.when(n == 1)
        def _():
            pass_on(2, DOWN)

        @pl.when(n == 2)
        def _():
            finish(2, UP)
            to_result(UP)

        @pl.when(n == 3)
        def _():
            finish(2, DOWN)
            to_result(DOWN)

    ones = jnp.ones((8, BLOCK), BF)

    def block(iq, j, masked):
        here = _tokens(j)
        mine = _tokens(iq)
        scores = [_mt(k_s[here, :], q_s[n, mine, :]) for n in range(heads)]
        weights, keeps = [], []
        for n, s in enumerate(scores):
            if masked:
                s = jnp.where(_visible(), s, HIDDEN)
            old = top_s[n : n + ONE, :]
            top = jnp.maximum(old, s.max(axis=ZERO, keepdims=ONE))
            top_s[n : n + ONE, :] = top
            weights.append(jnp.exp2((s - top) * E).astype(BF))
            keeps.append(jnp.exp2((old - top) * E))
        values = jnp.concatenate([v_s[here, :].T, ones], axis=ZERO)
        for n, (p, keep) in enumerate(zip(weights, keeps, strict=ONE)):
            mix_s[n] = mix_s[n] * keep + _mm(values, p)

    def row(iq, _):
        top_s[...] = jnp.full(top_s.shape, NEG, F32)
        mix_s[...] = jnp.zeros(mix_s.shape, F32)

        def step(j, _):
            block(iq, j, False)
            between(iq * (iq + ONE) // TWO + j)

        lax.fori_loop(0, iq, step, None)
        block(iq, iq, True)
        between(iq * (iq + ONE) // TWO + iq)
        mine = _tokens(iq)
        for n in range(heads):
            total = mix_s[n, HEAD : HEAD + 1, :]
            o_s[n, mine, :] = (mix_s[n, :HEAD, :] * (1 / total)).T.astype(BF)
            lse_o[n : n + ONE, mine] = top_s[n : n + ONE, :] * SCALE + jnp.log(total)
        _start(o_s.at[:, mine], o_o.at[:, mine], own_sem.at[4])

    lax.fori_loop(0, blocks, row, None)
    _arrived(o_s, own_sem.at[4])
    for ref, sem in sent.values():
        _arrived(ref(), sem())
    for t in (MIXED, *rest):
        src = wds if t == DOWN else ws.at[t]
        _arrived(src, pair_sems.at[ZERO, t])
        if t != MIXED:
            _arrived(src, pair_sems.at[ONE, t])
            _arrived(src, own_sem.at[t])

    @pl.when(at["k"] == ONE)
    def _():
        _arrived(ws.at[MIXED], own_sem.at[MIXED])

    for ref, sem in kept:
        _arrived(ref, sem)


def advance(x, dy, *shards):
    n, d = x.shape
    heads = d // HEAD
    half = HEAD // TWO
    freq = np.tile(float(THETA) ** (-np.arange(half) / half), (half, 2)).astype(np.float32)
    vmem, anywhere = pl.BlockSpec(memory_space=pltpu.VMEM), pl.BlockSpec(memory_space=pl.ANY)
    wide, narrow = (*GRID, COLOURS, ROWS, FULL), (*GRID, COLOURS, ROWS, HALF)
    tall = (*GRID, PLACES, 2, ROWS, DIM)
    many, one = (heads, n, HEAD), (n, HEAD)
    shapes = (narrow, narrow, wide, wide, tall, (d, n), (d, n), many, one, one, many)
    dma = pltpu.SemaphoreType.DMA
    qkv, wo, gate, up, down, *rest = pl.pallas_call(
        _advance,
        in_specs=[vmem] * 8 + [anywhere] * 2,
        out_specs=[anywhere] * (len(shapes) + 2) + [vmem],
        out_shape=[jax.ShapeDtypeStruct(s, BF) for s in shapes] + [jax.ShapeDtypeStruct(s, F32) for s in (one, one, (heads, n))],
        scratch_shapes=[pltpu.VMEM(s, BF) for s in ((MATES, 3, MATES, WIDE), (MATES, 3, MATES, WIDE), (3, *narrow), (*GRID, PLACES, ROWS, DIM), narrow,
                                                    (n, d), (n, d), (n, d), (d, n), (d, n), many, one, one, many)]
        + [pltpu.VMEM(s, F32) for s in ((heads, BLOCK), (heads, HEAD + 8, BLOCK), one, one)]
        + [dma((2, 8)), dma((PLACES, COLOURS, COLOURS, PLACES)), dma((PLACES, COLOURS, COLOURS, PLACES)), dma((2, 4)), dma((5,)), dma((2,)), dma((8,))],
        compiler_params=pltpu.CompilerParams(collective_id=0, has_side_effects=True, vmem_limit_bytes=VMEM),
        name="advance",
    )(*shards, freq, x, dy)
    return qkv.reshape(d, -1), wo.reshape(d, -1), gate.reshape(d, -1), up.reshape(d, -1), down.reshape(-1, d), *rest


class _Sums:
    STEPS = 5

    def __init__(self, at, ts, own, theirs, bufs, total, down_o, ring_send, ring_recv, pair_sems, own_sems):
        self.at, self.ts, self.own, self.theirs, self.bufs, self.total, self.down_o = at, ts, own, theirs, bufs, total, down_o
        self.ring_send, self.ring_recv, self.pair_sems, self.own_sems = ring_send, ring_recv, pair_sems, own_sems
        self.partner = _device(at, k=ONE - at["k"])

    def give(self, t, ref):
        n = self.ts.index(t)
        _remote(ref, self.theirs[n], self.pair_sems.at[ZERO, n], self.pair_sems.at[ONE, n], self.partner)

    def keep(self, t, ref):
        n = self.ts.index(t)
        _start(ref, self.own[n], self.own_sems.at[n])

    def kept(self, t):
        n = self.ts.index(t)
        _arrived(self.own[n], self.own_sems.at[n])

    def term(self, n, c, phase, q, i, j):
        if phase:
            acc = self.bufs[phase - 1][-1]
            return acc[n, c, q, j] if phase == 1 else acc[n, c, q]
        place = dict(zip(ORDERS[c], (q, i, j), strict=ONE))
        x, y, z = (place[a] for a in "xyz")
        if self.ts[n] == DOWN:
            both = (ref[x, y, z, :, WIDE * c : WIDE * c + WIDE] for ref in (self.own[n], self.theirs[n]))
        else:
            both = (ref[x, y, c, :, _lanes(z)] for ref in (self.own[n], self.theirs[n]))
        return sum(b.astype(F32) for b in both)

    @staticmethod
    def over_cells(phase, act):
        if phase == 0:
            lax.fori_loop(0, 4, lambda i, _: [act(i, j, (i, j)) for j in range(PLACES)] and None, None)
        elif phase == 1:
            for j in range(PLACES):
                act(0, j, (j,))
        else:
            act(0, 0, ())

    def hop(self, n, c, phase, slot, by, src, dst):
        _remote(src, dst, self.ring_send.at[n, c, phase, slot], self.ring_recv.at[n, c, phase, slot], _beside(self.at, ORDERS[c][phase], by))

    def near(self, c, phase, by):
        return (self.at[ORDERS[c][phase]] + by) % RING

    def begin(self, n, c, phase):
        to, into = self.bufs[phase][:2]
        places = [self.near(c, phase, by) for by in (1, 2, 3)]

        def act(i, j, where):
            above, opposite, below = (self.term(n, c, phase, q, i, j) for q in places)
            to[(n, c, 0, *where)] = jnp.concatenate([above[:, :HEAD], opposite[:, HEAD:]], axis=ONE).astype(BF)
            to[(n, c, 1, *where)] = jnp.concatenate([opposite[:, :HEAD], below[:, HEAD:]], axis=ONE).astype(BF)

        def straight(i, j, where):
            for slot, q in enumerate(places):
                to[(n, c, slot, *where)] = self.term(n, c, phase, q, i, j).astype(BF)

        self.over_cells(phase, straight if phase else act)
        for slot, by in enumerate((1, 2, 3) if phase else (1, 3)):
            self.hop(n, c, phase, slot, by, to.at[n, c, slot], into.at[n, c, slot])

    def relay(self, n, c, phase):
        into, over, last = self.bufs[phase][1:4]
        for slot, by, half in ((0, 1, slice(HEAD, WIDE)), (1, 3, slice(0, HEAD))):
            _arrived(into.at[n, c, slot], self.ring_recv.at[n, c, phase, slot])
            place = self.near(c, phase, by)

            def act(i, j, where, slot=slot, half=half, place=place):
                mine = self.term(n, c, phase, place, i, j)[:, half]
                over[(n, c, slot, *where)] = (mine + into[(n, c, slot, *where)][:, half].astype(F32)).astype(BF)

            self.over_cells(phase, act)
            self.hop(n, c, phase, 2 + slot, by, over.at[n, c, slot], last.at[n, c, slot])

    def finish(self, n, c, phase):
        into = self.bufs[phase][1]
        if phase:
            for slot in range(COLOURS):
                _arrived(into.at[n, c, slot], self.ring_recv.at[n, c, phase, slot])
        else:
            last = self.bufs[phase][3]
            for slot in (ZERO, ONE):
                _arrived(last.at[n, c, slot], self.ring_recv.at[n, c, phase, 2 + slot])

        def act(i, j, where):
            mine = self.term(n, c, phase, self.near(c, phase, 0), i, j)
            if phase:
                whole = sum((into[(n, c, slot, *where)].astype(F32) for slot in range(COLOURS)), mine)
            else:
                a = mine[:, :HEAD] + into[(n, c, 0, *where)][:, :HEAD].astype(F32) + last[(n, c, 1, *where)].astype(F32)
                b = mine[:, HEAD:] + into[(n, c, 1, *where)][:, HEAD:].astype(F32) + last[(n, c, 0, *where)].astype(F32)
                whole = jnp.concatenate([a, b], axis=ONE)
            if phase < 2:
                self.bufs[phase][-1][(n, c, *where)] = whole
            elif self.ts[n] == DOWN:
                self.down_o[:, WIDE * c : WIDE * c + WIDE] = whole.astype(BF)
            else:
                self.total[n, ROWS * c : ROWS * c + ROWS, :] = whole

        self.over_cells(phase, act)

    def step(self, n, what):
        if what == 0:
            _arrived(self.theirs[n], self.pair_sems.at[ONE, n])
        for c in range(COLOURS):
            if what == 0:
                self.begin(n, c, 0)
            elif what == 1:
                self.relay(n, c, 0)
            else:
                self.finish(n, c, what - 2)
                if what < 4:
                    self.begin(n, c, what - 1)

    def steps(self, slot):
        for n in range(len(self.ts)):
            if 0 <= slot - n < self.STEPS:
                self.step(n, slot - n)

    def all_sent(self):
        for n in range(len(self.ts)):
            _arrived(self.theirs[n], self.pair_sems.at[ZERO, n])
            for c in range(COLOURS):
                for phase, (to, _, *more) in enumerate(self.bufs):
                    for slot in range(COLOURS) if phase else (ZERO, ONE):
                        _arrived(to.at[n, c, slot], self.ring_send.at[n, c, phase, slot])
                        if not phase:
                            _arrived(more[0].at[n, c, slot], self.ring_send.at[n, c, phase, 2 + slot])

    def deal_out(self, wide, out_s, in_s, mate_sems):
        seat = self.at["z"] * TWO + self.at["k"]
        for n in range(wide):
            for j in range(MATES):
                out_s[j, n, ZERO:SIX, :] = self.total[n, 6 * j : 6 * j + 6, :].astype(BF)
                out_s[j, n, SIX:MATES, :] = jnp.zeros((2, WIDE), BF)
        for by in range(ONE, MATES):
            _remote(out_s.at[(seat + by) % 8], in_s.at[seat], mate_sems.at[ZERO, by], mate_sems.at[ONE, by], _mate(self.at, by))
        in_s[seat] = out_s[seat]

    @staticmethod
    def dealt(out_s, in_s, mate_sems):
        for by in range(ONE, MATES):
            _arrived(in_s.at[ZERO], mate_sems.at[ONE, by])
            _arrived(out_s.at[ZERO], mate_sems.at[ZERO, by])


def _sum_scratch(ts):
    count = len(ts)
    scratch = [pltpu.VMEM((*GRID, PLACES, ROWS, DIM) if t == DOWN else (*GRID, COLOURS, ROWS, HALF), BF) for t in ts for _ in range(2)]
    for left in ((4, 4), (4,), ()):
        first = left == (4, 4)
        scratch += [pltpu.VMEM((count, 3, 2 if first else 3, *left, ROWS, WIDE), BF)] * 2
        scratch += [pltpu.VMEM((count, 3, 2, *left, ROWS, HEAD), BF)] * TWO if first else []
        scratch += [pltpu.VMEM((count, 3, *left, ROWS, WIDE), F32)] if left else []
    wide = count - (DOWN in ts)
    dma = pltpu.SemaphoreType.DMA
    return scratch + [pltpu.VMEM((wide, 48, WIDE), F32)] + [pltpu.VMEM((8, wide, 8, WIDE), BF)] * TWO + [
        dma((count, COLOURS, COLOURS, PLACES)), dma((count, COLOURS, COLOURS, PLACES)), dma((2, count)), dma((count,)), dma((2, 8))]


def _sums(at, ts, refs, down_o):
    refs = list(refs)
    pairs = [(refs.pop(0), refs.pop(0)) for _ in ts]
    bufs = [[refs.pop(0) for _ in range(many)] for many in (5, 3, 2)]
    total, out_s, in_s, ring_send, ring_recv, pair_sems, own_sems, mate_sems = refs
    sums = _Sums(at, ts, [a for a, _ in pairs], [b for _, b in pairs], bufs, total, down_o, ring_send, ring_recv, pair_sems, own_sems)
    return sums, (out_s, in_s, mate_sems)


LATER = (GATE, UP, DOWN)


def _attend_back(q, k, v, do, lse_ref, delta_ref, gate, up, down, dq_o, dk_o, dv_o, rows_o, down_o,
                 q_s, k_s, v_s, do_s, dq_s, dk_s, dv_s, sum_s, load_sems, out_sem, *refs):
    at = _place()
    heads = q_s.shape[ZERO]
    blocks = q_s.shape[ONE] // BLOCK
    sums, mates = _sums(at, LATER, refs, down_o)
    _start(k, k_s, load_sems.at[ZERO, 0])
    _start(v, v_s, load_sems.at[ONE, 0])
    for i in range(blocks):
        _start(q.at[:, _tokens(i)], q_s.at[:, _tokens(i)], load_sems.at[TWO, i])
        _start(do.at[:, _tokens(i)], do_s.at[:, _tokens(i)], load_sems.at[THREE, i])
    _greet(at)

    def part(t, k):
        return down.at[:, :, :, k] if t == DOWN else (gate, up)[t - GATE].at[:, :, :, :, _half_columns(k)]

    for t in LATER:
        sums.give(t, part(t, ONE - at["k"]))
        sums.keep(t, part(t, at["k"]))
    sum_s[...] = jnp.zeros_like(sum_s)
    dk_s[...] = jnp.zeros_like(dk_s)
    dv_s[...] = jnp.zeros_like(dv_s)
    _arrived(k_s, load_sems.at[ZERO, 0])
    _arrived(v_s, load_sems.at[ONE, 0])

    def between(slot):
        if 0 <= slot < 3:
            sums.kept(LATER[slot])
        sums.steps(slot)
        if slot == sums.STEPS + 1:
            sums.deal_out(2, *mates)

    def block(iq, j):
        here, mine = _tokens(j), _tokens(iq)

        def some(half, _):
            group = [half * (heads // TWO) + n for n in range(heads // TWO)]
            scores = [_mt(k_s[here, :], q_s[n, mine, :]) for n in group]
            dps = [_mt(v_s[here, :], do_s[n, mine, :]) for n in group]
            for n, s, dp in zip(group, scores, dps, strict=ONE):
                p = jnp.exp2(s * E - lse_ref[pl.ds(n, 1), mine] * LOG2E)
                if iq == j:
                    p = jnp.where(_visible(), p, 0.0)
                ds = (p * (dp - delta_ref[pl.ds(n, 1), mine])).astype(BF)
                dv_s[here, :] += _mm(p.astype(BF), do_s[n, mine, :])
                dk_s[here, :] += _mm(ds, q_s[n, mine, :])
                sum_s[n] += _mm(k_s[here, :].T, ds)

        lax.fori_loop(0, 2, some, None)

    for iq in range(blocks):
        mine = _tokens(iq)
        _arrived(q_s.at[:, mine], load_sems.at[TWO, iq])
        _arrived(do_s.at[:, mine], load_sems.at[THREE, iq])
        for j in range(iq + ONE):
            block(iq, j)
            between(iq * (iq + ONE) // TWO + j - 1)
        for n in range(heads):
            dq_s[n, mine, :] = (sum_s[n] * SCALE).T.astype(BF)
        sum_s[...] = jnp.zeros_like(sum_s)
        _start(dq_s.at[:, mine], dq_o.at[:, mine], out_sem.at[ZERO])

    k_s[...] = (dk_s[...] * SCALE).astype(BF)
    v_s[...] = dv_s[...].astype(BF)
    _start(k_s, dk_o, out_sem.at[ONE])
    _start(v_s, dv_o, out_sem.at[2])
    out_s, in_s, mate_sems = mates
    sums.dealt(out_s, in_s, mate_sems)
    rows_o[...] = in_s[...]
    sums.all_sent()
    _arrived(dq_s, out_sem.at[ZERO])
    _arrived(k_s, out_sem.at[ONE])
    _arrived(v_s, out_sem.at[2])


def attend_back(q, k, v, do, lse, delta, gate, up, down):
    heads, n, _ = q.shape
    vmem, anywhere = pl.BlockSpec(memory_space=pltpu.VMEM), pl.BlockSpec(memory_space=pl.ANY)
    shapes = (q.shape, k.shape, k.shape, (8, 2, 8, WIDE), (ROWS, DIM))
    dma = pltpu.SemaphoreType.DMA
    return pl.pallas_call(
        _attend_back,
        in_specs=[anywhere] * 4 + [vmem] * TWO + [anywhere] * 3,
        out_specs=[anywhere] * 3 + [vmem] * 2,
        out_shape=[jax.ShapeDtypeStruct(s, BF) for s in shapes],
        scratch_shapes=[pltpu.VMEM(s, BF) for s in (q.shape, k.shape, k.shape, q.shape, q.shape)]
        + [pltpu.VMEM(s, F32) for s in (k.shape, k.shape, (heads, HEAD, BLOCK))] + [dma((4, 4)), dma((3,))] + _sum_scratch(LATER),
        compiler_params=pltpu.CompilerParams(collective_id=1, has_side_effects=True, vmem_limit_bytes=VMEM),
        name="attend_back",
    )(q, k, v, do, lse, delta, gate.reshape(*GRID, COLOURS, ROWS, -ONE), up.reshape(*GRID, COLOURS, ROWS, -ONE), down.reshape(*GRID, PLACES, 2, ROWS, DIM))


def _project_back(dq, dk, dv, cos_ref, sin_ref, x, dh, turned, qkv, dwo, dx_o, rows_o,
                  dq_s, dk_s, dv_s, x_s, dh_s, at_s, w_s, by_s, dw_s, load_sems, out_sem, *refs):
    at = _place()
    heads, n, _ = dq_s.shape
    blocks = n // BLOCK
    sums, mates = _sums(at, (MIXED,), refs, None)
    for i in range(blocks):
        here = _tokens(i)
        _start(dq.at[:, here], dq_s.at[:, here], load_sems.at[ZERO, i])
        _start(dk.at[here], dk_s.at[here], load_sems.at[ONE, i])
        _start(dv.at[here], dv_s.at[here], load_sems.at[TWO, i])
    later = ((turned, at_s), (x, x_s), (dh, dh_s), (qkv, w_s))
    for i, (src, dst) in enumerate(later):
        _start(src, dst, load_sems.at[THREE, i])
    _greet(at)

    @pl.when(at["k"] == ZERO)
    def _():
        sums.give(MIXED, dwo)

    @pl.when(at["k"] == ONE)
    def _():
        sums.keep(MIXED, dwo)

    for i in range(blocks):
        here = slice(i * BLOCK, i * BLOCK + BLOCK)
        _arrived(dq_s.at[:, here], load_sems.at[ZERO, i])
        _arrived(dk_s.at[here], load_sems.at[ONE, i])
        _arrived(dv_s.at[here], load_sems.at[TWO, i])
        cos, sin = cos_ref[here, :], sin_ref[here, :]
        for m in range(heads + ONE):
            one = (dq_s[m, here, :] if m < heads else dk_s[here, :]).astype(F32)
            by_s[here, m * HEAD : (m + 1) * HEAD] = (one * cos - pltpu.roll(one, HEAD // TWO, 1) * sin).astype(BF)
        by_s[here, (heads + ONE) * HEAD :] = dv_s[here, :]
    _arrived(at_s, load_sems.at[THREE, 0])
    for c in range(0, by_s.shape[ONE], WIDE):
        dw_s[:, :, :, :, c : c + WIDE] = _mm(at_s[...], by_s[:, c : c + WIDE]).astype(BF).reshape(*GRID, COLOURS, ROWS, WIDE)

    @pl.when(at["k"] == ZERO)
    def _():
        sums.own[0][...] = dw_s[...]

    @pl.when(at["k"] == ONE)
    def _():
        sums.give(MIXED, dw_s)
        sums.kept(MIXED)

    for i, (_, dst) in enumerate(later[1:]):
        _arrived(dst, load_sems.at[THREE, i + 1])
    w = w_s[...]

    def back(i):
        here = slice(i * BLOCK, i * BLOCK + BLOCK)
        da = _mt(by_s[here, :], w).astype(BF)
        dh_s[here, :] = (dh_s[here, :].astype(F32) + _norm_back(x_s[here, :], da)).astype(BF)
        _start(dh_s.at[here], dx_o.at[here], out_sem.at[i])

    for i in range(sums.STEPS):
        if i < blocks:
            back(i)
        sums.steps(i)
    sums.deal_out(1, *mates)
    out_s, in_s, mate_sems = mates
    sums.dealt(out_s, in_s, mate_sems)
    rows_o[...] = in_s[...]
    sums.all_sent()
    for i in range(blocks):
        _arrived(dh_s.at[slice(i * BLOCK, i * BLOCK + BLOCK)], out_sem.at[i])


def project_back(dq, dk, dv, cos, sin, x, dh, turned, qkv, dwo):
    n, d = x.shape
    width = qkv.shape[ONE]
    vmem, anywhere = pl.BlockSpec(memory_space=pltpu.VMEM), pl.BlockSpec(memory_space=pl.ANY)
    dma = pltpu.SemaphoreType.DMA
    return pl.pallas_call(
        _project_back,
        in_specs=[anywhere] * 3 + [vmem] * TWO + [anywhere] * 5,
        out_specs=[anywhere, vmem],
        out_shape=[jax.ShapeDtypeStruct(s, BF) for s in ((n, d), (8, 1, 8, WIDE))],
        scratch_shapes=[pltpu.VMEM(s, BF) for s in (dq.shape, dk.shape, dk.shape, (n, d), (n, d), (d, n), (d, width), (n, width),
                                                    (*GRID, COLOURS, ROWS, width))] + [dma((4, 4)), dma((4,))] + _sum_scratch((MIXED,)),
        compiler_params=pltpu.CompilerParams(collective_id=2, has_side_effects=True, vmem_limit_bytes=VMEM),
        name="project_back",
    )(dq, dk, dv, cos, sin, x, dh, turned, qkv, dwo.reshape(*GRID, COLOURS, ROWS, -ONE))


def _deal(dx_ref, mixed_ref, wide_ref, down_ref, dx_o, wq_o, wk_o, wv_o, wo_o, wg_o, wu_o, wd_o):
    dx_o[...] = dx_ref[...]

    @pl.when(_first())
    def _():
        for j in range(MATES):
            for lo in (0, HEAD):
                found = _from_mixed((wq_o, wk_o, wv_o, wo_o), _columns(j) + lo)
                if found:
                    ref, first = found
                    ref[:, first : first + HEAD] = mixed_ref[j, 0, ZERO:SIX, lo : lo + HEAD]
            for n, ref in enumerate((wg_o, wu_o)):
                ref[:, _columns(j) : _columns(j) + WIDE] = wide_ref[j, n, ZERO:SIX, :]
        wd_o[...] = down_ref[...]


def deal(dx, mixed, wide, down):
    n, d = dx.shape
    outs = ((6, DIM), (6, HEAD), (6, HEAD), (6, DIM), (6, FULL), (6, FULL), (ROWS, DIM))
    return _call(_deal, "deal", n // BLOCK, [(dx, *_rows(BLOCK, d))] + [(a, *_all(*a.shape)) for a in (mixed, wide, down)],
                 [((n, d), BF, *_rows(BLOCK, d))] + [(shape, BF, *_all(*shape)) for shape in outs])


def solution(mesh):
    def step(x, dy, *weights):
        x, dy = x[0], dy[0]
        qkv, wo, gate, up, down, at, dyt, q, k, v, o, cos, sin, lse = advance(x, dy, *(w[0] for w in weights))
        dh, do, delta, dwo, dwg, dwu, dwd = middle(o, x, dy, dyt, wo, gate, up, down)
        dq, dk, dv, wide, tall = attend_back(q, k, v, do, lse, delta, dwg, dwu, dwd)
        dx, mixed = project_back(dq, dk, dv, cos, sin, x, dh, at, qkv, dwo)
        return tuple(g[None] for g in deal(dx, mixed, wide, tall))

    states, cut = P(("rep", "dp"), None, None), P(None, "dp", None)
    return jax.shard_map(
        step,
        mesh=mesh,
        in_specs=(states, states) + (cut,) * 7,
        out_specs=(states,) + (P("rep", "dp", None),) * 7,
        check_vma=False,
    )
```

```python
import jax
import jax.numpy as jnp
import numpy as np
from jax import lax
from jax.experimental import pallas as pl
from jax.experimental.pallas import tpu as pltpu
from jax.sharding import PartitionSpec as P

HEAD = 128
THETA = 10000
EPS = 1e-6
ZERO, ONE, HALF, FULL, DIM, WIDE, ROWS, MATES, PLACES, SIX, TWO, THREE, COLOURS = 0, 1, 1024, 2048, 768, 256, 16, 8, 4, 6, 2, 3, 3
GRID = (PLACES, PLACES)
NEG = -1e30
HIDDEN = 2 * NEG
LOG2E = 1.4426950408889634
VMEM = 56 * 2**20
BLOCK = 512
BF, F32 = jnp.bfloat16, jnp.float32
SCALE = HEAD**-0.5
E = SCALE * LOG2E


def _dot(a, b, ca, cb):
    return lax.dot_general(a, b, (((ca,), (cb,)), ((), ())), preferred_element_type=F32)


def _mm(a, b):
    return _dot(a, b, ONE, ZERO)


def _mt(a, b):
    return _dot(a, b, ONE, ONE)


def _first():
    return pl.program_id(ZERO) == ZERO


def _last():
    return pl.program_id(ZERO) == pl.num_programs(ZERO) - ONE


def _visible(keys, queries, first):
    return lax.broadcasted_iota(jnp.int32, (keys, queries), 0) <= lax.broadcasted_iota(jnp.int32, (keys, queries), 1) + first


def _call(kernel, name, grid, ins, outs, scratch=(), flops=0):
    given = [a for a, _, _ in ins]
    moved = sum(a.size * a.dtype.itemsize for a in given)
    return pl.pallas_call(
        kernel,
        grid=(grid,),
        in_specs=[pl.BlockSpec(block, index) for _, block, index in ins],
        out_specs=[pl.BlockSpec(block, index) for _, _, block, index in outs],
        out_shape=[jax.ShapeDtypeStruct(shape, dtype) for shape, dtype, _, _ in outs],
        scratch_shapes=list(scratch),
        compiler_params=pltpu.CompilerParams(dimension_semantics=("arbitrary",), vmem_limit_bytes=VMEM),
        cost_estimate=pl.CostEstimate(flops=flops, transcendentals=0, bytes_accessed=2 * moved),
        name=name,
    )(*given)


def _rows(*shape):
    return shape, lambda i: (i,) + (0,) * (len(shape) - 1)


def _all(*shape):
    return shape, lambda i: (0,) * len(shape)


def _norm(h):
    wide = h.astype(F32)
    return (wide * lax.rsqrt(jnp.mean(wide * wide, -1, keepdims=ONE) + EPS)).astype(BF)


def _norm_back(h, g):
    wide, g = h.astype(F32), g.astype(F32)
    scale = lax.rsqrt(jnp.mean(wide * wide, -1, keepdims=ONE) + EPS)
    return scale * (g - wide * (scale * scale * jnp.mean(g * wide, -1, keepdims=ONE)))


FEED_STEP = 512
PIECE = 512
ROWS_AT_ONCE = DIM


def _middle(o, x, dy, dyt, wo, wg_ref, wu_ref, wd_ref, dh_o, do_o, delta_ref, dwo_ref, dwg_ref, dwu_ref, dwd_ref,
            o_s, h_s, dy_s, dyt_s, wo_s, b_s, bt_s, db_s, z_s, load_sems, out_sems):
    f = wg_ref.shape[ONE]
    heads, n, _ = o_s.shape
    d = h_s.shape[ONE]
    pieces = [slice(lo, lo + BLOCK) for lo in range(0, n, BLOCK)]

    @pl.when(_first())
    def _():
        pltpu.make_async_copy(wo, wo_s, load_sems.at[TWO, 0]).start()
        for i, here in enumerate(pieces):
            pltpu.make_async_copy(o.at[:, here], o_s.at[:, here], load_sems.at[ZERO, i]).start()
            pltpu.make_async_copy(x.at[here], h_s.at[here], load_sems.at[ONE, i]).start()
        pltpu.make_async_copy(dy, dy_s, load_sems.at[TWO, 1]).start()
        pltpu.make_async_copy(dyt, dyt_s, load_sems.at[TWO, 2]).start()
        pltpu.make_async_copy(wo, wo_s, load_sems.at[TWO, 0]).wait()

        def open_(i, _):
            here = pl.ds(pl.multiple_of(i * BLOCK, BLOCK), BLOCK)
            pltpu.make_async_copy(o.at[:, here], o_s.at[:, here], load_sems.at[ZERO, i]).wait()
            pltpu.make_async_copy(x.at[here], h_s.at[here], load_sems.at[ONE, i]).wait()
            heard = jnp.concatenate([o_s[m, here, :] for m in range(heads)], axis=ONE)
            h = h_s[here, :] + _mm(heard, wo_s[:, :d]).astype(BF)
            h_s[here, :] = h
            b = _norm(h)
            b_s[here, :] = b
            bt_s[:, here] = b.T

        lax.fori_loop(0, n // BLOCK, open_, None)
        db_s[...] = jnp.zeros_like(db_s)
        pltpu.make_async_copy(dy, dy_s, load_sems.at[TWO, 1]).wait()
        pltpu.make_async_copy(dyt, dyt_s, load_sems.at[TWO, 2]).wait()

    both = jnp.concatenate([wg_ref[...], wu_ref[...]], axis=ONE)

    def forward(i):
        here = slice(i * PIECE, i * PIECE + PIECE)
        return _mm(b_s[here, :], both), _mt(dy_s[here, :], wd_ref[...])

    def piece(i, gate_up, dmid):
        here = slice(i * PIECE, i * PIECE + PIECE)
        gate, up, dmid = gate_up[:, :f], gate_up[:, f:], dmid.astype(BF).astype(F32)
        sig = 0.5 * jnp.tanh(0.5 * gate) + 0.5
        silu = gate * sig
        z_s[here, 2 * f :] = (silu * up).astype(BF)
        z_s[here, f : 2 * f] = (dmid * silu).astype(BF)
        z_s[here, :f] = (dmid * up * (sig + silu * (1 - sig))).astype(BF)

    def to_b(i):
        here = slice(i * PIECE, i * PIECE + PIECE)
        db_s[here, :] += _mt(z_s[here, : 2 * f], both)

    ahead = forward(0)
    for i in range(n // PIECE):
        now, ahead = ahead, forward(i + ONE) if i + 1 < n // PIECE else None
        piece(i, *now)
        if i:
            to_b(i - 1)
    to_b(n // PIECE - 1)

    def weights(i, _):
        here = pl.ds(pl.multiple_of(i * ROWS_AT_ONCE, ROWS_AT_ONCE), ROWS_AT_ONCE)
        dw = _mm(bt_s[here, :], z_s[:, : 2 * f])
        dwg_ref[here, :] = dw[:, :f].astype(BF)
        dwu_ref[here, :] = dw[:, f:].astype(BF)
        dwd_ref[:, here] = _mm(dyt_s[here, :], z_s[:, 2 * f :]).astype(BF).T

    lax.fori_loop(0, d // ROWS_AT_ONCE, weights, None)

    @pl.when(_last())
    def _():

        def back(i, _):
            here = pl.ds(pl.multiple_of(i * BLOCK, BLOCK), BLOCK)
            dy_s[here, :] = (dy_s[here, :].astype(F32) + _norm_back(h_s[here, :], db_s[here, :].astype(BF))).astype(BF)
            pltpu.make_async_copy(dy_s.at[here], dh_o.at[here], out_sems.at[ZERO, i]).start()

        lax.fori_loop(0, n // BLOCK, back, None)

        def by_wo(m, _):
            here = pl.ds(pl.multiple_of(m * HEAD, HEAD), HEAD)
            dwo_ref[here, :d] = _dot(o_s[m], dy_s[...], 0, 0).astype(BF)

        lax.fori_loop(0, heads, by_wo, None)
        dwo_ref[:, d:] = jnp.zeros_like(dwo_ref[:, d:])

        def by_o(i, _):
            here = pl.ds(pl.multiple_of(i * BLOCK, BLOCK), BLOCK)
            do = _mt(dy_s[here, :], wo_s[:, :d]).astype(BF)
            for m in range(heads):
                mine = do[:, m * HEAD : (m + 1) * HEAD]
                delta_ref[m : m + 1, here] = (mine.astype(F32) * o_s[m, here, :].astype(F32)).T.sum(axis=ZERO, keepdims=ONE)
                o_s[m, here, :] = mine
            pltpu.make_async_copy(o_s.at[:, here], do_o.at[:, here], out_sems.at[ONE, i]).start()

        lax.fori_loop(0, n // BLOCK, by_o, None)
        for i, here in enumerate(pieces):
            pltpu.make_async_copy(dy_s.at[here], dh_o.at[here], out_sems.at[ZERO, i]).wait()
            pltpu.make_async_copy(o_s.at[:, here], do_o.at[:, here], out_sems.at[ONE, i]).wait()


def middle(o, x, dy, dyt, wo, gate, up, down):
    n, d = x.shape
    heads, f, ff = o.shape[ZERO], FEED_STEP, gate.shape[ONE]
    anywhere = pl.BlockSpec(memory_space=pl.ANY)
    cols, rows = pl.BlockSpec((d, f), lambda i: (0, i)), pl.BlockSpec((f, d), lambda i: (i, 0))
    dma = pltpu.SemaphoreType.DMA
    return pl.pallas_call(
        _middle,
        grid=(ff // f,),
        in_specs=[anywhere] * 5 + [cols, cols, rows],
        out_specs=[anywhere] * TWO + [pl.BlockSpec((heads, n), lambda i: (0, 0)), pl.BlockSpec(wo.shape, lambda i: (0, 0)), cols, cols, rows],
        out_shape=[jax.ShapeDtypeStruct(s, t) for s, t in (((n, d), BF), (o.shape, BF), ((heads, n), F32), (wo.shape, BF),
                                                           (gate.shape, BF), (up.shape, BF), (down.shape, BF))],
        scratch_shapes=[pltpu.VMEM(s, BF) for s in (o.shape, (n, d), (n, d), (d, n), wo.shape, (n, d), (d, n))]
        + [pltpu.VMEM((n, d), F32), pltpu.VMEM((n, 3 * f), BF), dma((3, 4)), dma((2, 4))],
        compiler_params=pltpu.CompilerParams(dimension_semantics=("arbitrary",), vmem_limit_bytes=VMEM),
        cost_estimate=pl.CostEstimate(flops=ROWS * n * d * ff, transcendentals=0, bytes_accessed=2 * n * d * 20),
        name="middle",
    )(o, x, dy, dyt, wo, gate, up, down)


RING = 4
ORDERS = ("xyz", "yzx", "zxy")
MIXED, GATE, UP, DOWN = range(PLACES)


def _place():
    me = lax.axis_index("dp")
    return {"x": me // 32, "y": me // 8 % RING, "z": me // TWO % RING, "k": me % TWO}


def _device(at, **other):
    at = {**at, **other}
    return {"dp": ((at["x"] * 4 + at["y"]) * 4 + at["z"]) * TWO + at["k"]}


def _beside(at, axis, by):
    return _device(at, **{axis: (at[axis] + by) % RING})


def _mate(at, by):
    other = (at["z"] * TWO + at["k"] + by) % 8
    return _device(at, z=other // TWO, k=other % TWO)


def _greet(at):
    barrier = pltpu.get_barrier_semaphore()
    peers = [_beside(at, axis, by) for axis in "xy" for by in range(1, RING)] + [_mate(at, by) for by in range(ONE, MATES)]
    for peer in peers:
        pl.semaphore_signal(barrier, inc=1, device_id=peer, device_id_type=pl.DeviceIdType.MESH)
    pl.semaphore_wait(barrier, len(peers))


def _remote(src, dst, send, recv, device):
    pltpu.make_async_remote_copy(src_ref=src, dst_ref=dst, send_sem=send, recv_sem=recv, device_id=device,
                                 device_id_type=pl.DeviceIdType.MESH).start()


def _start(src, dst, sem):
    pltpu.make_async_copy(src, dst, sem).start()


def _arrived(ref, sem):
    pltpu.make_async_copy(ref, ref, sem).wait()


def _lanes(z, lo=0, n=WIDE):
    return pl.ds(pl.multiple_of(z * WIDE + lo, HEAD), n)


def _half_columns(k):
    return pl.ds(pl.multiple_of(k * HALF, HALF), HALF)


def _tokens(i, first=0, many=BLOCK):
    return pl.ds(i * BLOCK + first if isinstance(i, int) else pl.multiple_of(i * BLOCK + first, BLOCK // TWO), many)


def _columns(j):
    return (j % TWO) * HALF + (j // TWO) * WIDE


STARTS = (0, DIM, 896, HALF)


def _from_mixed(refs, lo):
    return next(((ref, lo - base) for ref, base in zip(refs, STARTS, strict=ONE) if 0 <= lo - base < ref.shape[ONE]), None)


def _advance(wq, wk, wv, wo, wg, wu, wd, freq, x, dy, qkv_o, wo_o, gate_o, up_o, down_o, at_o, dyt_o, q_o, k_o, v_o, o_o, cos_o, sin_o, lse_o,
             out_s, in_s, ws, wds, mixed_s, x_s, dy_s, a_s, at_s, dyt_s, q_s, k_s, v_s, o_s, top_s, mix_s, cos_s, sin_s,
             mate_sems, ring_send, ring_recv, pair_sems, own_sem, load_sems, store_sems):
    at = _place()
    seat = at["z"] * TWO + at["k"]
    outs = (None, gate_o, up_o)
    heads = q_s.shape[ZERO]
    blocks = x_s.shape[ZERO] // BLOCK
    sent = {}
    kept = []

    def send(key, ref, dst, sem, recv, device):
        _remote(ref(), dst(), sem(), recv, device)
        sent[key] = ref, sem

    def store(src, dst, n):
        _start(src, dst, store_sems.at[n])
        kept.append((src, store_sems.at[n]))

    _start(x, x_s, load_sems.at[ZERO])
    _start(dy, dy_s, load_sems.at[ONE])
    for j in range(MATES):
        for lo in (0, HEAD):
            found = _from_mixed((wq, wk, wv, wo), _columns(j) + lo)
            if found:
                ref, first = found
                out_s[j, MIXED, ZERO:SIX, lo : lo + HEAD] = ref[:, first : first + HEAD]
            else:
                out_s[j, MIXED, ZERO:SIX, lo : lo + HEAD] = jnp.zeros((6, HEAD), BF)
        for t, ref in ((GATE, wg), (UP, wu)):
            out_s[j, t, ZERO:SIX, :] = ref[:, _columns(j) : _columns(j) + WIDE]
        out_s[j, :, SIX:MATES, :] = jnp.zeros((3, 2, WIDE), BF)
    _greet(at)
    for by in range(ONE, MATES):
        send(by, lambda by=by: out_s.at[(seat + by) % 8], lambda: in_s.at[seat], lambda by=by: mate_sems.at[ZERO, by], mate_sems.at[ONE, by],
             _mate(at, by))
    in_s[seat] = out_s[seat]
    for c in range(COLOURS):
        wds[at["x"], at["y"], at["z"], :, WIDE * c : WIDE * c + WIDE] = wd[:, WIDE * c : WIDE * c + WIDE]

    def region(t, c, fixed, half=None):
        x, y = (fixed.get(axis, slice(None)) for axis in "xy")
        if t != DOWN and "z" not in fixed:
            return ws.at[t, x, y, c, :, slice(None) if half is None else slice(512 * half, 512 * half + 512)]
        lo, n = (0, WIDE) if half is None else (HEAD * half, HEAD)
        if t == DOWN:
            return wds.at[x, y, fixed.get("z", slice(None)), :, WIDE * c + lo : WIDE * c + lo + n]
        return ws.at[t, x, y, c, :, _lanes(fixed["z"], lo, n)]

    def known(c, phase, place):
        order = ORDERS[c][::-1]
        return {**{a: at[a] for a in order[phase + 1 :]}, order[phase]: place}

    def hop(t, c, phase, slot, by, here):
        key = t, c, phase, slot
        send(key, here, here, lambda: ring_send.at[key], ring_recv.at[key], _beside(at, ORDERS[c][::-1][phase], by))

    def send_own(phase, *ts):
        for t in ts:
            for c in range(COLOURS):
                for slot, by in enumerate((1, 2, 3) if phase < 2 else (1, 3)):
                    hop(t, c, phase, slot, by, lambda t=t, c=c: region(t, c, known(c, phase, at[ORDERS[c][::-1][phase]])))

    def pass_on(phase, *ts):
        for t in ts:
            for c in range(COLOURS):
                axis = ORDERS[c][::-1][phase]
                for slot, by in ((0, 3), (1, 1)):

                    def here(half, t=t, c=c, axis=axis, by=by):
                        return region(t, c, known(c, phase, (at[axis] + by) % RING), half)

                    _arrived(here(None), ring_recv.at[t, c, phase, slot])
                    hop(t, c, phase, 2 + slot, RING - by, lambda here=here, slot=slot: here(1 - slot))

    def finish(phase, *ts):
        for t in ts:
            for c in range(COLOURS):
                place = at[ORDERS[c][::-1][phase]]
                for slot in range(COLOURS) if phase < 2 else (2, 3):
                    by, half = (3 - slot, None) if phase < 2 else (2, 3 - slot)
                    _arrived(region(t, c, known(c, phase, (place + by) % RING), half), ring_recv.at[t, c, phase, slot])

    partner = _device(at, k=ONE - at["k"])

    def half(t, k):
        return down_o.at[:, :, :, k] if t == DOWN else outs[t].at[:, :, :, :, _half_columns(k)]

    def to_result(t):
        src = wds if t == DOWN else ws.at[t]
        _remote(src, half(t, at["k"]), pair_sems.at[ZERO, t], pair_sems.at[ONE, t], partner)
        _start(src, half(t, at["k"]), own_sem.at[t])

    def prepare(i):
        here = slice(i * BLOCK, i * BLOCK + BLOCK)
        a = _norm(x_s[here, :])
        a_s[here, :] = a
        at_s[:, here] = a.T

    def turn(i):
        here = slice(i * BLOCK, i * BLOCK + BLOCK)
        dyt_s[:, here] = dy_s[here, :].T

    def tables():
        half, rows = HEAD // TWO, 64
        place = lax.broadcasted_iota(jnp.int32, (rows, HEAD), 0).astype(F32)
        left = lax.broadcasted_iota(jnp.int32, (rows, HEAD), 1) < half
        near, far = place * freq[...], place[: x_s.shape[ZERO] // rows] * rows * freq[: x_s.shape[ZERO] // rows]
        near_cos, near_sin, far_cos, far_sin = jnp.cos(near), jnp.sin(near), jnp.cos(far), jnp.sin(far)
        for n in range(x_s.shape[ZERO] // rows):
            c, s = far_cos[n : n + ONE, :], far_sin[n : n + ONE, :]
            cos_s[n * rows : n * rows + rows, :] = near_cos * c - near_sin * s
            sin = near_sin * c + near_cos * s
            sin_s[n * rows : n * rows + rows, :] = jnp.where(left, -sin, sin)
        store(cos_s, cos_o, 6)
        store(sin_s, sin_o, 7)

    def project(i):
        here = slice(i * BLOCK, i * BLOCK + BLOCK)
        t = _mm(a_s[here, :], mixed_s[...].reshape(a_s.shape[ONE], -1)).astype(BF)
        cos, sin = cos_s[here, :], sin_s[here, :]
        for n in range(heads + ONE):
            one = t[:, n * HEAD : (n + ONE) * HEAD].astype(F32)
            one = (one * cos + pltpu.roll(one, HEAD // TWO, 1) * sin).astype(BF)
            if n < heads:
                q_s[n, here, :] = one
            else:
                k_s[here, :] = one
        v_s[here, :] = t[:, (heads + ONE) * HEAD :]

    rest = (GATE, UP, DOWN)
    _arrived(x_s, load_sems.at[ZERO])
    prepare(0)
    for by in range(ONE, MATES):
        _arrived(in_s.at[ZERO], mate_sems.at[ONE, by])
    for t in range(COLOURS):
        rows = jnp.concatenate([in_s[j, t].astype(F32)[ZERO:SIX, :] for j in range(MATES)], axis=ZERO).astype(BF)
        for c in range(COLOURS):
            ws[t, at["x"], at["y"], c, :, _lanes(at["z"])] = rows[ROWS * c : ROWS * c + ROWS, :]
    send_own(0, MIXED)
    send_own(0, *rest)
    prepare(1)
    prepare(2)
    finish(0, MIXED)
    send_own(1, MIXED)
    finish(0, *rest)
    send_own(1, *rest)
    prepare(3)
    store(at_s, at_o, 0)
    tables()
    finish(1, MIXED)
    send_own(2, MIXED)
    finish(1, *rest)
    send_own(2, GATE)
    _arrived(dy_s, load_sems.at[ONE])
    turn(0)
    turn(1)
    pass_on(2, MIXED)
    send_own(2, UP)
    turn(2)
    turn(3)
    store(dyt_s, dyt_o, 1)
    finish(2, MIXED)

    @pl.when(at["k"] == ZERO)
    def _():
        _remote(ws.at[MIXED], mixed_s, pair_sems.at[ZERO, MIXED], pair_sems.at[ONE, MIXED], partner)
        mixed_s[...] = ws[MIXED]

    @pl.when(at["k"] == ONE)
    def _():
        _remote(ws.at[MIXED], wo_o, pair_sems.at[ZERO, MIXED], pair_sems.at[ONE, MIXED], partner)
        _start(ws.at[MIXED], wo_o, own_sem.at[MIXED])

    pass_on(2, GATE)
    send_own(2, DOWN)
    _arrived(mixed_s, pair_sems.at[ONE, MIXED])
    store(mixed_s, qkv_o, 2)
    for i in range(blocks):
        project(i)
        if i == 1:
            pass_on(2, UP)
    store(q_s, q_o, 3)
    store(k_s, k_o, 4)
    store(v_s, v_o, 5)

    def between(n):
        @pl.when(n == 0)
        def _():
            finish(2, GATE)
            to_result(GATE)

        @pl.when(n == 1)
        def _():
            pass_on(2, DOWN)

        @pl.when(n == 2)
        def _():
            finish(2, UP)
            to_result(UP)

        @pl.when(n == 3)
        def _():
            finish(2, DOWN)
            to_result(DOWN)

    ones = jnp.ones((8, BLOCK), BF)

    def block(iq, j, first=0, queries=BLOCK, keys=BLOCK, masked=False):
        here, mine, cols = _tokens(j, 0, keys), _tokens(iq, first, queries), slice(first, first + queries)
        scores = [_mt(k_s[here, :], q_s[n, mine, :]) for n in range(heads)]
        weights, keeps = [], []
        for n, s in enumerate(scores):
            if masked:
                s = jnp.where(_visible(keys, queries, first), s, HIDDEN)
            old = top_s[n : n + ONE, cols]
            top = jnp.maximum(old, s.max(axis=ZERO, keepdims=ONE))
            top_s[n : n + ONE, cols] = top
            weights.append(jnp.exp2((s - top) * E).astype(BF))
            keeps.append(jnp.exp2((old - top) * E))
        values = jnp.concatenate([v_s[here, :].T, ones[:, :keys]], axis=ZERO)
        for n, (p, keep) in enumerate(zip(weights, keeps, strict=ONE)):
            mix_s[n, :, cols] = mix_s[n, :, cols] * keep + _mm(values, p)

    def row(iq, _):
        top_s[...] = jnp.full(top_s.shape, NEG, F32)
        mix_s[...] = jnp.zeros(mix_s.shape, F32)

        def step(j, _):
            block(iq, j)
            between(iq * (iq + ONE) // TWO + j)

        lax.fori_loop(0, iq, step, None)
        for first in (0, BLOCK // TWO):
            block(iq, iq, first, BLOCK // TWO, first + BLOCK // TWO, True)
        between(iq * (iq + ONE) // TWO + iq)
        mine = _tokens(iq)
        for n in range(heads):
            total = mix_s[n, HEAD : HEAD + 1, :]
            o_s[n, mine, :] = (mix_s[n, :HEAD, :] * (1 / total)).T.astype(BF)
            lse_o[n : n + ONE, mine] = top_s[n : n + ONE, :] * SCALE + jnp.log(total)
        _start(o_s.at[:, mine], o_o.at[:, mine], own_sem.at[4])

    lax.fori_loop(0, blocks, row, None)
    _arrived(o_s, own_sem.at[4])
    for ref, sem in sent.values():
        _arrived(ref(), sem())
    for t in (MIXED, *rest):
        src = wds if t == DOWN else ws.at[t]
        _arrived(src, pair_sems.at[ZERO, t])
        if t != MIXED:
            _arrived(src, pair_sems.at[ONE, t])
            _arrived(src, own_sem.at[t])

    @pl.when(at["k"] == ONE)
    def _():
        _arrived(ws.at[MIXED], own_sem.at[MIXED])

    for ref, sem in kept:
        _arrived(ref, sem)


def advance(x, dy, *shards):
    n, d = x.shape
    heads = d // HEAD
    half = HEAD // TWO
    freq = np.tile(float(THETA) ** (-np.arange(half) / half), (half, 2)).astype(np.float32)
    vmem, anywhere = pl.BlockSpec(memory_space=pltpu.VMEM), pl.BlockSpec(memory_space=pl.ANY)
    wide, narrow = (*GRID, COLOURS, ROWS, FULL), (*GRID, COLOURS, ROWS, HALF)
    tall = (*GRID, PLACES, 2, ROWS, DIM)
    many, one = (heads, n, HEAD), (n, HEAD)
    shapes = (narrow, narrow, wide, wide, tall, (d, n), (d, n), many, one, one, many)
    dma = pltpu.SemaphoreType.DMA
    qkv, wo, gate, up, down, *rest = pl.pallas_call(
        _advance,
        in_specs=[vmem] * 8 + [anywhere] * 2,
        out_specs=[anywhere] * (len(shapes) + 2) + [vmem],
        out_shape=[jax.ShapeDtypeStruct(s, BF) for s in shapes] + [jax.ShapeDtypeStruct(s, F32) for s in (one, one, (heads, n))],
        scratch_shapes=[pltpu.VMEM(s, BF) for s in ((MATES, 3, MATES, WIDE), (MATES, 3, MATES, WIDE), (3, *narrow), (*GRID, PLACES, ROWS, DIM), narrow,
                                                    (n, d), (n, d), (n, d), (d, n), (d, n), many, one, one, many)]
        + [pltpu.VMEM(s, F32) for s in ((heads, BLOCK), (heads, HEAD + 8, BLOCK), one, one)]
        + [dma((2, 8)), dma((PLACES, COLOURS, COLOURS, PLACES)), dma((PLACES, COLOURS, COLOURS, PLACES)), dma((2, 4)), dma((5,)), dma((2,)), dma((8,))],
        compiler_params=pltpu.CompilerParams(collective_id=0, has_side_effects=True, vmem_limit_bytes=VMEM),
        name="advance",
    )(*shards, freq, x, dy)
    return qkv.reshape(d, -1), wo.reshape(d, -1), gate.reshape(d, -1), up.reshape(d, -1), down.reshape(-1, d), *rest


class _Sums:
    STEPS = 5

    def __init__(self, at, ts, own, theirs, bufs, total, down_o, ring_send, ring_recv, pair_sems, own_sems):
        self.at, self.ts, self.own, self.theirs, self.bufs, self.total, self.down_o = at, ts, own, theirs, bufs, total, down_o
        self.ring_send, self.ring_recv, self.pair_sems, self.own_sems = ring_send, ring_recv, pair_sems, own_sems
        self.partner = _device(at, k=ONE - at["k"])

    def give(self, t, ref):
        n = self.ts.index(t)
        _remote(ref, self.theirs[n], self.pair_sems.at[ZERO, n], self.pair_sems.at[ONE, n], self.partner)

    def keep(self, t, ref):
        n = self.ts.index(t)
        _start(ref, self.own[n], self.own_sems.at[n])

    def kept(self, t):
        n = self.ts.index(t)
        _arrived(self.own[n], self.own_sems.at[n])

    def term(self, n, c, phase, q, i, j):
        if phase:
            acc = self.bufs[phase - 1][-1]
            return acc[n, c, q, j] if phase == 1 else acc[n, c, q]
        place = dict(zip(ORDERS[c], (q, i, j), strict=ONE))
        x, y, z = (place[a] for a in "xyz")
        if self.ts[n] == DOWN:
            both = (ref[x, y, z, :, WIDE * c : WIDE * c + WIDE] for ref in (self.own[n], self.theirs[n]))
        else:
            both = (ref[x, y, c, :, _lanes(z)] for ref in (self.own[n], self.theirs[n]))
        return sum(b.astype(F32) for b in both)

    @staticmethod
    def over_cells(phase, act):
        if phase == 0:
            lax.fori_loop(0, 4, lambda i, _: [act(i, j, (i, j)) for j in range(PLACES)] and None, None)
        elif phase == 1:
            for j in range(PLACES):
                act(0, j, (j,))
        else:
            act(0, 0, ())

    def hop(self, n, c, phase, slot, by, src, dst):
        _remote(src, dst, self.ring_send.at[n, c, phase, slot], self.ring_recv.at[n, c, phase, slot], _beside(self.at, ORDERS[c][phase], by))

    def near(self, c, phase, by):
        return (self.at[ORDERS[c][phase]] + by) % RING

    def begin(self, n, c, phase):
        to, into = self.bufs[phase][:2]
        places = [self.near(c, phase, by) for by in (1, 2, 3)]

        def act(i, j, where):
            above, opposite, below = (self.term(n, c, phase, q, i, j) for q in places)
            to[(n, c, 0, *where)] = jnp.concatenate([above[:, :HEAD], opposite[:, HEAD:]], axis=ONE).astype(BF)
            to[(n, c, 1, *where)] = jnp.concatenate([opposite[:, :HEAD], below[:, HEAD:]], axis=ONE).astype(BF)

        def straight(i, j, where):
            for slot, q in enumerate(places):
                to[(n, c, slot, *where)] = self.term(n, c, phase, q, i, j).astype(BF)

        self.over_cells(phase, straight if phase else act)
        for slot, by in enumerate((1, 2, 3) if phase else (1, 3)):
            self.hop(n, c, phase, slot, by, to.at[n, c, slot], into.at[n, c, slot])

    def relay(self, n, c, phase):
        into, over, last = self.bufs[phase][1:4]
        for slot, by, half in ((0, 1, slice(HEAD, WIDE)), (1, 3, slice(0, HEAD))):
            _arrived(into.at[n, c, slot], self.ring_recv.at[n, c, phase, slot])
            place = self.near(c, phase, by)

            def act(i, j, where, slot=slot, half=half, place=place):
                mine = self.term(n, c, phase, place, i, j)[:, half]
                over[(n, c, slot, *where)] = (mine + into[(n, c, slot, *where)][:, half].astype(F32)).astype(BF)

            self.over_cells(phase, act)
            self.hop(n, c, phase, 2 + slot, by, over.at[n, c, slot], last.at[n, c, slot])

    def finish(self, n, c, phase):
        into = self.bufs[phase][1]
        if phase:
            for slot in range(COLOURS):
                _arrived(into.at[n, c, slot], self.ring_recv.at[n, c, phase, slot])
        else:
            last = self.bufs[phase][3]
            for slot in (ZERO, ONE):
                _arrived(last.at[n, c, slot], self.ring_recv.at[n, c, phase, 2 + slot])

        def act(i, j, where):
            mine = self.term(n, c, phase, self.near(c, phase, 0), i, j)
            if phase:
                whole = sum((into[(n, c, slot, *where)].astype(F32) for slot in range(COLOURS)), mine)
            else:
                a = mine[:, :HEAD] + into[(n, c, 0, *where)][:, :HEAD].astype(F32) + last[(n, c, 1, *where)].astype(F32)
                b = mine[:, HEAD:] + into[(n, c, 1, *where)][:, HEAD:].astype(F32) + last[(n, c, 0, *where)].astype(F32)
                whole = jnp.concatenate([a, b], axis=ONE)
            if phase < 2:
                self.bufs[phase][-1][(n, c, *where)] = whole
            elif self.ts[n] == DOWN:
                self.down_o[:, WIDE * c : WIDE * c + WIDE] = whole.astype(BF)
            else:
                self.total[n, ROWS * c : ROWS * c + ROWS, :] = whole

        self.over_cells(phase, act)

    def step(self, n, what):
        if what == 0 and self.ts[n] != MIXED:
            _arrived(self.theirs[n], self.pair_sems.at[ONE, n])
        for c in range(COLOURS):
            if what == 0:
                self.begin(n, c, 0)
            elif what == 1:
                self.relay(n, c, 0)
            else:
                self.finish(n, c, what - 2)
                if what < 4:
                    self.begin(n, c, what - 1)

    def steps(self, slot):
        for n in range(len(self.ts)):
            if 0 <= slot - n < self.STEPS:
                self.step(n, slot - n)

    def all_sent(self):
        for n in range(len(self.ts)):
            if self.ts[n] != MIXED:
                _arrived(self.theirs[n], self.pair_sems.at[ZERO, n])
            for c in range(COLOURS):
                for phase, (to, _, *more) in enumerate(self.bufs):
                    for slot in range(COLOURS) if phase else (ZERO, ONE):
                        _arrived(to.at[n, c, slot], self.ring_send.at[n, c, phase, slot])
                        if not phase:
                            _arrived(more[0].at[n, c, slot], self.ring_send.at[n, c, phase, 2 + slot])

    def deal_out(self, wide, out_s, in_s, mate_sems):
        seat = self.at["z"] * TWO + self.at["k"]
        for n in range(wide):
            for j in range(MATES):
                out_s[j, n, ZERO:SIX, :] = self.total[n, 6 * j : 6 * j + 6, :].astype(BF)
                out_s[j, n, SIX:MATES, :] = jnp.zeros((2, WIDE), BF)
        for by in range(ONE, MATES):
            _remote(out_s.at[(seat + by) % 8], in_s.at[seat], mate_sems.at[ZERO, by], mate_sems.at[ONE, by], _mate(self.at, by))
        in_s[seat] = out_s[seat]

    @staticmethod
    def dealt(out_s, in_s, mate_sems):
        for by in range(ONE, MATES):
            _arrived(in_s.at[ZERO], mate_sems.at[ONE, by])
            _arrived(out_s.at[ZERO], mate_sems.at[ZERO, by])


def _sum_scratch(ts):
    count = len(ts)
    scratch = [pltpu.VMEM((*GRID, PLACES, ROWS, DIM) if t == DOWN else (*GRID, COLOURS, ROWS, HALF), BF) for t in ts for _ in range(2)]
    for left in ((4, 4), (4,), ()):
        first = left == (4, 4)
        scratch += [pltpu.VMEM((count, 3, 2 if first else 3, *left, ROWS, WIDE), BF)] * 2
        scratch += [pltpu.VMEM((count, 3, 2, *left, ROWS, HEAD), BF)] * TWO if first else []
        scratch += [pltpu.VMEM((count, 3, *left, ROWS, WIDE), F32)] if left else []
    wide = count - (DOWN in ts)
    dma = pltpu.SemaphoreType.DMA
    return scratch + [pltpu.VMEM((wide, 48, WIDE), F32)] + [pltpu.VMEM((8, wide, 8, WIDE), BF)] * TWO + [
        dma((count, COLOURS, COLOURS, PLACES)), dma((count, COLOURS, COLOURS, PLACES)), dma((2, count)), dma((count,)), dma((2, 8))]


def _sums(at, ts, refs, down_o):
    refs = list(refs)
    pairs = [(refs.pop(0), refs.pop(0)) for _ in ts]
    bufs = [[refs.pop(0) for _ in range(many)] for many in (5, 3, 2)]
    total, out_s, in_s, ring_send, ring_recv, pair_sems, own_sems, mate_sems = refs
    sums = _Sums(at, ts, [a for a, _ in pairs], [b for _, b in pairs], bufs, total, down_o, ring_send, ring_recv, pair_sems, own_sems)
    return sums, (out_s, in_s, mate_sems)


LATER = (GATE, UP, DOWN)


def _attend_back(q, k, v, do, lse_ref, delta_ref, gate, up, down, dq_o, dk_o, dv_o, rows_o, down_o,
                 q_s, k_s, v_s, do_s, dq_s, dk_s, dv_s, sum_s, load_sems, out_sem, *refs):
    at = _place()
    heads = q_s.shape[ZERO]
    blocks = q_s.shape[ONE] // BLOCK
    sums, mates = _sums(at, LATER, refs, down_o)
    _start(k, k_s, load_sems.at[ZERO, 0])
    _start(v, v_s, load_sems.at[ONE, 0])
    for i in range(blocks):
        _start(q.at[:, _tokens(i)], q_s.at[:, _tokens(i)], load_sems.at[TWO, i])
        _start(do.at[:, _tokens(i)], do_s.at[:, _tokens(i)], load_sems.at[THREE, i])
    _greet(at)

    def part(t, k):
        return down.at[:, :, :, k] if t == DOWN else (gate, up)[t - GATE].at[:, :, :, :, _half_columns(k)]

    for t in LATER:
        sums.give(t, part(t, ONE - at["k"]))
        sums.keep(t, part(t, at["k"]))
    sum_s[...] = jnp.zeros_like(sum_s)
    dk_s[...] = jnp.zeros_like(dk_s)
    dv_s[...] = jnp.zeros_like(dv_s)
    _arrived(k_s, load_sems.at[ZERO, 0])
    _arrived(v_s, load_sems.at[ONE, 0])

    def between(slot):
        if 0 <= slot < 3:
            sums.kept(LATER[slot])
        sums.steps(slot)
        if slot == sums.STEPS + 1:
            sums.deal_out(2, *mates)

    def block(iq, j, first=0, queries=BLOCK, keys=BLOCK):
        here, mine, cols = _tokens(j, 0, keys), _tokens(iq, first, queries), slice(first, first + queries)

        def some(half, _):
            group = [half * (heads // TWO) + n for n in range(heads // TWO)]
            scores = [_mt(k_s[here, :], q_s[n, mine, :]) for n in group]
            dps = [_mt(v_s[here, :], do_s[n, mine, :]) for n in group]
            for n, s, dp in zip(group, scores, dps, strict=ONE):
                p = jnp.exp2(s * E - lse_ref[pl.ds(n, 1), mine] * LOG2E)
                if iq == j:
                    p = jnp.where(_visible(keys, queries, first), p, 0.0)
                ds = (p * (dp - delta_ref[pl.ds(n, 1), mine])).astype(BF)
                dv_s[here, :] += _mm(p.astype(BF), do_s[n, mine, :])
                dk_s[here, :] += _mm(ds, q_s[n, mine, :])
                sum_s[n, :, cols] += _mm(k_s[here, :].T, ds)

        lax.fori_loop(0, 2, some, None)

    for iq in range(blocks):
        mine = _tokens(iq)
        _arrived(q_s.at[:, mine], load_sems.at[TWO, iq])
        _arrived(do_s.at[:, mine], load_sems.at[THREE, iq])
        for j in range(iq + ONE):
            if j < iq:
                block(iq, j)
            else:
                for first in (0, BLOCK // TWO):
                    block(iq, j, first, BLOCK // TWO, first + BLOCK // TWO)
            between(iq * (iq + ONE) // TWO + j - 1)
        for n in range(heads):
            dq_s[n, mine, :] = (sum_s[n] * SCALE).T.astype(BF)
        sum_s[...] = jnp.zeros_like(sum_s)
        _start(dq_s.at[:, mine], dq_o.at[:, mine], out_sem.at[ZERO])

    k_s[...] = (dk_s[...] * SCALE).astype(BF)
    v_s[...] = dv_s[...].astype(BF)
    _start(k_s, dk_o, out_sem.at[ONE])
    _start(v_s, dv_o, out_sem.at[2])
    out_s, in_s, mate_sems = mates
    sums.dealt(out_s, in_s, mate_sems)
    rows_o[...] = in_s[...]
    sums.all_sent()
    _arrived(dq_s, out_sem.at[ZERO])
    _arrived(k_s, out_sem.at[ONE])
    _arrived(v_s, out_sem.at[2])


def attend_back(q, k, v, do, lse, delta, gate, up, down):
    heads, n, _ = q.shape
    vmem, anywhere = pl.BlockSpec(memory_space=pltpu.VMEM), pl.BlockSpec(memory_space=pl.ANY)
    shapes = (q.shape, k.shape, k.shape, (8, 2, 8, WIDE), (ROWS, DIM))
    dma = pltpu.SemaphoreType.DMA
    return pl.pallas_call(
        _attend_back,
        in_specs=[anywhere] * 4 + [vmem] * TWO + [anywhere] * 3,
        out_specs=[anywhere] * 3 + [vmem] * 2,
        out_shape=[jax.ShapeDtypeStruct(s, BF) for s in shapes],
        scratch_shapes=[pltpu.VMEM(s, BF) for s in (q.shape, k.shape, k.shape, q.shape, q.shape)]
        + [pltpu.VMEM(s, F32) for s in (k.shape, k.shape, (heads, HEAD, BLOCK))] + [dma((4, 4)), dma((3,))] + _sum_scratch(LATER),
        compiler_params=pltpu.CompilerParams(collective_id=1, has_side_effects=True, vmem_limit_bytes=VMEM),
        name="attend_back",
    )(q, k, v, do, lse, delta, gate.reshape(*GRID, COLOURS, ROWS, -ONE), up.reshape(*GRID, COLOURS, ROWS, -ONE), down.reshape(*GRID, PLACES, 2, ROWS, DIM))


def _project_back(dq, dk, dv, cos_ref, sin_ref, x, dh, turned, qkv, dwo, dx_o, rows_o,
                  dq_s, dk_s, dv_s, x_s, dh_s, at_s, w_s, by_s, dw_s, load_sems, out_sem, *refs):
    at = _place()
    heads, n, _ = dq_s.shape
    blocks = n // BLOCK
    sums, mates = _sums(at, (MIXED,), refs[:-1], None)
    quarter_sems = refs[-1]
    quarters = [(Ellipsis, slice(lo, lo + WIDE)) for lo in range(0, by_s.shape[ONE], WIDE)]

    def give(ref, i):
        _remote(ref.at[quarters[i]], sums.theirs[0].at[quarters[i]], quarter_sems.at[ZERO, i], quarter_sems.at[ONE, i], sums.partner)

    for i in range(blocks):
        here = _tokens(i)
        _start(dq.at[:, here], dq_s.at[:, here], load_sems.at[ZERO, i])
        _start(dk.at[here], dk_s.at[here], load_sems.at[ONE, i])
        _start(dv.at[here], dv_s.at[here], load_sems.at[TWO, i])
    later = ((turned, at_s), (x, x_s), (dh, dh_s), (qkv, w_s))
    for i, (src, dst) in enumerate(later):
        _start(src, dst, load_sems.at[THREE, i])
    _greet(at)

    @pl.when(at["k"] == ZERO)
    def _():
        for i in range(len(quarters)):
            give(dwo, i)

    @pl.when(at["k"] == ONE)
    def _():
        sums.keep(MIXED, dwo)

    for i in range(blocks):
        here = slice(i * BLOCK, i * BLOCK + BLOCK)
        _arrived(dq_s.at[:, here], load_sems.at[ZERO, i])
        _arrived(dk_s.at[here], load_sems.at[ONE, i])
        _arrived(dv_s.at[here], load_sems.at[TWO, i])
        cos, sin = cos_ref[here, :], sin_ref[here, :]
        for m in range(heads + ONE):
            one = (dq_s[m, here, :] if m < heads else dk_s[here, :]).astype(F32)
            by_s[here, m * HEAD : (m + 1) * HEAD] = (one * cos - pltpu.roll(one, HEAD // TWO, 1) * sin).astype(BF)
        by_s[here, (heads + ONE) * HEAD :] = dv_s[here, :]
    _arrived(at_s, load_sems.at[THREE, 0])
    for i, part in enumerate(quarters):
        dw_s[part] = _mm(at_s[...], by_s[part]).astype(BF).reshape(*GRID, COLOURS, ROWS, WIDE)
        pl.when(at["k"] == ONE)(lambda i=i: give(dw_s, i))

    @pl.when(at["k"] == ZERO)
    def _():
        sums.own[0][...] = dw_s[...]

    @pl.when(at["k"] == ONE)
    def _():
        sums.kept(MIXED)

    for i, (_, dst) in enumerate(later[1:]):
        _arrived(dst, load_sems.at[THREE, i + 1])
    w = w_s[...]

    def back(i):
        here = slice(i * BLOCK, i * BLOCK + BLOCK)
        da = _mt(by_s[here, :], w).astype(BF)
        dh_s[here, :] = (dh_s[here, :].astype(F32) + _norm_back(x_s[here, :], da)).astype(BF)
        _start(dh_s.at[here], dx_o.at[here], out_sem.at[i])

    for i in range(sums.STEPS):
        if i < blocks:
            back(i)
        if i == 0:
            for j, part in enumerate(quarters):
                _arrived(sums.theirs[0].at[part], quarter_sems.at[ONE, j])
        sums.steps(i)
    sums.deal_out(1, *mates)
    out_s, in_s, mate_sems = mates
    sums.dealt(out_s, in_s, mate_sems)
    rows_o[...] = in_s[...]
    sums.all_sent()
    for j, part in enumerate(quarters):
        _arrived(dw_s.at[part], quarter_sems.at[ZERO, j])
    for i in range(blocks):
        _arrived(dh_s.at[slice(i * BLOCK, i * BLOCK + BLOCK)], out_sem.at[i])


def project_back(dq, dk, dv, cos, sin, x, dh, turned, qkv, dwo):
    n, d = x.shape
    width = qkv.shape[ONE]
    vmem, anywhere = pl.BlockSpec(memory_space=pltpu.VMEM), pl.BlockSpec(memory_space=pl.ANY)
    dma = pltpu.SemaphoreType.DMA
    return pl.pallas_call(
        _project_back,
        in_specs=[anywhere] * 3 + [vmem] * TWO + [anywhere] * 5,
        out_specs=[anywhere, vmem],
        out_shape=[jax.ShapeDtypeStruct(s, BF) for s in ((n, d), (8, 1, 8, WIDE))],
        scratch_shapes=[pltpu.VMEM(s, BF) for s in (dq.shape, dk.shape, dk.shape, (n, d), (n, d), (d, n), (d, width), (n, width),
                                                    (*GRID, COLOURS, ROWS, width))] + [dma((4, 4)), dma((4,))] + _sum_scratch((MIXED,)) + [dma((2, 4))],
        compiler_params=pltpu.CompilerParams(collective_id=2, has_side_effects=True, vmem_limit_bytes=VMEM),
        name="project_back",
    )(dq, dk, dv, cos, sin, x, dh, turned, qkv, dwo.reshape(*GRID, COLOURS, ROWS, -ONE))


def _deal(dx_ref, mixed_ref, wide_ref, down_ref, dx_o, wq_o, wk_o, wv_o, wo_o, wg_o, wu_o, wd_o):
    dx_o[...] = dx_ref[...]

    @pl.when(_first())
    def _():
        for j in range(MATES):
            for lo in (0, HEAD):
                found = _from_mixed((wq_o, wk_o, wv_o, wo_o), _columns(j) + lo)
                if found:
                    ref, first = found
                    ref[:, first : first + HEAD] = mixed_ref[j, 0, ZERO:SIX, lo : lo + HEAD]
            for n, ref in enumerate((wg_o, wu_o)):
                ref[:, _columns(j) : _columns(j) + WIDE] = wide_ref[j, n, ZERO:SIX, :]
        wd_o[...] = down_ref[...]


def deal(dx, mixed, wide, down):
    n, d = dx.shape
    outs = ((6, DIM), (6, HEAD), (6, HEAD), (6, DIM), (6, FULL), (6, FULL), (ROWS, DIM))
    return _call(_deal, "deal", n // BLOCK, [(dx, *_rows(BLOCK, d))] + [(a, *_all(*a.shape)) for a in (mixed, wide, down)],
                 [((n, d), BF, *_rows(BLOCK, d))] + [(shape, BF, *_all(*shape)) for shape in outs])


def solution(mesh):
    def step(x, dy, *weights):
        x, dy = x[0], dy[0]
        qkv, wo, gate, up, down, at, dyt, q, k, v, o, cos, sin, lse = advance(x, dy, *(w[0] for w in weights))
        dh, do, delta, dwo, dwg, dwu, dwd = middle(o, x, dy, dyt, wo, gate, up, down)
        dq, dk, dv, wide, tall = attend_back(q, k, v, do, lse, delta, dwg, dwu, dwd)
        dx, mixed = project_back(dq, dk, dv, cos, sin, x, dh, at, qkv, dwo)
        return tuple(g[None] for g in deal(dx, mixed, wide, tall))

    states, cut = P(("rep", "dp"), None, None), P(None, "dp", None)
    return jax.shard_map(
        step,
        mesh=mesh,
        in_specs=(states, states) + (cut,) * 7,
        out_specs=(states,) + (P("rep", "dp", None),) * 7,
        check_vma=False,
    )
```

```python
import jax
import jax.numpy as jnp
import numpy as np
from jax import lax
from jax.experimental import pallas as pl
from jax.experimental.pallas import tpu as pltpu
from jax.sharding import PartitionSpec as P

HEAD = 128
THETA = 10000
EPS = 1e-6
ZERO, ONE, HALF, FULL, DIM, WIDE, ROWS, MATES, PLACES, SIX, TWO, THREE, COLOURS = 0, 1, 1024, 2048, 768, 256, 16, 8, 4, 6, 2, 3, 3
GRID = (PLACES, PLACES)
NEG = -1e30
HIDDEN = 2 * NEG
LOG2E = 1.4426950408889634
VMEM = 56 * 2**20
BLOCK = 512
BF, F32 = jnp.bfloat16, jnp.float32
SCALE = HEAD**-0.5
E = SCALE * LOG2E


def _dot(a, b, ca, cb):
    return lax.dot_general(a, b, (((ca,), (cb,)), ((), ())), preferred_element_type=F32)


def _mm(a, b):
    return _dot(a, b, ONE, ZERO)


def _mt(a, b):
    return _dot(a, b, ONE, ONE)


def _first():
    return pl.program_id(ZERO) == ZERO


def _last():
    return pl.program_id(ZERO) == pl.num_programs(ZERO) - ONE


def _visible(keys, queries, first):
    return lax.broadcasted_iota(jnp.int32, (keys, queries), 0) <= lax.broadcasted_iota(jnp.int32, (keys, queries), 1) + first


def _call(kernel, name, grid, ins, outs, scratch=(), flops=0):
    given = [a for a, _, _ in ins]
    moved = sum(a.size * a.dtype.itemsize for a in given)
    return pl.pallas_call(
        kernel,
        grid=(grid,),
        in_specs=[pl.BlockSpec(block, index) for _, block, index in ins],
        out_specs=[pl.BlockSpec(block, index) for _, _, block, index in outs],
        out_shape=[jax.ShapeDtypeStruct(shape, dtype) for shape, dtype, _, _ in outs],
        scratch_shapes=list(scratch),
        compiler_params=pltpu.CompilerParams(dimension_semantics=("arbitrary",), vmem_limit_bytes=VMEM),
        cost_estimate=pl.CostEstimate(flops=flops, transcendentals=0, bytes_accessed=2 * moved),
        name=name,
    )(*given)


def _rows(*shape):
    return shape, lambda i: (i,) + (0,) * (len(shape) - 1)


def _all(*shape):
    return shape, lambda i: (0,) * len(shape)


def _norm(h):
    wide = h.astype(F32)
    return (wide * lax.rsqrt(jnp.mean(wide * wide, -1, keepdims=ONE) + EPS)).astype(BF)


def _norm_back(h, g):
    wide, g = h.astype(F32), g.astype(F32)
    scale = lax.rsqrt(jnp.mean(wide * wide, -1, keepdims=ONE) + EPS)
    return scale * (g - wide * (scale * scale * jnp.mean(g * wide, -1, keepdims=ONE)))


FEED_STEP = 512
PIECE = 512
ROWS_AT_ONCE = DIM


def _middle(o, x, dy, dyt, wo, wg_ref, wu_ref, wd_ref, dh_o, do_o, delta_ref, dwo_ref, dwg_ref, dwu_ref, dwd_ref,
            o_s, h_s, dy_s, dyt_s, wo_s, b_s, bt_s, db_s, z_s, load_sems, out_sems):
    f = wg_ref.shape[ONE]
    heads, n, _ = o_s.shape
    d = h_s.shape[ONE]
    pieces = [slice(lo, lo + BLOCK) for lo in range(0, n, BLOCK)]

    @pl.when(_first())
    def _():
        pltpu.make_async_copy(wo, wo_s, load_sems.at[TWO, 0]).start()
        for i, here in enumerate(pieces):
            pltpu.make_async_copy(o.at[:, here], o_s.at[:, here], load_sems.at[ZERO, i]).start()
            pltpu.make_async_copy(x.at[here], h_s.at[here], load_sems.at[ONE, i]).start()
        pltpu.make_async_copy(dy, dy_s, load_sems.at[TWO, 1]).start()
        pltpu.make_async_copy(dyt, dyt_s, load_sems.at[TWO, 2]).start()
        pltpu.make_async_copy(wo, wo_s, load_sems.at[TWO, 0]).wait()

        def open_(i, _):
            here = pl.ds(pl.multiple_of(i * BLOCK, BLOCK), BLOCK)
            pltpu.make_async_copy(o.at[:, here], o_s.at[:, here], load_sems.at[ZERO, i]).wait()
            pltpu.make_async_copy(x.at[here], h_s.at[here], load_sems.at[ONE, i]).wait()
            heard = jnp.concatenate([o_s[m, here, :] for m in range(heads)], axis=ONE)
            h = h_s[here, :] + _mm(heard, wo_s[:, :d]).astype(BF)
            h_s[here, :] = h
            b = _norm(h)
            b_s[here, :] = b
            bt_s[:, here] = b.T

        lax.fori_loop(0, n // BLOCK, open_, None)
        db_s[...] = jnp.zeros_like(db_s)
        pltpu.make_async_copy(dy, dy_s, load_sems.at[TWO, 1]).wait()
        pltpu.make_async_copy(dyt, dyt_s, load_sems.at[TWO, 2]).wait()

    both = jnp.concatenate([wg_ref[...], wu_ref[...]], axis=ONE)

    def forward(i):
        here = slice(i * PIECE, i * PIECE + PIECE)
        return _mm(b_s[here, :], both), _mt(dy_s[here, :], wd_ref[...])

    def piece(i, gate_up, dmid):
        here = slice(i * PIECE, i * PIECE + PIECE)
        gate, up, dmid = gate_up[:, :f], gate_up[:, f:], dmid.astype(BF).astype(F32)
        sig = 0.5 * jnp.tanh(0.5 * gate) + 0.5
        silu = gate * sig
        z_s[here, 2 * f :] = (silu * up).astype(BF)
        z_s[here, f : 2 * f] = (dmid * silu).astype(BF)
        z_s[here, :f] = (dmid * up * (sig + silu * (1 - sig))).astype(BF)

    def to_b(i):
        here = slice(i * PIECE, i * PIECE + PIECE)
        db_s[here, :] += _mt(z_s[here, : 2 * f], both)

    ahead = forward(0)
    for i in range(n // PIECE):
        now, ahead = ahead, forward(i + ONE) if i + 1 < n // PIECE else None
        piece(i, *now)
        if i:
            to_b(i - 1)
    to_b(n // PIECE - 1)

    def weights(i, _):
        here = pl.ds(pl.multiple_of(i * ROWS_AT_ONCE, ROWS_AT_ONCE), ROWS_AT_ONCE)
        dw = _mm(bt_s[here, :], z_s[:, : 2 * f])
        dwg_ref[here, :] = dw[:, :f].astype(BF)
        dwu_ref[here, :] = dw[:, f:].astype(BF)
        dwd_ref[:, here] = _mm(dyt_s[here, :], z_s[:, 2 * f :]).astype(BF).T

    lax.fori_loop(0, d // ROWS_AT_ONCE, weights, None)

    @pl.when(_last())
    def _():

        def back(i, _):
            here = pl.ds(pl.multiple_of(i * BLOCK, BLOCK), BLOCK)
            dy_s[here, :] = (dy_s[here, :].astype(F32) + _norm_back(h_s[here, :], db_s[here, :].astype(BF))).astype(BF)
            pltpu.make_async_copy(dy_s.at[here], dh_o.at[here], out_sems.at[ZERO, i]).start()

        lax.fori_loop(0, n // BLOCK, back, None)

        def by_wo(m, _):
            here = pl.ds(pl.multiple_of(m * HEAD, HEAD), HEAD)
            dwo_ref[here, :d] = _dot(o_s[m], dy_s[...], 0, 0).astype(BF)

        lax.fori_loop(0, heads, by_wo, None)
        dwo_ref[:, d:] = jnp.zeros_like(dwo_ref[:, d:])

        def by_o(i, _):
            here = pl.ds(pl.multiple_of(i * BLOCK, BLOCK), BLOCK)
            do = _mt(dy_s[here, :], wo_s[:, :d]).astype(BF)
            for m in range(heads):
                mine = do[:, m * HEAD : (m + 1) * HEAD]
                delta_ref[m : m + 1, here] = (mine.astype(F32) * o_s[m, here, :].astype(F32)).T.sum(axis=ZERO, keepdims=ONE)
                o_s[m, here, :] = mine
            pltpu.make_async_copy(o_s.at[:, here], do_o.at[:, here], out_sems.at[ONE, i]).start()

        lax.fori_loop(0, n // BLOCK, by_o, None)
        for i, here in enumerate(pieces):
            pltpu.make_async_copy(dy_s.at[here], dh_o.at[here], out_sems.at[ZERO, i]).wait()
            pltpu.make_async_copy(o_s.at[:, here], do_o.at[:, here], out_sems.at[ONE, i]).wait()


def middle(o, x, dy, dyt, wo, gate, up, down):
    n, d = x.shape
    heads, f, ff = o.shape[ZERO], FEED_STEP, gate.shape[ONE]
    anywhere = pl.BlockSpec(memory_space=pl.ANY)
    cols, rows = pl.BlockSpec((d, f), lambda i: (0, i)), pl.BlockSpec((f, d), lambda i: (i, 0))
    dma = pltpu.SemaphoreType.DMA
    return pl.pallas_call(
        _middle,
        grid=(ff // f,),
        in_specs=[anywhere] * 5 + [cols, cols, rows],
        out_specs=[anywhere] * TWO + [pl.BlockSpec((heads, n), lambda i: (0, 0)), pl.BlockSpec(wo.shape, lambda i: (0, 0)), cols, cols, rows],
        out_shape=[jax.ShapeDtypeStruct(s, t) for s, t in (((n, d), BF), (o.shape, BF), ((heads, n), F32), (wo.shape, BF),
                                                           (gate.shape, BF), (up.shape, BF), (down.shape, BF))],
        scratch_shapes=[pltpu.VMEM(s, BF) for s in (o.shape, (n, d), (n, d), (d, n), wo.shape, (n, d), (d, n))]
        + [pltpu.VMEM((n, d), F32), pltpu.VMEM((n, 3 * f), BF), dma((3, 4)), dma((2, 4))],
        compiler_params=pltpu.CompilerParams(dimension_semantics=("arbitrary",), vmem_limit_bytes=VMEM),
        cost_estimate=pl.CostEstimate(flops=ROWS * n * d * ff, transcendentals=0, bytes_accessed=2 * n * d * 20),
        name="middle",
    )(o, x, dy, dyt, wo, gate, up, down)


RING = 4
ORDERS = ("xyz", "yzx", "zxy")
MIXED, GATE, UP, DOWN = range(PLACES)


def _place():
    me = lax.axis_index("dp")
    return {"x": me // 32, "y": me // 8 % RING, "z": me // TWO % RING, "k": me % TWO}


def _device(at, **other):
    at = {**at, **other}
    return {"dp": ((at["x"] * 4 + at["y"]) * 4 + at["z"]) * TWO + at["k"]}


def _beside(at, axis, by):
    return _device(at, **{axis: (at[axis] + by) % RING})


def _mate(at, by):
    other = (at["z"] * TWO + at["k"] + by) % 8
    return _device(at, z=other // TWO, k=other % TWO)


def _greet(at):
    barrier = pltpu.get_barrier_semaphore()
    peers = [_beside(at, axis, by) for axis in "xy" for by in range(1, RING)] + [_mate(at, by) for by in range(ONE, MATES)]
    for peer in peers:
        pl.semaphore_signal(barrier, inc=1, device_id=peer, device_id_type=pl.DeviceIdType.MESH)
    pl.semaphore_wait(barrier, len(peers))


def _remote(src, dst, send, recv, device):
    pltpu.make_async_remote_copy(src_ref=src, dst_ref=dst, send_sem=send, recv_sem=recv, device_id=device,
                                 device_id_type=pl.DeviceIdType.MESH).start()


def _start(src, dst, sem):
    pltpu.make_async_copy(src, dst, sem).start()


def _arrived(ref, sem):
    pltpu.make_async_copy(ref, ref, sem).wait()


def _lanes(z, lo=0, n=WIDE):
    return pl.ds(pl.multiple_of(z * WIDE + lo, HEAD), n)


def _half_columns(k):
    return pl.ds(pl.multiple_of(k * HALF, HALF), HALF)


def _tokens(i, first=0, many=BLOCK):
    return pl.ds(i * BLOCK + first if isinstance(i, int) else pl.multiple_of(i * BLOCK + first, BLOCK // TWO), many)


def _columns(j):
    return (j % TWO) * HALF + (j // TWO) * WIDE


STARTS = (0, DIM, 896, HALF)


def _from_mixed(refs, lo):
    return next(((ref, lo - base) for ref, base in zip(refs, STARTS, strict=ONE) if 0 <= lo - base < ref.shape[ONE]), None)


def _advance(wq, wk, wv, wo, wg, wu, wd, freq, x, dy, qkv_o, wo_o, gate_o, up_o, down_o, at_o, dyt_o, q_o, k_o, v_o, o_o, cos_o, sin_o, lse_o,
             out_s, in_s, ws, wds, mixed_s, x_s, dy_s, a_s, at_s, dyt_s, q_s, k_s, v_s, o_s, top_s, mix_s, cos_s, sin_s,
             mate_sems, ring_send, ring_recv, pair_sems, own_sem, load_sems, store_sems):
    at = _place()
    seat = at["z"] * TWO + at["k"]
    outs = (None, gate_o, up_o)
    heads = q_s.shape[ZERO]
    blocks = x_s.shape[ZERO] // BLOCK
    sent = {}
    kept = []

    def send(key, ref, dst, sem, recv, device):
        _remote(ref(), dst(), sem(), recv, device)
        sent[key] = ref, sem

    def store(src, dst, n):
        _start(src, dst, store_sems.at[n])
        kept.append((src, store_sems.at[n]))

    _start(x, x_s, load_sems.at[ZERO])
    _start(dy, dy_s, load_sems.at[ONE])
    for j in range(MATES):
        for lo in (0, HEAD):
            found = _from_mixed((wq, wk, wv, wo), _columns(j) + lo)
            if found:
                ref, first = found
                out_s[j, MIXED, ZERO:SIX, lo : lo + HEAD] = ref[:, first : first + HEAD]
            else:
                out_s[j, MIXED, ZERO:SIX, lo : lo + HEAD] = jnp.zeros((6, HEAD), BF)
        for t, ref in ((GATE, wg), (UP, wu)):
            out_s[j, t, ZERO:SIX, :] = ref[:, _columns(j) : _columns(j) + WIDE]
        out_s[j, :, SIX:MATES, :] = jnp.zeros((3, 2, WIDE), BF)
    _greet(at)
    for by in range(ONE, MATES):
        send(by, lambda by=by: out_s.at[(seat + by) % 8], lambda: in_s.at[seat], lambda by=by: mate_sems.at[ZERO, by], mate_sems.at[ONE, by],
             _mate(at, by))
    in_s[seat] = out_s[seat]
    for c in range(COLOURS):
        wds[at["x"], at["y"], at["z"], :, WIDE * c : WIDE * c + WIDE] = wd[:, WIDE * c : WIDE * c + WIDE]

    def region(t, c, fixed, half=None):
        x, y = (fixed.get(axis, slice(None)) for axis in "xy")
        if t != DOWN and "z" not in fixed:
            return ws.at[t, x, y, c, :, slice(None) if half is None else slice(512 * half, 512 * half + 512)]
        lo, n = (0, WIDE) if half is None else (HEAD * half, HEAD)
        if t == DOWN:
            return wds.at[x, y, fixed.get("z", slice(None)), :, WIDE * c + lo : WIDE * c + lo + n]
        return ws.at[t, x, y, c, :, _lanes(fixed["z"], lo, n)]

    def known(c, phase, place):
        order = ORDERS[c][::-1]
        return {**{a: at[a] for a in order[phase + 1 :]}, order[phase]: place}

    def hop(t, c, phase, slot, by, here):
        key = t, c, phase, slot
        send(key, here, here, lambda: ring_send.at[key], ring_recv.at[key], _beside(at, ORDERS[c][::-1][phase], by))

    def send_own(phase, *ts):
        for t in ts:
            for c in range(COLOURS):
                for slot, by in enumerate((1, 2, 3) if phase < 2 else (1, 3)):
                    hop(t, c, phase, slot, by, lambda t=t, c=c: region(t, c, known(c, phase, at[ORDERS[c][::-1][phase]])))

    def pass_on(phase, *ts):
        for t in ts:
            for c in range(COLOURS):
                axis = ORDERS[c][::-1][phase]
                for slot, by in ((0, 3), (1, 1)):

                    def here(half, t=t, c=c, axis=axis, by=by):
                        return region(t, c, known(c, phase, (at[axis] + by) % RING), half)

                    _arrived(here(None), ring_recv.at[t, c, phase, slot])
                    hop(t, c, phase, 2 + slot, RING - by, lambda here=here, slot=slot: here(1 - slot))

    def finish(phase, *ts):
        for t in ts:
            for c in range(COLOURS):
                place = at[ORDERS[c][::-1][phase]]
                for slot in range(COLOURS) if phase < 2 else (2, 3):
                    by, half = (3 - slot, None) if phase < 2 else (2, 3 - slot)
                    _arrived(region(t, c, known(c, phase, (place + by) % RING), half), ring_recv.at[t, c, phase, slot])

    partner = _device(at, k=ONE - at["k"])

    def half(t, k):
        return down_o.at[:, :, :, k] if t == DOWN else outs[t].at[:, :, :, :, _half_columns(k)]

    def to_result(t):
        src = wds if t == DOWN else ws.at[t]
        _remote(src, half(t, at["k"]), pair_sems.at[ZERO, t], pair_sems.at[ONE, t], partner)
        _start(src, half(t, at["k"]), own_sem.at[t])

    def prepare(i):
        here = slice(i * BLOCK, i * BLOCK + BLOCK)
        a = _norm(x_s[here, :])
        a_s[here, :] = a
        at_s[:, here] = a.T

    def turn(i):
        here = slice(i * BLOCK, i * BLOCK + BLOCK)
        dyt_s[:, here] = dy_s[here, :].T

    def tables():
        half, rows = HEAD // TWO, 64
        place = lax.broadcasted_iota(jnp.int32, (rows, HEAD), 0).astype(F32)
        left = lax.broadcasted_iota(jnp.int32, (rows, HEAD), 1) < half
        near, far = place * freq[...], place[: x_s.shape[ZERO] // rows] * rows * freq[: x_s.shape[ZERO] // rows]
        near_cos, near_sin, far_cos, far_sin = jnp.cos(near), jnp.sin(near), jnp.cos(far), jnp.sin(far)
        for n in range(x_s.shape[ZERO] // rows):
            c, s = far_cos[n : n + ONE, :], far_sin[n : n + ONE, :]
            cos_s[n * rows : n * rows + rows, :] = near_cos * c - near_sin * s
            sin = near_sin * c + near_cos * s
            sin_s[n * rows : n * rows + rows, :] = jnp.where(left, -sin, sin)
        store(cos_s, cos_o, 6)
        store(sin_s, sin_o, 7)

    def project(i):
        here = slice(i * BLOCK, i * BLOCK + BLOCK)
        t = _mm(a_s[here, :], mixed_s[...].reshape(a_s.shape[ONE], -1)).astype(BF)
        cos, sin = cos_s[here, :], sin_s[here, :]
        for n in range(heads + ONE):
            one = t[:, n * HEAD : (n + ONE) * HEAD].astype(F32)
            one = (one * cos + pltpu.roll(one, HEAD // TWO, 1) * sin).astype(BF)
            if n < heads:
                q_s[n, here, :] = one
            else:
                k_s[here, :] = one
        v_s[here, :] = t[:, (heads + ONE) * HEAD :]

    rest = (GATE, UP, DOWN)
    _arrived(x_s, load_sems.at[ZERO])
    prepare(0)
    for by in range(ONE, MATES):
        _arrived(in_s.at[ZERO], mate_sems.at[ONE, by])
    for t in range(COLOURS):
        rows = jnp.concatenate([in_s[j, t].astype(F32)[ZERO:SIX, :] for j in range(MATES)], axis=ZERO).astype(BF)
        for c in range(COLOURS):
            ws[t, at["x"], at["y"], c, :, _lanes(at["z"])] = rows[ROWS * c : ROWS * c + ROWS, :]
    send_own(0, MIXED)
    send_own(0, *rest)
    prepare(1)
    finish(0, MIXED)
    send_own(1, MIXED)
    prepare(2)
    finish(1, MIXED)
    send_own(2, MIXED)
    prepare(3)
    store(at_s, at_o, 0)
    tables()
    pass_on(2, MIXED)
    finish(0, *rest)
    send_own(1, *rest)
    _arrived(dy_s, load_sems.at[ONE])
    for i in range(blocks):
        turn(i)
    store(dyt_s, dyt_o, 1)
    finish(2, MIXED)

    @pl.when(at["k"] == ZERO)
    def _():
        _remote(ws.at[MIXED], mixed_s, pair_sems.at[ZERO, MIXED], pair_sems.at[ONE, MIXED], partner)
        mixed_s[...] = ws[MIXED]

    @pl.when(at["k"] == ONE)
    def _():
        _remote(ws.at[MIXED], wo_o, pair_sems.at[ZERO, MIXED], pair_sems.at[ONE, MIXED], partner)
        _start(ws.at[MIXED], wo_o, own_sem.at[MIXED])

    finish(1, *rest)
    send_own(2, GATE, UP)
    _arrived(mixed_s, pair_sems.at[ONE, MIXED])
    store(mixed_s, qkv_o, 2)
    for i in range(blocks):
        project(i)
        if i == 1:
            pass_on(2, GATE)
            send_own(2, DOWN)
    store(q_s, q_o, 3)
    store(k_s, k_o, 4)
    store(v_s, v_o, 5)

    def between(n):
        @pl.when(n == 0)
        def _():
            pass_on(2, UP)

        @pl.when(n == 1)
        def _():
            finish(2, GATE)
            to_result(GATE)
            pass_on(2, DOWN)

        @pl.when(n == 2)
        def _():
            finish(2, UP)
            to_result(UP)

        @pl.when(n == 3)
        def _():
            finish(2, DOWN)
            to_result(DOWN)

    ones = jnp.ones((8, BLOCK), BF)

    def block(iq, j, first=0, queries=BLOCK, keys=BLOCK, masked=False):
        here, mine, cols = _tokens(j, 0, keys), _tokens(iq, first, queries), slice(first, first + queries)
        scores = [_mt(k_s[here, :], q_s[n, mine, :]) for n in range(heads)]
        weights, keeps = [], []
        for n, s in enumerate(scores):
            if masked:
                s = jnp.where(_visible(keys, queries, first), s, HIDDEN)
            old = top_s[n : n + ONE, cols]
            top = jnp.maximum(old, s.max(axis=ZERO, keepdims=ONE))
            top_s[n : n + ONE, cols] = top
            weights.append(jnp.exp2((s - top) * E).astype(BF))
            keeps.append(jnp.exp2((old - top) * E))
        values = jnp.concatenate([v_s[here, :].T, ones[:, :keys]], axis=ZERO)
        for n, (p, keep) in enumerate(zip(weights, keeps, strict=ONE)):
            mix_s[n, :, cols] = mix_s[n, :, cols] * keep + _mm(values, p)

    def row(iq, _):
        top_s[...] = jnp.full(top_s.shape, NEG, F32)
        mix_s[...] = jnp.zeros(mix_s.shape, F32)

        def step(j, _):
            block(iq, j)
            between(iq * (iq + ONE) // TWO + j)

        lax.fori_loop(0, iq, step, None)
        for first in (0, BLOCK // TWO):
            block(iq, iq, first, BLOCK // TWO, first + BLOCK // TWO, True)
        between(iq * (iq + ONE) // TWO + iq)
        mine = _tokens(iq)
        for n in range(heads):
            total = mix_s[n, HEAD : HEAD + 1, :]
            o_s[n, mine, :] = (mix_s[n, :HEAD, :] * (1 / total)).T.astype(BF)
            lse_o[n : n + ONE, mine] = top_s[n : n + ONE, :] * SCALE + jnp.log(total)
        _start(o_s.at[:, mine], o_o.at[:, mine], own_sem.at[4])

    lax.fori_loop(0, blocks, row, None)
    _arrived(o_s, own_sem.at[4])
    for ref, sem in sent.values():
        _arrived(ref(), sem())
    for t in (MIXED, *rest):
        src = wds if t == DOWN else ws.at[t]
        _arrived(src, pair_sems.at[ZERO, t])
        if t != MIXED:
            _arrived(src, pair_sems.at[ONE, t])
            _arrived(src, own_sem.at[t])

    @pl.when(at["k"] == ONE)
    def _():
        _arrived(ws.at[MIXED], own_sem.at[MIXED])

    for ref, sem in kept:
        _arrived(ref, sem)


def advance(x, dy, *shards):
    n, d = x.shape
    heads = d // HEAD
    half = HEAD // TWO
    freq = np.tile(float(THETA) ** (-np.arange(half) / half), (half, 2)).astype(np.float32)
    vmem, anywhere = pl.BlockSpec(memory_space=pltpu.VMEM), pl.BlockSpec(memory_space=pl.ANY)
    wide, narrow = (*GRID, COLOURS, ROWS, FULL), (*GRID, COLOURS, ROWS, HALF)
    tall = (*GRID, PLACES, 2, ROWS, DIM)
    many, one = (heads, n, HEAD), (n, HEAD)
    shapes = (narrow, narrow, wide, wide, tall, (d, n), (d, n), many, one, one, many)
    dma = pltpu.SemaphoreType.DMA
    qkv, wo, gate, up, down, *rest = pl.pallas_call(
        _advance,
        in_specs=[vmem] * 8 + [anywhere] * 2,
        out_specs=[anywhere] * (len(shapes) + 2) + [vmem],
        out_shape=[jax.ShapeDtypeStruct(s, BF) for s in shapes] + [jax.ShapeDtypeStruct(s, F32) for s in (one, one, (heads, n))],
        scratch_shapes=[pltpu.VMEM(s, BF) for s in ((MATES, 3, MATES, WIDE), (MATES, 3, MATES, WIDE), (3, *narrow), (*GRID, PLACES, ROWS, DIM), narrow,
                                                    (n, d), (n, d), (n, d), (d, n), (d, n), many, one, one, many)]
        + [pltpu.VMEM(s, F32) for s in ((heads, BLOCK), (heads, HEAD + 8, BLOCK), one, one)]
        + [dma((2, 8)), dma((PLACES, COLOURS, COLOURS, PLACES)), dma((PLACES, COLOURS, COLOURS, PLACES)), dma((2, 4)), dma((5,)), dma((2,)), dma((8,))],
        compiler_params=pltpu.CompilerParams(collective_id=0, has_side_effects=True, vmem_limit_bytes=VMEM),
        name="advance",
    )(*shards, freq, x, dy)
    return qkv.reshape(d, -1), wo.reshape(d, -1), gate.reshape(d, -1), up.reshape(d, -1), down.reshape(-1, d), *rest


class _Sums:
    STEPS = 5

    def __init__(self, at, ts, own, theirs, bufs, total, down_o, ring_send, ring_recv, pair_sems, own_sems):
        self.at, self.ts, self.own, self.theirs, self.bufs, self.total, self.down_o = at, ts, own, theirs, bufs, total, down_o
        self.ring_send, self.ring_recv, self.pair_sems, self.own_sems = ring_send, ring_recv, pair_sems, own_sems
        self.partner = _device(at, k=ONE - at["k"])

    def give(self, t, ref):
        n = self.ts.index(t)
        _remote(ref, self.theirs[n], self.pair_sems.at[ZERO, n], self.pair_sems.at[ONE, n], self.partner)

    def keep(self, t, ref):
        n = self.ts.index(t)
        _start(ref, self.own[n], self.own_sems.at[n])

    def kept(self, t):
        n = self.ts.index(t)
        _arrived(self.own[n], self.own_sems.at[n])

    def term(self, n, c, phase, q, i, j):
        if phase:
            acc = self.bufs[phase - 1][-1]
            return acc[n, c, q, j] if phase == 1 else acc[n, c, q]
        place = dict(zip(ORDERS[c], (q, i, j), strict=ONE))
        x, y, z = (place[a] for a in "xyz")
        if self.ts[n] == DOWN:
            both = (ref[x, y, z, :, WIDE * c : WIDE * c + WIDE] for ref in (self.own[n], self.theirs[n]))
        else:
            both = (ref[x, y, c, :, _lanes(z)] for ref in (self.own[n], self.theirs[n]))
        return sum(b.astype(F32) for b in both)

    @staticmethod
    def over_cells(phase, act):
        if phase == 0:
            lax.fori_loop(0, 4, lambda i, _: [act(i, j, (i, j)) for j in range(PLACES)] and None, None)
        elif phase == 1:
            for j in range(PLACES):
                act(0, j, (j,))
        else:
            act(0, 0, ())

    def hop(self, n, c, phase, slot, by, src, dst):
        _remote(src, dst, self.ring_send.at[n, c, phase, slot], self.ring_recv.at[n, c, phase, slot], _beside(self.at, ORDERS[c][phase], by))

    def near(self, c, phase, by):
        return (self.at[ORDERS[c][phase]] + by) % RING

    def begin(self, n, c, phase):
        to, into = self.bufs[phase][:2]
        places = [self.near(c, phase, by) for by in (1, 2, 3)]

        def act(i, j, where):
            above, opposite, below = (self.term(n, c, phase, q, i, j) for q in places)
            to[(n, c, 0, *where)] = jnp.concatenate([above[:, :HEAD], opposite[:, HEAD:]], axis=ONE).astype(BF)
            to[(n, c, 1, *where)] = jnp.concatenate([opposite[:, :HEAD], below[:, HEAD:]], axis=ONE).astype(BF)

        def straight(i, j, where):
            for slot, q in enumerate(places):
                to[(n, c, slot, *where)] = self.term(n, c, phase, q, i, j).astype(BF)

        self.over_cells(phase, straight if phase else act)
        for slot, by in enumerate((1, 2, 3) if phase else (1, 3)):
            self.hop(n, c, phase, slot, by, to.at[n, c, slot], into.at[n, c, slot])

    def relay(self, n, c, phase):
        into, over, last = self.bufs[phase][1:4]
        for slot, by, half in ((0, 1, slice(HEAD, WIDE)), (1, 3, slice(0, HEAD))):
            _arrived(into.at[n, c, slot], self.ring_recv.at[n, c, phase, slot])
            place = self.near(c, phase, by)

            def act(i, j, where, slot=slot, half=half, place=place):
                mine = self.term(n, c, phase, place, i, j)[:, half]
                over[(n, c, slot, *where)] = (mine + into[(n, c, slot, *where)][:, half].astype(F32)).astype(BF)

            self.over_cells(phase, act)
            self.hop(n, c, phase, 2 + slot, by, over.at[n, c, slot], last.at[n, c, slot])

    def finish(self, n, c, phase):
        into = self.bufs[phase][1]
        if phase:
            for slot in range(COLOURS):
                _arrived(into.at[n, c, slot], self.ring_recv.at[n, c, phase, slot])
        else:
            last = self.bufs[phase][3]
            for slot in (ZERO, ONE):
                _arrived(last.at[n, c, slot], self.ring_recv.at[n, c, phase, 2 + slot])

        def act(i, j, where):
            mine = self.term(n, c, phase, self.near(c, phase, 0), i, j)
            if phase:
                whole = sum((into[(n, c, slot, *where)].astype(F32) for slot in range(COLOURS)), mine)
            else:
                a = mine[:, :HEAD] + into[(n, c, 0, *where)][:, :HEAD].astype(F32) + last[(n, c, 1, *where)].astype(F32)
                b = mine[:, HEAD:] + into[(n, c, 1, *where)][:, HEAD:].astype(F32) + last[(n, c, 0, *where)].astype(F32)
                whole = jnp.concatenate([a, b], axis=ONE)
            if phase < 2:
                self.bufs[phase][-1][(n, c, *where)] = whole
            elif self.ts[n] == DOWN:
                self.down_o[:, WIDE * c : WIDE * c + WIDE] = whole.astype(BF)
            else:
                self.total[n, ROWS * c : ROWS * c + ROWS, :] = whole

        self.over_cells(phase, act)

    def step(self, n, what):
        if what == 0:
            _arrived(self.theirs[n], self.pair_sems.at[ONE, n])
        for c in range(COLOURS):
            if what == 0:
                self.begin(n, c, 0)
            elif what == 1:
                self.relay(n, c, 0)
            else:
                self.finish(n, c, what - 2)
                if what < 4:
                    self.begin(n, c, what - 1)

    def steps(self, slot):
        for n in range(len(self.ts)):
            if 0 <= slot - n < self.STEPS:
                self.step(n, slot - n)

    def all_sent(self):
        for n in range(len(self.ts)):
            _arrived(self.theirs[n], self.pair_sems.at[ZERO, n])
            for c in range(COLOURS):
                for phase, (to, _, *more) in enumerate(self.bufs):
                    for slot in range(COLOURS) if phase else (ZERO, ONE):
                        _arrived(to.at[n, c, slot], self.ring_send.at[n, c, phase, slot])
                        if not phase:
                            _arrived(more[0].at[n, c, slot], self.ring_send.at[n, c, phase, 2 + slot])

    def deal_out(self, wide, out_s, in_s, mate_sems):
        seat = self.at["z"] * TWO + self.at["k"]
        for n in range(wide):
            for j in range(MATES):
                out_s[j, n, ZERO:SIX, :] = self.total[n, 6 * j : 6 * j + 6, :].astype(BF)
                out_s[j, n, SIX:MATES, :] = jnp.zeros((2, WIDE), BF)
        for by in range(ONE, MATES):
            _remote(out_s.at[(seat + by) % 8], in_s.at[seat], mate_sems.at[ZERO, by], mate_sems.at[ONE, by], _mate(self.at, by))
        in_s[seat] = out_s[seat]

    @staticmethod
    def dealt(out_s, in_s, mate_sems):
        for by in range(ONE, MATES):
            _arrived(in_s.at[ZERO], mate_sems.at[ONE, by])
            _arrived(out_s.at[ZERO], mate_sems.at[ZERO, by])


def _sum_scratch(ts):
    count = len(ts)
    scratch = [pltpu.VMEM((*GRID, PLACES, ROWS, DIM) if t == DOWN else (*GRID, COLOURS, ROWS, HALF), BF) for t in ts for _ in range(2)]
    for left in ((4, 4), (4,), ()):
        first = left == (4, 4)
        scratch += [pltpu.VMEM((count, 3, 2 if first else 3, *left, ROWS, WIDE), BF)] * 2
        scratch += [pltpu.VMEM((count, 3, 2, *left, ROWS, HEAD), BF)] * TWO if first else []
        scratch += [pltpu.VMEM((count, 3, *left, ROWS, WIDE), F32)] if left else []
    wide = count - (DOWN in ts)
    dma = pltpu.SemaphoreType.DMA
    return scratch + [pltpu.VMEM((wide, 48, WIDE), F32)] + [pltpu.VMEM((8, wide, 8, WIDE), BF)] * TWO + [
        dma((count, COLOURS, COLOURS, PLACES)), dma((count, COLOURS, COLOURS, PLACES)), dma((2, count)), dma((count,)), dma((2, 8))]


def _sums(at, ts, refs, down_o):
    refs = list(refs)
    pairs = [(refs.pop(0), refs.pop(0)) for _ in ts]
    bufs = [[refs.pop(0) for _ in range(many)] for many in (5, 3, 2)]
    total, out_s, in_s, ring_send, ring_recv, pair_sems, own_sems, mate_sems = refs
    sums = _Sums(at, ts, [a for a, _ in pairs], [b for _, b in pairs], bufs, total, down_o, ring_send, ring_recv, pair_sems, own_sems)
    return sums, (out_s, in_s, mate_sems)


LATER = (GATE, UP, DOWN)


def _attend_back(q, k, v, do, lse_ref, delta_ref, gate, up, down, dq_o, dk_o, dv_o, rows_o, down_o,
                 q_s, k_s, v_s, do_s, dq_s, dk_s, dv_s, sum_s, load_sems, out_sem, *refs):
    at = _place()
    heads = q_s.shape[ZERO]
    blocks = q_s.shape[ONE] // BLOCK
    sums, mates = _sums(at, LATER, refs, down_o)
    _start(k, k_s, load_sems.at[ZERO, 0])
    _start(v, v_s, load_sems.at[ONE, 0])
    for i in range(blocks):
        _start(q.at[:, _tokens(i)], q_s.at[:, _tokens(i)], load_sems.at[TWO, i])
        _start(do.at[:, _tokens(i)], do_s.at[:, _tokens(i)], load_sems.at[THREE, i])
    _greet(at)

    def part(t, k):
        return down.at[:, :, :, k] if t == DOWN else (gate, up)[t - GATE].at[:, :, :, :, _half_columns(k)]

    for t in LATER:
        sums.give(t, part(t, ONE - at["k"]))
        sums.keep(t, part(t, at["k"]))
    sum_s[...] = jnp.zeros_like(sum_s)
    dk_s[...] = jnp.zeros_like(dk_s)
    dv_s[...] = jnp.zeros_like(dv_s)
    _arrived(k_s, load_sems.at[ZERO, 0])
    _arrived(v_s, load_sems.at[ONE, 0])

    def between(slot):
        if 0 <= slot < 3:
            sums.kept(LATER[slot])
        sums.steps(slot)
        if slot == sums.STEPS + 1:
            sums.deal_out(2, *mates)

    def block(iq, j, first=0, queries=BLOCK, keys=BLOCK):
        here, mine, cols = _tokens(j, 0, keys), _tokens(iq, first, queries), slice(first, first + queries)

        def some(half, _):
            group = [half * (heads // TWO) + n for n in range(heads // TWO)]
            scores = [_mt(k_s[here, :], q_s[n, mine, :]) for n in group]
            dps = [_mt(v_s[here, :], do_s[n, mine, :]) for n in group]
            for n, s, dp in zip(group, scores, dps, strict=ONE):
                p = jnp.exp2(s * E - lse_ref[pl.ds(n, 1), mine] * LOG2E)
                if iq == j:
                    p = jnp.where(_visible(keys, queries, first), p, 0.0)
                ds = (p * (dp - delta_ref[pl.ds(n, 1), mine])).astype(BF)
                dv_s[here, :] += _mm(p.astype(BF), do_s[n, mine, :])
                dk_s[here, :] += _mm(ds, q_s[n, mine, :])
                sum_s[n, :, cols] += _mm(k_s[here, :].T, ds)

        lax.fori_loop(0, 2, some, None)

    for iq in range(blocks):
        mine = _tokens(iq)
        _arrived(q_s.at[:, mine], load_sems.at[TWO, iq])
        _arrived(do_s.at[:, mine], load_sems.at[THREE, iq])
        for j in range(iq + ONE):
            if j < iq:
                block(iq, j)
            else:
                for first in (0, BLOCK // TWO):
                    block(iq, j, first, BLOCK // TWO, first + BLOCK // TWO)
            between(iq * (iq + ONE) // TWO + j - 1)
        for n in range(heads):
            dq_s[n, mine, :] = (sum_s[n] * SCALE).T.astype(BF)
        sum_s[...] = jnp.zeros_like(sum_s)
        _start(dq_s.at[:, mine], dq_o.at[:, mine], out_sem.at[ZERO])

    k_s[...] = (dk_s[...] * SCALE).astype(BF)
    v_s[...] = dv_s[...].astype(BF)
    _start(k_s, dk_o, out_sem.at[ONE])
    _start(v_s, dv_o, out_sem.at[2])
    out_s, in_s, mate_sems = mates
    sums.dealt(out_s, in_s, mate_sems)
    rows_o[...] = in_s[...]
    sums.all_sent()
    _arrived(dq_s, out_sem.at[ZERO])
    _arrived(k_s, out_sem.at[ONE])
    _arrived(v_s, out_sem.at[2])


def attend_back(q, k, v, do, lse, delta, gate, up, down):
    heads, n, _ = q.shape
    vmem, anywhere = pl.BlockSpec(memory_space=pltpu.VMEM), pl.BlockSpec(memory_space=pl.ANY)
    shapes = (q.shape, k.shape, k.shape, (8, 2, 8, WIDE), (ROWS, DIM))
    dma = pltpu.SemaphoreType.DMA
    return pl.pallas_call(
        _attend_back,
        in_specs=[anywhere] * 4 + [vmem] * TWO + [anywhere] * 3,
        out_specs=[anywhere] * 3 + [vmem] * 2,
        out_shape=[jax.ShapeDtypeStruct(s, BF) for s in shapes],
        scratch_shapes=[pltpu.VMEM(s, BF) for s in (q.shape, k.shape, k.shape, q.shape, q.shape)]
        + [pltpu.VMEM(s, F32) for s in (k.shape, k.shape, (heads, HEAD, BLOCK))] + [dma((4, 4)), dma((3,))] + _sum_scratch(LATER),
        compiler_params=pltpu.CompilerParams(collective_id=1, has_side_effects=True, vmem_limit_bytes=VMEM),
        name="attend_back",
    )(q, k, v, do, lse, delta, gate.reshape(*GRID, COLOURS, ROWS, -ONE), up.reshape(*GRID, COLOURS, ROWS, -ONE), down.reshape(*GRID, PLACES, 2, ROWS, DIM))


def _project_back(dq, dk, dv, cos_ref, sin_ref, x, dh, turned, qkv, dwo, dx_o, rows_o,
                  dq_s, dk_s, dv_s, x_s, dh_s, at_s, w_s, by_s, dw_s, load_sems, out_sem, *refs):
    at = _place()
    heads, n, _ = dq_s.shape
    blocks = n // BLOCK
    sums, mates = _sums(at, (MIXED,), refs, None)
    for i in range(blocks):
        here = _tokens(i)
        _start(dq.at[:, here], dq_s.at[:, here], load_sems.at[ZERO, i])
        _start(dk.at[here], dk_s.at[here], load_sems.at[ONE, i])
        _start(dv.at[here], dv_s.at[here], load_sems.at[TWO, i])
    later = ((turned, at_s), (x, x_s), (dh, dh_s), (qkv, w_s))
    for i, (src, dst) in enumerate(later):
        _start(src, dst, load_sems.at[THREE, i])
    _greet(at)

    @pl.when(at["k"] == ZERO)
    def _():
        sums.give(MIXED, dwo)

    @pl.when(at["k"] == ONE)
    def _():
        sums.keep(MIXED, dwo)

    for i in range(blocks):
        here = slice(i * BLOCK, i * BLOCK + BLOCK)
        _arrived(dq_s.at[:, here], load_sems.at[ZERO, i])
        _arrived(dk_s.at[here], load_sems.at[ONE, i])
        _arrived(dv_s.at[here], load_sems.at[TWO, i])
        cos, sin = cos_ref[here, :], sin_ref[here, :]
        for m in range(heads + ONE):
            one = (dq_s[m, here, :] if m < heads else dk_s[here, :]).astype(F32)
            by_s[here, m * HEAD : (m + 1) * HEAD] = (one * cos - pltpu.roll(one, HEAD // TWO, 1) * sin).astype(BF)
        by_s[here, (heads + ONE) * HEAD :] = dv_s[here, :]
    _arrived(at_s, load_sems.at[THREE, 0])
    for c in range(0, by_s.shape[ONE], WIDE):
        dw_s[:, :, :, :, c : c + WIDE] = _mm(at_s[...], by_s[:, c : c + WIDE]).astype(BF).reshape(*GRID, COLOURS, ROWS, WIDE)

    @pl.when(at["k"] == ZERO)
    def _():
        sums.own[0][...] = dw_s[...]

    @pl.when(at["k"] == ONE)
    def _():
        sums.give(MIXED, dw_s)
        sums.kept(MIXED)

    for i, (_, dst) in enumerate(later[1:]):
        _arrived(dst, load_sems.at[THREE, i + 1])
    w = w_s[...]

    def back(i):
        here = slice(i * BLOCK, i * BLOCK + BLOCK)
        da = _mt(by_s[here, :], w).astype(BF)
        dh_s[here, :] = (dh_s[here, :].astype(F32) + _norm_back(x_s[here, :], da)).astype(BF)
        _start(dh_s.at[here], dx_o.at[here], out_sem.at[i])

    for i in range(sums.STEPS):
        if i < blocks:
            back(i)
        sums.steps(i)
    sums.deal_out(1, *mates)
    out_s, in_s, mate_sems = mates
    sums.dealt(out_s, in_s, mate_sems)
    rows_o[...] = in_s[...]
    sums.all_sent()
    for i in range(blocks):
        _arrived(dh_s.at[slice(i * BLOCK, i * BLOCK + BLOCK)], out_sem.at[i])


def project_back(dq, dk, dv, cos, sin, x, dh, turned, qkv, dwo):
    n, d = x.shape
    width = qkv.shape[ONE]
    vmem, anywhere = pl.BlockSpec(memory_space=pltpu.VMEM), pl.BlockSpec(memory_space=pl.ANY)
    dma = pltpu.SemaphoreType.DMA
    return pl.pallas_call(
        _project_back,
        in_specs=[anywhere] * 3 + [vmem] * TWO + [anywhere] * 5,
        out_specs=[anywhere, vmem],
        out_shape=[jax.ShapeDtypeStruct(s, BF) for s in ((n, d), (8, 1, 8, WIDE))],
        scratch_shapes=[pltpu.VMEM(s, BF) for s in (dq.shape, dk.shape, dk.shape, (n, d), (n, d), (d, n), (d, width), (n, width),
                                                    (*GRID, COLOURS, ROWS, width))] + [dma((4, 4)), dma((4,))] + _sum_scratch((MIXED,)),
        compiler_params=pltpu.CompilerParams(collective_id=2, has_side_effects=True, vmem_limit_bytes=VMEM),
        name="project_back",
    )(dq, dk, dv, cos, sin, x, dh, turned, qkv, dwo.reshape(*GRID, COLOURS, ROWS, -ONE))


def _deal(dx_ref, mixed_ref, wide_ref, down_ref, dx_o, wq_o, wk_o, wv_o, wo_o, wg_o, wu_o, wd_o):
    dx_o[...] = dx_ref[...]

    @pl.when(_first())
    def _():
        for j in range(MATES):
            for lo in (0, HEAD):
                found = _from_mixed((wq_o, wk_o, wv_o, wo_o), _columns(j) + lo)
                if found:
                    ref, first = found
                    ref[:, first : first + HEAD] = mixed_ref[j, 0, ZERO:SIX, lo : lo + HEAD]
            for n, ref in enumerate((wg_o, wu_o)):
                ref[:, _columns(j) : _columns(j) + WIDE] = wide_ref[j, n, ZERO:SIX, :]
        wd_o[...] = down_ref[...]


def deal(dx, mixed, wide, down):
    n, d = dx.shape
    outs = ((6, DIM), (6, HEAD), (6, HEAD), (6, DIM), (6, FULL), (6, FULL), (ROWS, DIM))
    return _call(_deal, "deal", n // BLOCK, [(dx, *_rows(BLOCK, d))] + [(a, *_all(*a.shape)) for a in (mixed, wide, down)],
                 [((n, d), BF, *_rows(BLOCK, d))] + [(shape, BF, *_all(*shape)) for shape in outs])


def solution(mesh):
    def step(x, dy, *weights):
        x, dy = x[0], dy[0]
        qkv, wo, gate, up, down, at, dyt, q, k, v, o, cos, sin, lse = advance(x, dy, *(w[0] for w in weights))
        dh, do, delta, dwo, dwg, dwu, dwd = middle(o, x, dy, dyt, wo, gate, up, down)
        dq, dk, dv, wide, tall = attend_back(q, k, v, do, lse, delta, dwg, dwu, dwd)
        dx, mixed = project_back(dq, dk, dv, cos, sin, x, dh, at, qkv, dwo)
        return tuple(g[None] for g in deal(dx, mixed, wide, tall))

    states, cut = P(("rep", "dp"), None, None), P(None, "dp", None)
    return jax.shard_map(
        step,
        mesh=mesh,
        in_specs=(states, states) + (cut,) * 7,
        out_specs=(states,) + (P("rep", "dp", None),) * 7,
        check_vma=False,
    )
```
